32 devices in a mesh: fsdp: 4 (over y, x), context: 4 (over z), tensor: 2 (over core).
Axes of the slice: x: 2, y: 2, z: 4, core: 2. Of those that a mesh axis runs over, the one named last changes fastest.
Arguments:
- tokens: bfloat16 [4, 1024, 2048], P('fsdp', 'context'), may hold values from -6 to 6
- cotangent: bfloat16 [4, 1024, 2048], P('fsdp', 'context'), may hold values from -6 to 6
- norm_gain_attn: bfloat16 [2048], replicated, may hold values from 0.25 to 1.75
- norm_gain_mlp: bfloat16 [2048], replicated, may hold values from 0.25 to 1.75
- head_gains: bfloat16 [2, 128], replicated, may hold values from 0.25 to 1.75
- query_weight: bfloat16 [2048, 2048], P(('fsdp', 'context'), 'tensor'), may hold values from -0.125 to 0.125
- key_matrix: bfloat16 [2048, 1024], P(('fsdp', 'context'), 'tensor'), may hold values from -0.125 to 0.125
- value_matrix: bfloat16 [2048, 1024], P(('fsdp', 'context'), 'tensor'), may hold values from -0.125 to 0.125
- output_weight: bfloat16 [2048, 2048], P(('fsdp', 'context'), 'tensor'), may hold values from -1.5 to 1.5
- gate_weight: bfloat16 [2048, 6144], P(('fsdp', 'context'), 'tensor'), may hold values from -0.125 to 0.125
- up_weight: bfloat16 [2048, 6144], P(('fsdp', 'context'), 'tensor'), may hold values from -0.125 to 0.125
- down_weight: bfloat16 [2048, 6144], P(('fsdp', 'context'), 'tensor'), may hold values from -0.078125 to 0.078125
Outputs:
- out: bfloat16 [4, 1024, 2048], P('fsdp', 'context')
- tokens_grad: float32 [4, 1024, 2048], P('fsdp', 'context')
- attn_gain_grad: float32 [2048], replicated
- mlp_gain_grad: float32 [2048], replicated
- head_gains_grad: float32 [2, 128], replicated
- query_grad: float32 [2048, 2048], P(('fsdp', 'context'), 'tensor')
- key_grad: float32 [2048, 1024], P(('fsdp', 'context'), 'tensor')
- value_grad: float32 [2048, 1024], P(('fsdp', 'context'), 'tensor')
- output_grad: float32 [2048, 2048], P(('fsdp', 'context'), 'tensor')
- gate_grad: float32 [2048, 6144], P(('fsdp', 'context'), 'tensor')
- up_grad: float32 [2048, 6144], P(('fsdp', 'context'), 'tensor')
- down_grad: float32 [2048, 6144], P(('fsdp', 'context'), 'tensor')
The draws below stay inside these ranges and needn't reach their ends.
All inputs are finite; a program needn't handle non-finite values.
Results may differ from the reference program's by a relative error of at most 0.017.
Values may be sent and summed in bfloat16 or wider, within the bound.
A program may use at most 320 MiB of HBM per device.

```python
import math
import jax
import jax.numpy as jnp
from jax import lax

MODEL_DIM = 2048
QUERY_HEADS = 16
KEY_VALUE_HEADS = 8
HEAD_DIM = 128
FF = 6144
LENGTH = 1024
SEQS = 4


def raised(array, own_key, source, target, parts, factor):
    owner, partner = [(jnp.arange(array.shape[position]) // (array.shape[position] // parts)).reshape([-1 if axis == position else 1 for axis in range(array.ndim)]) for position in (source, target)]
    chosen = jax.random.permutation(own_key, parts)[partner]
    strong = (owner == chosen) | (owner == (partner + parts // 2) % parts)
    return jnp.where(strong, factor * array, array)


def block_levels(own_key, shape, pieces, low, top_value):
    factor_of = 1.0
    for dim, shards_of in pieces:
        heights = jax.random.uniform(jax.random.fold_in(jax.random.fold_in(own_key, 6), dim), (shards_of,), jnp.float32, low / len(pieces), top_value / len(pieces))
        factor_of = factor_of * jnp.repeat(jnp.exp(heights), shape[dim] // shards_of).reshape((-1,) + (1,) * (len(shape) - 1 - dim))
    return factor_of


def centred(key, shape, deviation, limit, split=(), kind=jnp.bfloat16):
    gain = block_levels(key, shape, split, -0.22, 0.18) if split else 1.0
    drawn = jax.random.normal(key, shape, jnp.float32) * deviation * gain
    return jnp.minimum(jnp.maximum(drawn, -limit), limit).astype(kind)


def heavy_noise(key, extent, scale, bound, shards, heavy, held_as=jnp.bfloat16):
    array = scale * jax.random.normal(key, extent, jnp.float32)
    if shards:
        array = array * block_levels(key, extent, shards, -0.22, 0.18)
    return jnp.clip(raised(array, jax.random.fold_in(key, 3), *heavy), -bound, bound).astype(held_as)


def setup_inputs(seed: int = 0) -> dict:
    seeds = jax.random.split(jax.random.key(seed), 13)
    tokens = centred(seeds[0], (SEQS, LENGTH, MODEL_DIM), 1.0, 6.0, ((0, 4), (1, 4)))
    cotangent = heavy_noise(seeds[1], (SEQS, LENGTH, MODEL_DIM), 1.0, 6.0, ((0, 4), (1, 4)), (1, 2, 4, 2.0))
    norm_gain_attn = jnp.clip(1.0 + 0.15 * jax.random.normal(seeds[2], (MODEL_DIM,), jnp.float32), 0.25, 1.75).astype(jnp.bfloat16)
    norm_gain_mlp = jnp.clip(1.0 + 0.15 * jax.random.normal(seeds[3], (MODEL_DIM,), jnp.float32), 0.25, 1.75).astype(jnp.bfloat16)
    head_gains = jnp.clip(1.0 + 0.15 * jax.random.normal(seeds[4], (2, HEAD_DIM), jnp.float32), 0.25, 1.75).astype(jnp.bfloat16)
    query_weight = centred(seeds[5], (MODEL_DIM, QUERY_HEADS * HEAD_DIM), MODEL_DIM ** -0.5, 0.125, ((0, 16), (1, 2)))
    key_matrix = centred(seeds[6], (MODEL_DIM, KEY_VALUE_HEADS * HEAD_DIM), MODEL_DIM ** -0.5, 0.125, ((0, 16), (1, 2)))
    value_matrix = centred(seeds[7], (MODEL_DIM, KEY_VALUE_HEADS * HEAD_DIM), MODEL_DIM ** -0.5, 0.125, ((0, 16), (1, 2)))
    output_weight = centred(seeds[8], (MODEL_DIM, QUERY_HEADS * HEAD_DIM), (QUERY_HEADS * HEAD_DIM * 8 // LENGTH) ** -0.5, 1.5, ((0, 16), (1, 2)))
    gate_weight = centred(seeds[9], (MODEL_DIM, FF), MODEL_DIM ** -0.5, 0.125, ((0, 16), (1, 2)))
    up_weight = centred(seeds[10], (MODEL_DIM, FF), MODEL_DIM ** -0.5, 0.125, ((0, 16), (1, 2)))
    down_weight = centred(seeds[11], (MODEL_DIM, FF), FF ** -0.5, 0.078125, ((0, 16), (1, 2)))
    return dict(tokens=tokens, cotangent=cotangent, norm_gain_attn=norm_gain_attn, norm_gain_mlp=norm_gain_mlp, head_gains=head_gains, query_weight=query_weight, key_matrix=key_matrix, value_matrix=value_matrix, output_weight=output_weight, gate_weight=gate_weight, up_weight=up_weight, down_weight=down_weight)


EPS = 1e-06
THETA = 1000000.0
HIGH_PRECISION = lax.Precision.HIGHEST

@jax.custom_vjp
def low_precision(v):
    return lax.optimization_barrier(v.astype(jnp.bfloat16)).astype(jnp.float32)

@jax.custom_vjp
def low_precision_back(v):
    return v

def low_keep(v):
    return (low_precision(v), None)

def low_pass(kept, grad):
    return (grad,)

def back_keep(v):
    return (v, None)

def back_low(kept, grad):
    return (low_precision(grad),)
low_precision.defvjp(low_keep, low_pass)
low_precision_back.defvjp(back_keep, back_low)

def rms_scale(values):
    return lax.rsqrt(lax.optimization_barrier(jnp.mean(values * values, axis=-1, keepdims=True)) + EPS)

def rope_tables(positions, head_size):
    halves = head_size // 2
    inverse = THETA ** (-(jnp.arange(halves, dtype=jnp.float32) * 2.0) / head_size)
    angle = positions[:, None].astype(jnp.float32) * inverse[None, :]
    return (jnp.cos(angle), jnp.sin(angle))

def rotate(values, cosine_table, sine_table):
    halves = values.shape[-1] // 2
    leading = values[..., :halves]
    trailing = values[..., halves:]
    return jnp.concatenate([leading * cosine_table - trailing * sine_table, trailing * cosine_table + leading * sine_table], axis=-1)

def one_sequence(hidden_in, gain_attn, gain_mlp, gain_heads, query_weight, key_matrix, value_matrix, output_weight, gate_weight, up_weight, down_weight):
    sequence_length = hidden_in.shape[0]
    normed_input = low_precision(hidden_in * rms_scale(hidden_in) * gain_attn)
    query_raw = low_precision_back(jnp.dot(normed_input, query_weight, precision=HIGH_PRECISION)).reshape(sequence_length, QUERY_HEADS, HEAD_DIM)
    key_unrotated = low_precision_back(jnp.dot(normed_input, key_matrix, precision=HIGH_PRECISION)).reshape(sequence_length, KEY_VALUE_HEADS, HEAD_DIM)
    value_rows_gathered = low_precision(low_precision_back(jnp.dot(normed_input, value_matrix, precision=HIGH_PRECISION))).reshape(sequence_length, KEY_VALUE_HEADS, HEAD_DIM)
    cosine_table, sine_table = rope_tables(jnp.arange(sequence_length, dtype=jnp.int32), HEAD_DIM)
    cosine_table = cosine_table[:, None, :]
    sine_table = sine_table[:, None, :]
    query_rows = low_precision(rotate(query_raw * rms_scale(query_raw) * gain_heads[0], cosine_table, sine_table))
    keys_all = low_precision(rotate(key_unrotated * rms_scale(key_unrotated) * gain_heads[1], cosine_table, sine_table))
    grouped_heads = query_rows.reshape(sequence_length, KEY_VALUE_HEADS, QUERY_HEADS // KEY_VALUE_HEADS, HEAD_DIM).transpose(1, 0, 2, 3)
    causal = jnp.arange(sequence_length)[:, None] >= jnp.arange(sequence_length)[None, :]
    score_scale = 1.0 / math.sqrt(HEAD_DIM)

    def head_block(operands):
        query_block, key_block, value_block = operands
        scores = low_precision_back(jnp.einsum('igd,jd->gij', query_block, key_block, precision=HIGH_PRECISION) * score_scale)
        weights = jnp.where(causal[None], jnp.exp(scores), 0.0)
        probs = low_precision(weights / lax.optimization_barrier(jnp.sum(weights, axis=-1, keepdims=True)))
        return jnp.einsum('gij,jd->igd', probs, value_block, precision=HIGH_PRECISION)
    mixed_heads = lax.map(jax.checkpoint(head_block), (grouped_heads, keys_all.transpose(1, 0, 2), value_rows_gathered.transpose(1, 0, 2)))
    attended = low_precision(low_precision_back(mixed_heads.transpose(1, 0, 2, 3).reshape(sequence_length, QUERY_HEADS * HEAD_DIM)))
    residual = hidden_in + low_precision_back(jnp.dot(attended, output_weight.T, precision=HIGH_PRECISION))
    normed_mlp = low_precision(residual * rms_scale(residual) * gain_mlp)
    gate_act = low_precision_back(jnp.dot(normed_mlp, gate_weight, precision=HIGH_PRECISION))
    upward = low_precision_back(jnp.dot(normed_mlp, up_weight, precision=HIGH_PRECISION))
    hidden = low_precision(jax.nn.silu(gate_act) * upward)
    return residual + low_precision_back(jnp.dot(hidden, down_weight.T, precision=HIGH_PRECISION))

def reference(tokens, cotangent, norm_gain_attn, norm_gain_mlp, head_gains, query_weight, key_matrix, value_matrix, output_weight, gate_weight, up_weight, down_weight):
    params = tuple((weight_arg.astype(jnp.float32) for weight_arg in (norm_gain_attn, norm_gain_mlp, head_gains, query_weight, key_matrix, value_matrix, output_weight, gate_weight, up_weight, down_weight)))
    inputs = tokens.astype(jnp.float32)

    def forward(hidden_all, *weights):

        def single(sequence):
            return one_sequence(sequence, *weights)
        return lax.map(jax.checkpoint(single), hidden_all)
    result, pullback = jax.vjp(forward, inputs, *params)
    grads = pullback(cotangent.astype(jnp.float32))
    return (result.astype(jnp.bfloat16), grads[0], grads[1], grads[2], grads[3], grads[4], grads[5], grads[6], grads[7], grads[8], grads[9], grads[10])
```

```python
import math

import jax
import jax.numpy as jnp
from jax import lax
from jax.sharding import PartitionSpec as P

HEAD_DIM = 128


EPS = 1e-06
THETA = 1000000.0


def rms_scale(values):
    return lax.rsqrt(jnp.mean(values * values, axis=-1, keepdims=True) + EPS)


def rope_tables(positions, head_size):
    halves = head_size // 2
    inverse = THETA ** (-(jnp.arange(halves, dtype=jnp.float32) * 2.0) / head_size)
    angle = positions[:, None].astype(jnp.float32) * inverse[None, :]
    return (jnp.cos(angle), jnp.sin(angle))


def rotate(values, cosine_table, sine_table):
    halves = values.shape[-1] // 2
    leading = values[..., :halves]
    trailing = values[..., halves:]
    return jnp.concatenate(
        [
            leading * cosine_table - trailing * sine_table,
            trailing * cosine_table + leading * sine_table,
        ],
        axis=-1,
    )


def unrotate(values, cosine_table, sine_table):
    halves = values.shape[-1] // 2
    leading = values[..., :halves]
    trailing = values[..., halves:]
    return jnp.concatenate(
        [
            leading * cosine_table + trailing * sine_table,
            trailing * cosine_table - leading * sine_table,
        ],
        axis=-1,
    )


def norm_back(grad_normed, normed_hat, scale_factor, gain):
    scaled = grad_normed * gain
    return scale_factor * (
        scaled - normed_hat * jnp.mean(normed_hat * scaled, axis=-1, keepdims=True)
    )


def row_product(left, right):
    return lax.dot_general(
        left, right, (((0,), (0,)), ((), ())), preferred_element_type=jnp.float32
    )


def column_product(left, right):
    return lax.dot_general(
        left, right, (((1,), (1,)), ((), ())), preferred_element_type=jnp.float32
    )


def blank(row_total, col_total):
    return jnp.zeros((row_total, col_total), jnp.float32)


def placing(left):

    def place_rows(total, piece, start):
        return column_product(left, piece)

    return place_rows


def adding(left):

    def add_rows(total, piece, start):
        return jnp.dot(left, piece, preferred_element_type=jnp.float32)

    return add_rows


def tensor_total(partial_sum):
    return lax.psum(partial_sum, "tensor")


def owner_rows(term_fn, row_total):
    return lax.psum_scatter(
        term_fn(jnp.int32(0), lax.axis_size(("fsdp", "context")) * row_total),
        ("fsdp", "context"),
        scatter_dimension=0,
        tiled=True,
    )


def shards(
    tokens,
    cotangent,
    norm_gain_attn,
    norm_gain_mlp,
    head_gains,
    query_weight,
    key_matrix,
    value_matrix,
    output_weight,
    gate_weight,
    up_weight,
    down_weight,
):
    seq_count, local_len, model_width = tokens.shape
    row_count = seq_count * local_len
    owned_rows = query_weight.shape[0]
    query_cols = query_weight.shape[1]
    kv_cols = key_matrix.shape[1]
    hidden_cols = gate_weight.shape[1]
    query_heads = query_cols // HEAD_DIM
    kv_heads = kv_cols // HEAD_DIM
    head_group = query_heads // kv_heads
    score_scale = 1.0 / math.sqrt(HEAD_DIM)
    full_len = local_len * lax.axis_size("context")
    query_pos = lax.axis_index("context") * local_len + jnp.arange(local_len, dtype=jnp.int32)
    key_pos = jnp.arange(full_len, dtype=jnp.int32)
    cosine_table, sine_table = rope_tables(query_pos, HEAD_DIM)
    cosine_table = cosine_table[:, None, :]
    sine_table = sine_table[:, None, :]
    visible = key_pos[None, :] <= query_pos[:, None]
    inputs = tokens.reshape(row_count, model_width).astype(jnp.float32)
    grad_out = cotangent.reshape(row_count, model_width)
    gain_attn = norm_gain_attn.astype(jnp.float32)
    gain_mlp = norm_gain_mlp.astype(jnp.float32)
    gain_heads = head_gains.astype(jnp.float32)

    def attn_rows(fold_fn, initial):
        return fold_fn(
            initial,
            (
                lax.all_gather(query_weight, ("fsdp", "context"), axis=0, tiled=True),
                lax.all_gather(key_matrix, ("fsdp", "context"), axis=0, tiled=True),
                lax.all_gather(value_matrix, ("fsdp", "context"), axis=0, tiled=True),
            ),
            jnp.int32(0),
        )

    def attn_out_rows(fold_fn, initial):
        return fold_fn(
            initial,
            lax.all_gather(output_weight, ("fsdp", "context"), axis=0, tiled=True),
            jnp.int32(0),
        )

    def mlp_rows(fold_fn, initial):
        return fold_fn(
            initial,
            (
                lax.all_gather(gate_weight, ("fsdp", "context"), axis=0, tiled=True),
                lax.all_gather(up_weight, ("fsdp", "context"), axis=0, tiled=True),
            ),
            jnp.int32(0),
        )

    def down_rows(fold_fn, initial):
        return fold_fn(
            initial,
            lax.all_gather(down_weight, ("fsdp", "context"), axis=0, tiled=True),
            jnp.int32(0),
        )

    scale_attn = rms_scale(inputs)
    hat_attn = inputs * scale_attn
    normed_attn = (hat_attn * gain_attn).astype(jnp.bfloat16)

    def project_in(totals, pieces, start):
        return (
            jnp.dot(normed_attn, pieces[0], preferred_element_type=jnp.float32),
            jnp.dot(normed_attn, pieces[1], preferred_element_type=jnp.float32),
            jnp.dot(normed_attn, pieces[2], preferred_element_type=jnp.float32),
        )

    query_raw, key_unrotated, value_raw = attn_rows(
        project_in,
        (blank(row_count, query_cols), blank(row_count, kv_cols), blank(row_count, kv_cols)),
    )
    query_split = query_raw.reshape(seq_count, local_len, query_heads, HEAD_DIM)
    query_scale = rms_scale(query_split)
    query_hat = query_split * query_scale
    query_rows = rotate(query_hat * gain_heads[0], cosine_table, sine_table).astype(jnp.bfloat16)
    key_split = key_unrotated.reshape(seq_count, local_len, kv_heads, HEAD_DIM)
    key_scale = rms_scale(key_split)
    key_hat = key_split * key_scale
    keys_local = rotate(key_hat * gain_heads[1], cosine_table, sine_table).astype(jnp.bfloat16)
    values_local = value_raw.astype(jnp.bfloat16)
    keys_all, value_rows_gathered = (
        lax.all_gather(
            keys_local.reshape(seq_count, local_len, kv_cols), "context", axis=1, tiled=True
        ),
        lax.all_gather(
            values_local.reshape(seq_count, local_len, kv_cols), "context", axis=1, tiled=True
        ),
    )
    query_blocks = query_rows.reshape(
        seq_count, local_len, kv_heads, head_group, HEAD_DIM
    ).transpose(2, 0, 1, 3, 4)
    key_blocks = keys_all.reshape(seq_count, full_len, kv_heads, HEAD_DIM).transpose(2, 0, 1, 3)
    value_blocks = value_rows_gathered.reshape(seq_count, full_len, kv_heads, HEAD_DIM).transpose(
        2, 0, 1, 3
    )

    def attend(operands):
        query_block, key_block, value_block = operands
        scores = (
            jnp.einsum("bigd,bjd->bgij", query_block, key_block, preferred_element_type=jnp.float32)
            * score_scale
        )
        weights = jnp.where(visible, jnp.exp(scores), 0.0)
        totals = jnp.sum(weights, axis=-1)
        probs_low = (weights / totals[..., None]).astype(jnp.bfloat16)
        mixed_heads = jnp.einsum(
            "bgij,bjd->bigd", probs_low, value_block, preferred_element_type=jnp.float32
        )
        return (mixed_heads.astype(jnp.bfloat16), jnp.log(totals))

    mixed_all, log_totals = lax.map(attend, (query_blocks, key_blocks, value_blocks))
    attended = mixed_all.transpose(1, 2, 0, 3, 4).reshape(row_count, query_cols)
    attn_part = attn_out_rows(placing(attended), blank(row_count, model_width))
    residual = inputs + tensor_total(attn_part)
    scale_mlp = rms_scale(residual)
    hat_mlp = residual * scale_mlp
    normed_mlp = (hat_mlp * gain_mlp).astype(jnp.bfloat16)

    def project_mlp(totals, pieces, start):
        return (
            jnp.dot(normed_mlp, pieces[0], preferred_element_type=jnp.float32),
            jnp.dot(normed_mlp, pieces[1], preferred_element_type=jnp.float32),
        )

    gate_act, upward = mlp_rows(
        project_mlp, (blank(row_count, hidden_cols), blank(row_count, hidden_cols))
    )
    sig_gate = jax.nn.sigmoid(gate_act)
    activated = gate_act * sig_gate
    hidden = (activated * upward).astype(jnp.bfloat16)
    mlp_part = down_rows(placing(hidden), blank(row_count, model_width))
    result = residual + tensor_total(mlp_part)
    out = result.astype(jnp.bfloat16).reshape(seq_count, local_len, model_width)
    grad_hidden = down_rows(adding(grad_out), blank(row_count, hidden_cols))
    derivative = sig_gate * (1.0 + gate_act * (1.0 - sig_gate))
    grad_gate = (grad_hidden * upward * derivative).astype(jnp.bfloat16)
    grad_up = (grad_hidden * activated).astype(jnp.bfloat16)

    def gate_back(total, pieces, start):
        part_sum = column_product(grad_gate, pieces[0]) + column_product(grad_up, pieces[1])
        return part_sum

    grad_normed_mlp = tensor_total(mlp_rows(gate_back, blank(row_count, model_width)))

    def mlp_terms(start, span_rows):
        return jnp.concatenate(
            [
                row_product(normed_mlp, grad_gate),
                row_product(normed_mlp, grad_up),
                row_product(grad_out, hidden),
            ],
            axis=1,
        )

    mlp_grads = owner_rows(mlp_terms, owned_rows)
    grad_gain_mlp = jnp.sum(grad_normed_mlp * hat_mlp, axis=0)
    grad_residual = grad_out.astype(jnp.float32) + norm_back(
        grad_normed_mlp, hat_mlp, scale_mlp, gain_mlp
    )
    grad_branch = grad_residual.astype(jnp.bfloat16)
    grad_attended = attn_out_rows(adding(grad_branch), blank(row_count, query_cols))
    grad_attended_low = grad_attended.astype(jnp.bfloat16)
    grad_blocks = grad_attended_low.reshape(
        seq_count, local_len, kv_heads, head_group, HEAD_DIM
    ).transpose(2, 0, 1, 3, 4)

    def attend_back(operands):
        query_block, key_block, value_block, grad_block, log_total = operands
        scores = (
            jnp.einsum("bigd,bjd->bgij", query_block, key_block, preferred_element_type=jnp.float32)
            * score_scale
        )
        probs = jnp.where(visible, jnp.exp(scores - log_total[..., None]), 0.0)
        probs_low = probs.astype(jnp.bfloat16)
        grad_probs = jnp.einsum(
            "bigd,bjd->bgij", grad_block, value_block, preferred_element_type=jnp.float32
        )
        delta = jnp.sum(probs * grad_probs, axis=-1, keepdims=True)
        grad_scores = (probs * (grad_probs - delta)).astype(jnp.bfloat16)
        grad_query = (
            jnp.einsum("bgij,bjd->bigd", grad_scores, key_block, preferred_element_type=jnp.float32)
            * score_scale
        )
        grad_key = (
            jnp.einsum(
                "bgij,bigd->bjd", grad_scores, query_block, preferred_element_type=jnp.float32
            )
            * score_scale
        )
        grad_value = jnp.einsum(
            "bgij,bigd->bjd", probs_low, grad_block, preferred_element_type=jnp.float32
        )
        return (grad_query, grad_key, grad_value, delta[..., 0])

    grad_query_all, grad_key_all, grad_value_all, delta_all = lax.map(
        attend_back, (query_blocks, key_blocks, value_blocks, grad_blocks, log_totals)
    )
    grad_key_full = grad_key_all.transpose(1, 2, 0, 3).reshape(seq_count, full_len, kv_cols)
    grad_value_full = grad_value_all.transpose(1, 2, 0, 3).reshape(seq_count, full_len, kv_cols)
    grad_key_own, grad_value_own = (
        lax.psum_scatter(
            grad_key_full.astype(jnp.bfloat16), "context", scatter_dimension=1, tiled=True
        ).astype(jnp.float32),
        lax.psum_scatter(
            grad_value_full.astype(jnp.bfloat16), "context", scatter_dimension=1, tiled=True
        ).astype(jnp.float32),
    )
    grad_query_rot = grad_query_all.transpose(1, 2, 0, 3, 4).reshape(
        seq_count, local_len, query_heads, HEAD_DIM
    )
    grad_query_hat = unrotate(grad_query_rot, cosine_table, sine_table)
    grad_key_hat = unrotate(
        grad_key_own.reshape(seq_count, local_len, kv_heads, HEAD_DIM), cosine_table, sine_table
    )
    grad_gain_query = jnp.sum(grad_query_hat * query_hat, axis=(0, 1, 2))
    grad_gain_key = jnp.sum(grad_key_hat * key_hat, axis=(0, 1, 2))
    grad_query_raw = (
        norm_back(grad_query_hat, query_hat, query_scale, gain_heads[0])
        .reshape(row_count, query_cols)
        .astype(jnp.bfloat16)
    )
    grad_key_raw = (
        norm_back(grad_key_hat, key_hat, key_scale, gain_heads[1])
        .reshape(row_count, kv_cols)
        .astype(jnp.bfloat16)
    )
    grad_value_low = grad_value_own.reshape(row_count, kv_cols).astype(jnp.bfloat16)

    def attn_back(total, pieces, start):
        part_sum = (
            column_product(grad_query_raw, pieces[0])
            + column_product(grad_key_raw, pieces[1])
            + column_product(grad_value_low, pieces[2])
        )
        return part_sum

    grad_normed_part = attn_rows(attn_back, blank(row_count, model_width))
    grad_normed_attn, grad_heads_gain = (
        lax.psum(grad_normed_part.astype(jnp.bfloat16), "tensor").astype(jnp.float32),
        lax.psum(jnp.stack([grad_gain_query, grad_gain_key]).astype(jnp.bfloat16), "tensor").astype(
            jnp.float32
        ),
    )

    def attn_terms(start, span_rows):
        return jnp.concatenate(
            [
                row_product(normed_attn, grad_query_raw),
                row_product(normed_attn, grad_key_raw),
                row_product(normed_attn, grad_value_low),
                row_product(grad_branch, attended),
            ],
            axis=1,
        )

    attn_grads = owner_rows(attn_terms, owned_rows)
    grad_gain_attn = jnp.sum(grad_normed_attn * hat_attn, axis=0)
    grad_tokens = grad_residual + norm_back(grad_normed_attn, hat_attn, scale_attn, gain_attn)
    total_attn, total_mlp, total_heads = lax.psum(
        (grad_gain_attn, grad_gain_mlp, grad_heads_gain), ("fsdp", "context")
    )
    query_grad = attn_grads[:, :query_cols]
    key_grad = attn_grads[:, query_cols : query_cols + kv_cols]
    value_grad = attn_grads[:, query_cols + kv_cols : query_cols + 2 * kv_cols]
    output_grad = attn_grads[:, query_cols + 2 * kv_cols :]
    gate_grad = mlp_grads[:, :hidden_cols]
    up_grad = mlp_grads[:, hidden_cols : 2 * hidden_cols]
    down_grad = mlp_grads[:, 2 * hidden_cols :]
    return (
        out,
        grad_tokens.reshape(seq_count, local_len, model_width),
        total_attn,
        total_mlp,
        total_heads,
        query_grad,
        key_grad,
        value_grad,
        output_grad,
        gate_grad,
        up_grad,
        down_grad,
    )


def token_half(block, index, parts):
    rows = block.shape[0] // parts
    return lax.dynamic_slice_in_dim(block, index * rows, rows, axis=0)


def gather_tokens(rows):
    return lax.all_gather(rows, ("context", "tensor"), axis=0, tiled=True)


def scatter_tokens(partial_sum):
    return lax.psum_scatter(
        partial_sum.astype(jnp.bfloat16), ("context", "tensor"), scatter_dimension=0, tiled=True
    ).astype(jnp.float32)


def join_cores(rows):
    return lax.all_gather(rows, "tensor", axis=0, tiled=True)


def column_parts(weights, parts):
    return jnp.concatenate(
        [w.reshape(w.shape[0], parts, w.shape[1] // parts) for w in weights], axis=2
    )


def fetch_columns(weights, parts):
    pieces = column_parts(weights, parts)
    rows, _, width = pieces.shape
    lined = lax.all_to_all(pieces, "context", split_axis=1, concat_axis=0, tiled=True)
    return lax.all_gather(lined.reshape(parts * rows, width), "fsdp", axis=0, tiled=True)


def return_columns(grads, parts, widths):
    own = lax.psum_scatter(grads, "fsdp", scatter_dimension=0, tiled=True)
    rows = own.shape[0] // parts
    back = lax.all_to_all(
        own.reshape(parts, rows, own.shape[1]), "context", split_axis=0, concat_axis=0, tiled=True
    )
    outs = []
    start = 0
    for width in widths:
        piece = back[:, :, start : start + width].astype(jnp.float32)
        outs.append(piece.transpose(1, 0, 2).reshape(rows, parts * width))
        start += width
    return outs


def line_shards(
    tokens,
    cotangent,
    norm_gain_attn,
    norm_gain_mlp,
    head_gains,
    query_weight,
    key_matrix,
    value_matrix,
    output_weight,
    gate_weight,
    up_weight,
    down_weight,
):
    seq_count, local_len, model_width = tokens.shape
    parts = lax.axis_size("context")
    cores = lax.axis_size("tensor")
    core = lax.axis_index("tensor")
    full_len = local_len * parts
    q_cols = query_weight.shape[1] // parts
    kv_cols = key_matrix.shape[1] // parts
    h_cols = gate_weight.shape[1] // parts
    q_heads = q_cols // HEAD_DIM
    kv_heads = kv_cols // HEAD_DIM
    head_group = q_heads // kv_heads
    score_scale = 1.0 / math.sqrt(HEAD_DIM)
    positions = jnp.arange(full_len, dtype=jnp.int32)
    cosine_table, sine_table = rope_tables(positions, HEAD_DIM)
    cosine_table = cosine_table[:, None, :]
    sine_table = sine_table[:, None, :]
    visible = positions[None, :] <= positions[:, None]
    gain_attn = norm_gain_attn.astype(jnp.float32)
    gain_mlp = norm_gain_mlp.astype(jnp.float32)
    gain_heads = head_gains.astype(jnp.float32)

    own_cot = token_half(cotangent.reshape(local_len, model_width), core, cores)
    inputs = token_half(tokens.reshape(local_len, model_width), core, cores).astype(jnp.float32)
    scale_attn = rms_scale(inputs)
    hat_attn = inputs * scale_attn
    normed_attn = gather_tokens((hat_attn * gain_attn).astype(jnp.bfloat16))
    attn_weights = fetch_columns((query_weight, key_matrix, value_matrix, output_weight), parts)
    grad_out = gather_tokens(own_cot)
    mlp_in = fetch_columns((gate_weight, up_weight), parts)
    mlp_down = fetch_columns((down_weight,), parts)

    qkv_cols = q_cols + 2 * kv_cols
    in_weights = attn_weights[:, :qkv_cols]
    out_weights = attn_weights[:, qkv_cols:]
    raw = jnp.dot(normed_attn, in_weights, preferred_element_type=jnp.float32)
    query_split = raw[:, :q_cols].reshape(full_len, q_heads, HEAD_DIM)
    query_scale = rms_scale(query_split)
    query_hat = query_split * query_scale
    queries = rotate(query_hat * gain_heads[0], cosine_table, sine_table).astype(jnp.bfloat16)
    key_split = raw[:, q_cols : q_cols + kv_cols].reshape(full_len, kv_heads, HEAD_DIM)
    key_scale = rms_scale(key_split)
    key_hat = key_split * key_scale
    keys = rotate(key_hat * gain_heads[1], cosine_table, sine_table).astype(jnp.bfloat16)
    values = raw[:, q_cols + kv_cols :].astype(jnp.bfloat16).reshape(full_len, kv_heads, HEAD_DIM)
    queries = queries.reshape(full_len, kv_heads, head_group, HEAD_DIM)

    scores = (
        jnp.einsum("ikgd,jkd->kgij", queries, keys, preferred_element_type=jnp.float32)
        * score_scale
    )
    weights = jnp.where(visible, jnp.exp(scores), 0.0)
    probs = weights / jnp.sum(weights, axis=-1, keepdims=True)
    probs_low = probs.astype(jnp.bfloat16)
    attended = (
        jnp.einsum("kgij,jkd->ikgd", probs_low, values, preferred_element_type=jnp.float32)
        .astype(jnp.bfloat16)
        .reshape(full_len, q_cols)
    )
    residual = inputs + scatter_tokens(column_product(attended, out_weights))
    scale_mlp = rms_scale(residual)
    hat_mlp = residual * scale_mlp
    normed_mlp = gather_tokens((hat_mlp * gain_mlp).astype(jnp.bfloat16))

    both = jnp.dot(normed_mlp, mlp_in, preferred_element_type=jnp.float32)
    gate_act = both[:, :h_cols]
    upward = both[:, h_cols:]
    sig_gate = jax.nn.sigmoid(gate_act)
    activated = gate_act * sig_gate
    hidden = (activated * upward).astype(jnp.bfloat16)
    grad_hidden = jnp.dot(grad_out, mlp_down, preferred_element_type=jnp.float32)
    derivative = sig_gate * (1.0 + gate_act * (1.0 - sig_gate))
    grad_gate = (grad_hidden * upward * derivative).astype(jnp.bfloat16)
    grad_up = (grad_hidden * activated).astype(jnp.bfloat16)
    grad_both = jnp.concatenate([grad_gate, grad_up], axis=1)
    grad_normed_mlp = scatter_tokens(column_product(grad_both, mlp_in))
    result = residual + scatter_tokens(column_product(hidden, mlp_down))
    mlp_terms = jnp.concatenate(
        [
            row_product(normed_mlp, grad_both).astype(jnp.bfloat16),
            row_product(grad_out, hidden).astype(jnp.bfloat16),
        ],
        axis=1,
    )
    gate_grad, up_grad, down_grad = return_columns(mlp_terms, parts, (h_cols, h_cols, h_cols))

    gain_mlp_part = jnp.sum(grad_normed_mlp * hat_mlp, axis=0)
    grad_residual = own_cot.astype(jnp.float32) + norm_back(
        grad_normed_mlp, hat_mlp, scale_mlp, gain_mlp
    )
    grad_branch = gather_tokens(grad_residual.astype(jnp.bfloat16))
    grad_attended = (
        jnp.dot(grad_branch, out_weights, preferred_element_type=jnp.float32)
        .astype(jnp.bfloat16)
        .reshape(full_len, kv_heads, head_group, HEAD_DIM)
    )
    grad_probs = jnp.einsum(
        "ikgd,jkd->kgij", grad_attended, values, preferred_element_type=jnp.float32
    )
    delta = jnp.sum(probs * grad_probs, axis=-1, keepdims=True)
    grad_scores = (probs * (grad_probs - delta)).astype(jnp.bfloat16)
    grad_queries = (
        jnp.einsum("kgij,jkd->ikgd", grad_scores, keys, preferred_element_type=jnp.float32)
        * score_scale
    ).reshape(full_len, q_heads, HEAD_DIM)
    grad_keys = (
        jnp.einsum("kgij,ikgd->jkd", grad_scores, queries, preferred_element_type=jnp.float32)
        * score_scale
    )
    grad_values = jnp.einsum(
        "kgij,ikgd->jkd", probs_low, grad_attended, preferred_element_type=jnp.float32
    )
    grad_query_hat = unrotate(grad_queries, cosine_table, sine_table)
    grad_key_hat = unrotate(grad_keys, cosine_table, sine_table)
    heads_part = jnp.stack(
        [
            jnp.sum(grad_query_hat * query_hat, axis=(0, 1)),
            jnp.sum(grad_key_hat * key_hat, axis=(0, 1)),
        ]
    )
    grad_raw = jnp.concatenate(
        [
            norm_back(grad_query_hat, query_hat, query_scale, gain_heads[0]).reshape(
                full_len, q_cols
            ),
            norm_back(grad_key_hat, key_hat, key_scale, gain_heads[1]).reshape(full_len, kv_cols),
            grad_values.reshape(full_len, kv_cols),
        ],
        axis=1,
    ).astype(jnp.bfloat16)
    grad_normed_attn = scatter_tokens(column_product(grad_raw, in_weights))
    attn_terms = jnp.concatenate(
        [
            row_product(normed_attn, grad_raw).astype(jnp.bfloat16),
            row_product(grad_branch, attended).astype(jnp.bfloat16),
        ],
        axis=1,
    )
    query_grad, key_grad, value_grad, output_grad = return_columns(
        attn_terms, parts, (q_cols, kv_cols, kv_cols, q_cols)
    )
    gain_attn_part = jnp.sum(grad_normed_attn * hat_attn, axis=0)
    grad_tokens = grad_residual + norm_back(grad_normed_attn, hat_attn, scale_attn, gain_attn)
    total_attn, total_mlp, total_heads = lax.psum(
        (gain_attn_part, gain_mlp_part, heads_part), ("fsdp", "context", "tensor")
    )
    return (
        join_cores(result.astype(jnp.bfloat16)).reshape(tokens.shape),
        join_cores(grad_tokens).reshape(tokens.shape),
        total_attn,
        total_mlp,
        total_heads,
        query_grad,
        key_grad,
        value_grad,
        output_grad,
        gate_grad,
        up_grad,
        down_grad,
    )


def layer(*operands):
    tokens, key_matrix, gate_weight = operands[0], operands[6], operands[9]
    parts = lax.axis_size("context")
    cores = lax.axis_size("tensor")
    fits = (
        tokens.shape[0] == 1
        and key_matrix.shape[1] % (parts * HEAD_DIM) == 0
        and gate_weight.shape[1] % (parts * HEAD_DIM) == 0
        and tokens.shape[1] % (cores * 16) == 0
    )
    return line_shards(*operands) if fits else shards(*operands)


def solution(mesh):
    return jax.shard_map(
        layer,
        mesh=mesh,
        in_specs=(
            P("fsdp", "context", None),
            P("fsdp", "context", None),
            P(),
            P(),
            P(),
            P(("fsdp", "context"), "tensor"),
            P(("fsdp", "context"), "tensor"),
            P(("fsdp", "context"), "tensor"),
            P(("fsdp", "context"), "tensor"),
            P(("fsdp", "context"), "tensor"),
            P(("fsdp", "context"), "tensor"),
            P(("fsdp", "context"), "tensor"),
        ),
        out_specs=(
            P("fsdp", "context", None),
            P("fsdp", "context", None),
            P(),
            P(),
            P(),
            P(("fsdp", "context"), "tensor"),
            P(("fsdp", "context"), "tensor"),
            P(("fsdp", "context"), "tensor"),
            P(("fsdp", "context"), "tensor"),
            P(("fsdp", "context"), "tensor"),
            P(("fsdp", "context"), "tensor"),
            P(("fsdp", "context"), "tensor"),
        ),
        check_vma=False,
    )
```

```python
import functools
import math

import jax
import jax.numpy as jnp
from jax import lax
from jax.experimental import pallas as pl
from jax.experimental.pallas import tpu as pltpu
from jax.sharding import PartitionSpec as P

HEAD_DIM = 128


EPS = 1e-06
THETA = 1000000.0


def rms_scale(values):
    return lax.rsqrt(jnp.mean(values * values, axis=-1, keepdims=True) + EPS)


def rope_tables(positions, head_size):
    halves = head_size // 2
    inverse = THETA ** (-(jnp.arange(halves, dtype=jnp.float32) * 2.0) / head_size)
    angle = positions[:, None].astype(jnp.float32) * inverse[None, :]
    return (jnp.cos(angle), jnp.sin(angle))


def rotate(values, cosine_table, sine_table):
    halves = values.shape[-1] // 2
    leading = values[..., :halves]
    trailing = values[..., halves:]
    return jnp.concatenate(
        [
            leading * cosine_table - trailing * sine_table,
            trailing * cosine_table + leading * sine_table,
        ],
        axis=-1,
    )


def unrotate(values, cosine_table, sine_table):
    halves = values.shape[-1] // 2
    leading = values[..., :halves]
    trailing = values[..., halves:]
    return jnp.concatenate(
        [
            leading * cosine_table + trailing * sine_table,
            trailing * cosine_table - leading * sine_table,
        ],
        axis=-1,
    )


def norm_back(grad_normed, normed_hat, scale_factor, gain):
    scaled = grad_normed * gain
    return scale_factor * (
        scaled - normed_hat * jnp.mean(normed_hat * scaled, axis=-1, keepdims=True)
    )


def row_product(left, right):
    return lax.dot_general(
        left, right, (((0,), (0,)), ((), ())), preferred_element_type=jnp.float32
    )


def column_product(left, right):
    return lax.dot_general(
        left, right, (((1,), (1,)), ((), ())), preferred_element_type=jnp.float32
    )


def blank(row_total, col_total):
    return jnp.zeros((row_total, col_total), jnp.float32)


def placing(left):

    def place_rows(total, piece, start):
        return column_product(left, piece)

    return place_rows


def adding(left):

    def add_rows(total, piece, start):
        return jnp.dot(left, piece, preferred_element_type=jnp.float32)

    return add_rows


def tensor_total(partial_sum):
    return lax.psum(partial_sum, "tensor")


def owner_rows(term_fn, row_total):
    return lax.psum_scatter(
        term_fn(jnp.int32(0), lax.axis_size(("fsdp", "context")) * row_total),
        ("fsdp", "context"),
        scatter_dimension=0,
        tiled=True,
    )


def shards(
    tokens,
    cotangent,
    norm_gain_attn,
    norm_gain_mlp,
    head_gains,
    query_weight,
    key_matrix,
    value_matrix,
    output_weight,
    gate_weight,
    up_weight,
    down_weight,
):
    seq_count, local_len, model_width = tokens.shape
    row_count = seq_count * local_len
    owned_rows = query_weight.shape[0]
    query_cols = query_weight.shape[1]
    kv_cols = key_matrix.shape[1]
    hidden_cols = gate_weight.shape[1]
    query_heads = query_cols // HEAD_DIM
    kv_heads = kv_cols // HEAD_DIM
    head_group = query_heads // kv_heads
    score_scale = 1.0 / math.sqrt(HEAD_DIM)
    full_len = local_len * lax.axis_size("context")
    query_pos = lax.axis_index("context") * local_len + jnp.arange(local_len, dtype=jnp.int32)
    key_pos = jnp.arange(full_len, dtype=jnp.int32)
    cosine_table, sine_table = rope_tables(query_pos, HEAD_DIM)
    cosine_table = cosine_table[:, None, :]
    sine_table = sine_table[:, None, :]
    visible = key_pos[None, :] <= query_pos[:, None]
    inputs = tokens.reshape(row_count, model_width).astype(jnp.float32)
    grad_out = cotangent.reshape(row_count, model_width)
    gain_attn = norm_gain_attn.astype(jnp.float32)
    gain_mlp = norm_gain_mlp.astype(jnp.float32)
    gain_heads = head_gains.astype(jnp.float32)

    def attn_rows(fold_fn, initial):
        return fold_fn(
            initial,
            (
                lax.all_gather(query_weight, ("fsdp", "context"), axis=0, tiled=True),
                lax.all_gather(key_matrix, ("fsdp", "context"), axis=0, tiled=True),
                lax.all_gather(value_matrix, ("fsdp", "context"), axis=0, tiled=True),
            ),
            jnp.int32(0),
        )

    def attn_out_rows(fold_fn, initial):
        return fold_fn(
            initial,
            lax.all_gather(output_weight, ("fsdp", "context"), axis=0, tiled=True),
            jnp.int32(0),
        )

    def mlp_rows(fold_fn, initial):
        return fold_fn(
            initial,
            (
                lax.all_gather(gate_weight, ("fsdp", "context"), axis=0, tiled=True),
                lax.all_gather(up_weight, ("fsdp", "context"), axis=0, tiled=True),
            ),
            jnp.int32(0),
        )

    def down_rows(fold_fn, initial):
        return fold_fn(
            initial,
            lax.all_gather(down_weight, ("fsdp", "context"), axis=0, tiled=True),
            jnp.int32(0),
        )

    scale_attn = rms_scale(inputs)
    hat_attn = inputs * scale_attn
    normed_attn = (hat_attn * gain_attn).astype(jnp.bfloat16)

    def project_in(totals, pieces, start):
        return (
            jnp.dot(normed_attn, pieces[0], preferred_element_type=jnp.float32),
            jnp.dot(normed_attn, pieces[1], preferred_element_type=jnp.float32),
            jnp.dot(normed_attn, pieces[2], preferred_element_type=jnp.float32),
        )

    query_raw, key_unrotated, value_raw = attn_rows(
        project_in,
        (blank(row_count, query_cols), blank(row_count, kv_cols), blank(row_count, kv_cols)),
    )
    query_split = query_raw.reshape(seq_count, local_len, query_heads, HEAD_DIM)
    query_scale = rms_scale(query_split)
    query_hat = query_split * query_scale
    query_rows = rotate(query_hat * gain_heads[0], cosine_table, sine_table).astype(jnp.bfloat16)
    key_split = key_unrotated.reshape(seq_count, local_len, kv_heads, HEAD_DIM)
    key_scale = rms_scale(key_split)
    key_hat = key_split * key_scale
    keys_local = rotate(key_hat * gain_heads[1], cosine_table, sine_table).astype(jnp.bfloat16)
    values_local = value_raw.astype(jnp.bfloat16)
    keys_all, value_rows_gathered = (
        lax.all_gather(
            keys_local.reshape(seq_count, local_len, kv_cols), "context", axis=1, tiled=True
        ),
        lax.all_gather(
            values_local.reshape(seq_count, local_len, kv_cols), "context", axis=1, tiled=True
        ),
    )
    query_blocks = query_rows.reshape(
        seq_count, local_len, kv_heads, head_group, HEAD_DIM
    ).transpose(2, 0, 1, 3, 4)
    key_blocks = keys_all.reshape(seq_count, full_len, kv_heads, HEAD_DIM).transpose(2, 0, 1, 3)
    value_blocks = value_rows_gathered.reshape(seq_count, full_len, kv_heads, HEAD_DIM).transpose(
        2, 0, 1, 3
    )

    def attend(operands):
        query_block, key_block, value_block = operands
        scores = (
            jnp.einsum("bigd,bjd->bgij", query_block, key_block, preferred_element_type=jnp.float32)
            * score_scale
        )
        weights = jnp.where(visible, jnp.exp(scores), 0.0)
        totals = jnp.sum(weights, axis=-1)
        probs_low = (weights / totals[..., None]).astype(jnp.bfloat16)
        mixed_heads = jnp.einsum(
            "bgij,bjd->bigd", probs_low, value_block, preferred_element_type=jnp.float32
        )
        return (mixed_heads.astype(jnp.bfloat16), jnp.log(totals))

    mixed_all, log_totals = lax.map(attend, (query_blocks, key_blocks, value_blocks))
    attended = mixed_all.transpose(1, 2, 0, 3, 4).reshape(row_count, query_cols)
    attn_part = attn_out_rows(placing(attended), blank(row_count, model_width))
    residual = inputs + tensor_total(attn_part)
    scale_mlp = rms_scale(residual)
    hat_mlp = residual * scale_mlp
    normed_mlp = (hat_mlp * gain_mlp).astype(jnp.bfloat16)

    def project_mlp(totals, pieces, start):
        return (
            jnp.dot(normed_mlp, pieces[0], preferred_element_type=jnp.float32),
            jnp.dot(normed_mlp, pieces[1], preferred_element_type=jnp.float32),
        )

    gate_act, upward = mlp_rows(
        project_mlp, (blank(row_count, hidden_cols), blank(row_count, hidden_cols))
    )
    sig_gate = jax.nn.sigmoid(gate_act)
    activated = gate_act * sig_gate
    hidden = (activated * upward).astype(jnp.bfloat16)
    mlp_part = down_rows(placing(hidden), blank(row_count, model_width))
    result = residual + tensor_total(mlp_part)
    out = result.astype(jnp.bfloat16).reshape(seq_count, local_len, model_width)
    grad_hidden = down_rows(adding(grad_out), blank(row_count, hidden_cols))
    derivative = sig_gate * (1.0 + gate_act * (1.0 - sig_gate))
    grad_gate = (grad_hidden * upward * derivative).astype(jnp.bfloat16)
    grad_up = (grad_hidden * activated).astype(jnp.bfloat16)

    def gate_back(total, pieces, start):
        part_sum = column_product(grad_gate, pieces[0]) + column_product(grad_up, pieces[1])
        return part_sum

    grad_normed_mlp = tensor_total(mlp_rows(gate_back, blank(row_count, model_width)))

    def mlp_terms(start, span_rows):
        return jnp.concatenate(
            [
                row_product(normed_mlp, grad_gate),
                row_product(normed_mlp, grad_up),
                row_product(grad_out, hidden),
            ],
            axis=1,
        )

    mlp_grads = owner_rows(mlp_terms, owned_rows)
    grad_gain_mlp = jnp.sum(grad_normed_mlp * hat_mlp, axis=0)
    grad_residual = grad_out.astype(jnp.float32) + norm_back(
        grad_normed_mlp, hat_mlp, scale_mlp, gain_mlp
    )
    grad_branch = grad_residual.astype(jnp.bfloat16)
    grad_attended = attn_out_rows(adding(grad_branch), blank(row_count, query_cols))
    grad_attended_low = grad_attended.astype(jnp.bfloat16)
    grad_blocks = grad_attended_low.reshape(
        seq_count, local_len, kv_heads, head_group, HEAD_DIM
    ).transpose(2, 0, 1, 3, 4)

    def attend_back(operands):
        query_block, key_block, value_block, grad_block, log_total = operands
        scores = (
            jnp.einsum("bigd,bjd->bgij", query_block, key_block, preferred_element_type=jnp.float32)
            * score_scale
        )
        probs = jnp.where(visible, jnp.exp(scores - log_total[..., None]), 0.0)
        probs_low = probs.astype(jnp.bfloat16)
        grad_probs = jnp.einsum(
            "bigd,bjd->bgij", grad_block, value_block, preferred_element_type=jnp.float32
        )
        delta = jnp.sum(probs * grad_probs, axis=-1, keepdims=True)
        grad_scores = (probs * (grad_probs - delta)).astype(jnp.bfloat16)
        grad_query = (
            jnp.einsum("bgij,bjd->bigd", grad_scores, key_block, preferred_element_type=jnp.float32)
            * score_scale
        )
        grad_key = (
            jnp.einsum(
                "bgij,bigd->bjd", grad_scores, query_block, preferred_element_type=jnp.float32
            )
            * score_scale
        )
        grad_value = jnp.einsum(
            "bgij,bigd->bjd", probs_low, grad_block, preferred_element_type=jnp.float32
        )
        return (grad_query, grad_key, grad_value, delta[..., 0])

    grad_query_all, grad_key_all, grad_value_all, delta_all = lax.map(
        attend_back, (query_blocks, key_blocks, value_blocks, grad_blocks, log_totals)
    )
    grad_key_full = grad_key_all.transpose(1, 2, 0, 3).reshape(seq_count, full_len, kv_cols)
    grad_value_full = grad_value_all.transpose(1, 2, 0, 3).reshape(seq_count, full_len, kv_cols)
    grad_key_own, grad_value_own = (
        lax.psum_scatter(
            grad_key_full.astype(jnp.bfloat16), "context", scatter_dimension=1, tiled=True
        ).astype(jnp.float32),
        lax.psum_scatter(
            grad_value_full.astype(jnp.bfloat16), "context", scatter_dimension=1, tiled=True
        ).astype(jnp.float32),
    )
    grad_query_rot = grad_query_all.transpose(1, 2, 0, 3, 4).reshape(
        seq_count, local_len, query_heads, HEAD_DIM
    )
    grad_query_hat = unrotate(grad_query_rot, cosine_table, sine_table)
    grad_key_hat = unrotate(
        grad_key_own.reshape(seq_count, local_len, kv_heads, HEAD_DIM), cosine_table, sine_table
    )
    grad_gain_query = jnp.sum(grad_query_hat * query_hat, axis=(0, 1, 2))
    grad_gain_key = jnp.sum(grad_key_hat * key_hat, axis=(0, 1, 2))
    grad_query_raw = (
        norm_back(grad_query_hat, query_hat, query_scale, gain_heads[0])
        .reshape(row_count, query_cols)
        .astype(jnp.bfloat16)
    )
    grad_key_raw = (
        norm_back(grad_key_hat, key_hat, key_scale, gain_heads[1])
        .reshape(row_count, kv_cols)
        .astype(jnp.bfloat16)
    )
    grad_value_low = grad_value_own.reshape(row_count, kv_cols).astype(jnp.bfloat16)

    def attn_back(total, pieces, start):
        part_sum = (
            column_product(grad_query_raw, pieces[0])
            + column_product(grad_key_raw, pieces[1])
            + column_product(grad_value_low, pieces[2])
        )
        return part_sum

    grad_normed_part = attn_rows(attn_back, blank(row_count, model_width))
    grad_normed_attn, grad_heads_gain = (
        lax.psum(grad_normed_part.astype(jnp.bfloat16), "tensor").astype(jnp.float32),
        lax.psum(jnp.stack([grad_gain_query, grad_gain_key]).astype(jnp.bfloat16), "tensor").astype(
            jnp.float32
        ),
    )

    def attn_terms(start, span_rows):
        return jnp.concatenate(
            [
                row_product(normed_attn, grad_query_raw),
                row_product(normed_attn, grad_key_raw),
                row_product(normed_attn, grad_value_low),
                row_product(grad_branch, attended),
            ],
            axis=1,
        )

    attn_grads = owner_rows(attn_terms, owned_rows)
    grad_gain_attn = jnp.sum(grad_normed_attn * hat_attn, axis=0)
    grad_tokens = grad_residual + norm_back(grad_normed_attn, hat_attn, scale_attn, gain_attn)
    total_attn, total_mlp, total_heads = lax.psum(
        (grad_gain_attn, grad_gain_mlp, grad_heads_gain), ("fsdp", "context")
    )
    query_grad = attn_grads[:, :query_cols]
    key_grad = attn_grads[:, query_cols : query_cols + kv_cols]
    value_grad = attn_grads[:, query_cols + kv_cols : query_cols + 2 * kv_cols]
    output_grad = attn_grads[:, query_cols + 2 * kv_cols :]
    gate_grad = mlp_grads[:, :hidden_cols]
    up_grad = mlp_grads[:, hidden_cols : 2 * hidden_cols]
    down_grad = mlp_grads[:, 2 * hidden_cols :]
    return (
        out,
        grad_tokens.reshape(seq_count, local_len, model_width),
        total_attn,
        total_mlp,
        total_heads,
        query_grad,
        key_grad,
        value_grad,
        output_grad,
        gate_grad,
        up_grad,
        down_grad,
    )


LINE_CHUNKS = 8
LINE_LAG = 2
LINE_START_TURNS = 6
MESH = pl.DeviceIdType.MESH


def line_copy(src, dst, send, recv, device):
    return pltpu.make_async_remote_copy(
        src_ref=src,
        dst_ref=dst,
        send_sem=send,
        recv_sem=recv,
        device_id=device,
        device_id_type=MESH,
    )


def line_barrier(n, place, core, fetching):
    barrier = pltpu.get_barrier_semaphore()

    def greet(device):
        pl.semaphore_signal(barrier, inc=1, device_id=device, device_id_type=MESH)

    greet({"tensor": 1 - core})
    if fetching:
        group = lax.axis_index("fsdp")
        greet({"fsdp": jnp.bitwise_xor(group, 1)})
        greet({"fsdp": jnp.bitwise_xor(group, 2)})
        for shift in range(1, n):
            greet({"context": lax.rem(place + shift, n)})
        pl.semaphore_wait(barrier, n + 2)
        return

    @pl.when(place > 0)
    def _():
        greet({"context": place - 1})

    @pl.when(place < n - 1)
    def _():
        greet({"context": place + 1})

    ends = jnp.where(place > 0, 1, 0) + jnp.where(place < n - 1, 1, 0)
    pl.semaphore_wait(barrier, ends + 1)


def fetch_steps(n, place, groups, weights, outs, sems, turns, start_turns):
    own_send, line_send, line_recv, near_send, near_recv, far_send, far_recv = sems
    group = lax.axis_index("fsdp")
    rows = weights[0].shape[0]
    neighbours = ({"fsdp": jnp.bitwise_xor(group, 1)}, {"fsdp": jnp.bitwise_xor(group, 2)})
    spans = []
    for g, members in enumerate(groups):
        start = 0
        for a in members:
            width = weights[a].shape[1] // n
            spans.append((a, g, start, width))
            start += width

    def block(out, of_group, at):
        return out.at[pl.ds(pl.multiple_of((of_group * n + at) * rows, rows), rows)]

    def held(s):
        return lax.rem(place + n - s, n)

    def columns(a, at, width):
        return weights[a].at[:, pl.ds(pl.multiple_of(at * width, 128), width)]

    def own_copy(a, g, start, width):
        return pltpu.make_async_copy(
            columns(a, place, width),
            block(outs[g], group, place).at[:, pl.ds(start, width)],
            own_send.at[a],
        )

    def line_move(a, g, start, width, s):
        to = lax.rem(place + s, n)
        return line_copy(
            columns(a, to, width),
            block(outs[g], group, place).at[:, pl.ds(start, width)],
            line_send.at[a, s - 1],
            line_recv.at[a, s - 1],
            {"context": to},
        )

    def line_arrival(a, g, start, width, s):
        return line_copy(
            columns(a, place, width),
            block(outs[g], group, held(s)).at[:, pl.ds(start, width)],
            line_send.at[a, s - 1],
            line_recv.at[a, s - 1],
            {"context": held(s)},
        )

    def near_copy(way, g, s, of_group):
        piece = block(outs[g], of_group, held(s))
        return line_copy(
            piece, piece, near_send.at[way, g, s], near_recv.at[way, g, s], neighbours[way]
        )

    def far_copy(g, s, of_group):
        way = 1 if s < n // 2 else 0
        piece = block(outs[g], of_group, held(s))
        return line_copy(piece, piece, far_send.at[g, s], far_recv.at[g, s], neighbours[way])

    def own_start():
        for span in spans:
            own_copy(*span).start()

    def line_start(span, s):
        return lambda: line_move(*span, s).start()

    def spread(g, s):
        def step():
            for span in spans:
                if span[1] == g:
                    if s == 0:
                        own_copy(*span).wait()
                    else:
                        line_arrival(*span, s).wait_recv()
            near_copy(0, g, s, group).start()
            near_copy(1, g, s, group).start()

        return step

    def pass_on(g, s):
        came = 0 if s < n // 2 else 1
        flip = 1 if came == 0 else 2

        def step():
            source = jnp.bitwise_xor(group, flip)
            near_copy(came, g, s, source).wait_recv()
            far_copy(g, s, source).start()

        return step

    def settle():
        for g in range(len(groups)):
            for s in range(n):
                came = 0 if s < n // 2 else 1
                rest = 1 - came
                flip = 1 if rest == 0 else 2
                near_copy(rest, g, s, jnp.bitwise_xor(group, flip)).wait_recv()
                far_copy(g, s, jnp.bitwise_xor(group, 3)).wait_recv()
                near_copy(0, g, s, group).wait_send()
                near_copy(1, g, s, group).wait_send()
                far_copy(g, s, group).wait_send()
        for span in spans:
            for s in range(1, n):
                line_move(*span, s).wait_send()

    issue = [(span, s) for s in range(1, n) for span in spans]
    at_turn = {(span[0], s): i * start_turns // len(issue) for i, (span, s) in enumerate(issue)}
    plan = [[] for _ in range(turns)]
    for span, s in issue:
        plan[at_turn[span[0], s]].append(line_start(span, s))
    order = [(g, s) for s in range(n) for g in range(len(groups))]
    moves = []
    for i, (g, s) in enumerate(order):
        ready = [at_turn[a, s] + 1 for a in groups[g]] if s else [0]
        moves.append((max(ready), spread(g, s)))
        if i >= 2:
            moves.append((0, pass_on(*order[i - 2])))
    moves += [(0, pass_on(*order[-2])), (0, pass_on(*order[-1]))]
    turn = 0
    for i, (ready, step) in enumerate(moves):
        turn = min(max(turn, ready, i * turns // len(moves)), turns - 1)
        plan[turn].append(step)
    return own_start, plan, settle


def piece_rows(count, body):
    @pl.loop(0, count // 16)
    def _(r):
        body(pl.ds(pl.multiple_of(r * 16, 16), 16))


def give_steps(n, place, groups, grads, outs, bufs, sems, turns):
    first_send, first_recv, second_send, second_recv, line_send, line_recv = sems
    group = lax.axis_index("fsdp")
    rows = outs[0].shape[0]

    def flips(s):
        return (1, 2) if s < n // 2 else (2, 1)

    def part(g, of_group, s):
        block = of_group * n + lax.rem(place + s, n)
        return grads[g].at[pl.ds(pl.multiple_of(block * rows, rows), rows)]

    def first_copy(g, s, k):
        one, two = flips(s)
        target = jnp.bitwise_xor(group, one if k == 0 else 3)
        return line_copy(
            part(g, target, s),
            bufs[g]["first"].at[s, k],
            first_send.at[g, s, k],
            first_recv.at[g, s, k],
            {"fsdp": jnp.bitwise_xor(group, one)},
        )

    def second_copy(g, s):
        return line_copy(
            bufs[g]["second_out"].at[s],
            bufs[g]["second"].at[s],
            second_send.at[g, s],
            second_recv.at[g, s],
            {"fsdp": jnp.bitwise_xor(group, flips(s)[1])},
        )

    def line_move(g, s):
        return line_copy(
            bufs[g]["line_out"].at[s - 1],
            bufs[g]["line"].at[s - 1],
            line_send.at[g, s - 1],
            line_recv.at[g, s - 1],
            {"context": lax.rem(place + s, n)},
        )

    def store(g, quarter, at, values):
        start = 0
        for a in groups[g]:
            width = outs[a].shape[1] // n
            cols = pl.ds(pl.multiple_of(quarter * width, 128), width)
            outs[a][at, cols] = values[:, start : start + width]
            start += width

    def begin():
        for s in order_s:
            for g in range(len(groups)):
                first_copy(g, s, 1).start()
                first_copy(g, s, 0).start()

    def across(g, s):
        def step():
            first_copy(g, s, 1).wait_recv()
            own = part(g, jnp.bitwise_xor(group, flips(s)[1]), s)
            came = bufs[g]["first"].at[s, 1]
            out = bufs[g]["second_out"].at[s]

            def add(at):
                out[at, :] = (
                    own[at, :].astype(jnp.float32) + came[at, :].astype(jnp.float32)
                ).astype(jnp.bfloat16)

            piece_rows(rows, add)
            second_copy(g, s).start()

        return step

    def total(g, s):
        def step():
            first_copy(g, s, 0).wait_recv()
            second_copy(g, s).wait_recv()
            own = part(g, group, s)
            one = bufs[g]["first"].at[s, 0]
            two = bufs[g]["second"].at[s]

            def add(at):
                value = own[at, :].astype(jnp.float32)
                value = value + one[at, :].astype(jnp.float32) + two[at, :].astype(jnp.float32)
                if s == 0:
                    store(g, place, at, value)
                else:
                    bufs[g]["line_out"][s - 1, at, :] = value.astype(jnp.bfloat16)

            piece_rows(rows, add)
            if s:
                line_move(g, s).start()

        return step

    def arrive(g, s):
        def step():
            line_move(g, s).wait_recv()
            quarter = lax.rem(place + n - s, n)

            def widen(at):
                store(g, quarter, at, bufs[g]["line"][s - 1, at, :].astype(jnp.float32))

            piece_rows(rows, widen)

        return step

    def settle():
        for g in range(len(groups)):
            for s in range(n):
                first_copy(g, s, 0).wait_send()
                first_copy(g, s, 1).wait_send()
                second_copy(g, s).wait_send()
                if s:
                    line_move(g, s).wait_send()

    order_s = list(range(1, n)) + [0]
    order = [(g, s) for s in order_s for g in range(len(groups))]
    steps = []
    for i in range(len(order) + 4):
        if i < len(order):
            steps.append(across(*order[i]))
        if 0 <= i - 1 < len(order):
            steps.append(total(*order[i - 1]))
        if 0 <= i - 4 < len(order) and order[i - 4][1]:
            steps.append(arrive(*order[i - 4]))
    plan = [[] for _ in range(turns)]
    for i, step in enumerate(steps):
        plan[1 + i * (turns - 1) // len(steps)].append(step)
    return begin, plan, settle


def line_body(n, chunks, n_part, gather, n_in, n_join, n_rest, groups, giving, extra, finish, *refs):
    refs = list(refs)
    take = lambda count: [refs.pop(0) for _ in range(count)]
    reduce = n_part > 0
    fetching = bool(groups) and not giving
    arrays = sum(len(members) for members in groups)
    parts = take(n_part)
    ins = take(n_in)
    weights = take(arrays) if fetching else []
    grads = take(len(groups)) if giving else []
    others = take(1)[0] if extra else None
    gathered = take(1)[0] if gather else None
    joined = take(n_join)
    rest = take(n_rest)
    fetched = take(len(groups)) if fetching else []
    given = take(arrays) if giving else []
    gains_out = take(1)[0] if extra else None
    if reduce:
        across, sums_in, sums_out, summed = take(4)
        cross_send, cross_recv, sum_send, sum_recv = take(4)
    if gather:
        row_send, row_recv, pair_send, pair_recv = take(4)
    if n_join:
        join_send, join_recv = take(2)
    fetch_sems = take(7) if fetching else None
    if giving:
        names = ("first", "second_out", "second", "line_out", "line")
        give_bufs = [dict(zip(names, take(5))) for _ in groups]
        give_sems = take(6)
    if extra:
        gain_own, gain_came, gain_line, gain_send, gain_recv, gain_line_send, gain_line_recv = take(7)

    place = lax.axis_index("context")
    core = lax.axis_index("tensor")
    other = {"tensor": 1 - core}
    step_rows = (ins[0].shape[0]) // chunks

    def rows(j):
        return pl.ds(j * step_rows, step_rows)

    line_barrier(n, place, core, bool(groups))
    lag = LINE_LAG if reduce else 0
    turns = chunks * max(n_part, 1) + lag + n
    plan = [[] for _ in range(turns)]
    if fetching:
        start_turns = min(LINE_START_TURNS, chunks) if reduce else 1
        own_start, plan, settle = fetch_steps(
            n, place, groups, weights, fetched, fetch_sems, turns, start_turns
        )
    if fetching:
        own_start()
    if giving:
        begin, plan, settle = give_steps(
            n, place, groups, grads, given, give_bufs, give_sems, turns
        )
        begin()

    def cross(j):
        return line_copy(
            parts[j // chunks].at[:, 1 - core, rows(j % chunks)],
            across.at[:, rows(j)],
            cross_send.at[j],
            cross_recv.at[j],
            other,
        )

    def sum_copy(way, k, j):
        return line_copy(
            sums_out.at[way, k, rows(j)],
            sums_in.at[way, k, rows(j)],
            sum_send.at[way, k, j],
            sum_recv.at[way, k, j],
            {"context": place + 1 - 2 * way},
        )

    def own_term(target, j):
        return parts[j // chunks][target, core, rows(j % chunks), :].astype(jnp.float32) + across[
            target, rows(j), :
        ].astype(jnp.float32)

    def send_sums(way, j):
        first = place == (n - 1) * way
        for k in range(n - 1):
            target = jnp.where(way == 0, n - 1 - k, k)
            passes = jnp.where(way == 0, target - place, place - target) > 0

            @pl.when(passes & first)
            def _(k=k, target=target):
                sums_out[way, k, rows(j), :] = own_term(target, j).astype(jnp.bfloat16)
                sum_copy(way, k, j).start()

            @pl.when(passes & jnp.logical_not(first))
            def _(k=k, target=target):
                sum_copy(way, k, j).wait_recv()
                sums_out[way, k, rows(j), :] = (
                    own_term(target, j) + sums_in[way, k, rows(j), :].astype(jnp.float32)
                ).astype(jnp.bfloat16)
                sum_copy(way, k, j).start()

    def row_copy(way, k, j):
        block = place - k if way == 0 else place + k
        device = {"context": place + 1 if way == 0 else place - 1}
        ref = gathered.at[block, core, rows(j)]
        return line_copy(ref, ref, row_send.at[way, k, j], row_recv.at[way, k, j], device)

    def row_arrival(way, k, j):
        block = place - 1 - k if way == 0 else place + 1 + k
        ref = gathered.at[block, core, rows(j)]
        return line_copy(
            ref, ref, row_send.at[way, k, j], row_recv.at[way, k, j], other
        )

    def pair_copy(block, half, j):
        ref = gathered.at[block, half, rows(j)]
        return line_copy(ref, ref, pair_send.at[block, j], pair_recv.at[block, j], other)

    def finish_rows(j):
        total = None
        if reduce:

            summed[...] = own_term(place, j)

            @pl.when(place > 0)
            def _():
                sum_copy(0, n - 1 - place, j).wait_recv()
                summed[...] += sums_in[0, n - 1 - place, rows(j), :].astype(jnp.float32)

            @pl.when(place < n - 1)
            def _():
                sum_copy(1, place, j).wait_recv()
                summed[...] += sums_in[1, place, rows(j), :].astype(jnp.float32)

            total = summed[...]
        made = finish(j, rows(j % chunks), total, ins, rest)
        made = made if isinstance(made, tuple) else (made,)
        made = list(made)
        if gather:
            gathered[place, core, rows(j), :] = made.pop(0)

            @pl.when(place < n - 1)
            def _():
                row_copy(0, 0, j).start()

            @pl.when(place > 0)
            def _():
                row_copy(1, 0, j).start()

            pair_copy(place, core, j).start()
        if n_join:
            i = j // chunks
            joined[i][core, rows(j % chunks), :] = made.pop(0)
            join_copy(i, core, j % chunks).start()

    def join_copy(i, half, j):
        ref = joined[i].at[half, rows(j)]
        return line_copy(ref, ref, join_send.at[i, j], join_recv.at[i, j], other)

    def pass_rows(k, j):
        for way in (0, 1):
            block = place - 1 - k if way == 0 else place + 1 + k
            here = block >= 0 if way == 0 else block <= n - 1
            onward = place < n - 1 if way == 0 else place > 0

            @pl.when(here)
            def _(way=way, block=block):
                row_arrival(way, k, j).wait_recv()

            if k + 1 <= n - 2:

                @pl.when(here & onward)
                def _(way=way):
                    row_copy(way, k + 1, j).start()

            @pl.when(here)
            def _(way=way, block=block):
                pair_copy(block, core, j).start()

    all_chunks = chunks * max(n_part, 1)
    if reduce:
        for j in range(all_chunks):
            cross(j).start()
    def gains_plan():
        group = lax.axis_index("fsdp")
        hops = (
            other,
            {"fsdp": jnp.bitwise_xor(group, 1)},
            {"fsdp": jnp.bitwise_xor(group, 2)},
        )

        def hop(h):
            return line_copy(
                gain_own.at[h], gain_came.at[h], gain_send.at[h], gain_recv.at[h], hops[h]
            )

        def line_hop(s):
            return line_copy(
                gain_line.at[place],
                gain_line.at[place],
                gain_line_send.at[s - 1],
                gain_line_recv.at[s - 1],
                {"context": lax.rem(place + s, n)},
            )

        def line_hop_in(s):
            ref = gain_line.at[lax.rem(place + n - s, n)]
            return line_copy(
                ref, ref, gain_line_send.at[s - 1], gain_line_recv.at[s - 1], other
            )

        def first():
            gain_own[0] = others[...]
            gain_own[0, 0:1, :] = rest[0][...]
            hop(0).start()

        def next_hop(h):
            def step():
                hop(h).wait_recv()
                value = gain_own[h] + gain_came[h]
                if h < 2:
                    gain_own[h + 1] = value
                    hop(h + 1).start()
                else:
                    gain_line[place] = value
                    for s in range(1, n):
                        line_hop(s).start()

            return step

        def last():
            for s in range(1, n):
                line_hop_in(s).wait_recv()
            value = gain_line[0]
            for p in range(1, n):
                value = value + gain_line[p]
            gains_out[...] = value
            for h in range(3):
                hop(h).wait_send()
            for s in range(1, n):
                line_hop(s).wait_send()

        return [first, next_hop(0), next_hop(1), next_hop(2), last]

    near = jnp.where(place < n // 2, 0, 1)
    gain_steps = gains_plan() if extra else []
    for i in range(turns):
        for step in plan[i]:
            step()
        if reduce and i < all_chunks:
            cross(i).wait_recv()
            send_sums(near, i)
        if reduce and 0 <= i - 1 < all_chunks:
            send_sums(1 - near, i - 1)
        if 0 <= i - lag < all_chunks:
            finish_rows(i - lag)
        if extra and i - lag >= chunks and gain_steps:
            gain_steps.pop(0)()
        if gather:
            for k in range(n - 1):
                if 0 <= i - lag - 1 - k < chunks:
                    pass_rows(k, i - lag - 1 - k)

    for step in gain_steps:
        step()
    if groups:
        settle()
    for j in range(all_chunks):
        if reduce:
            cross(j).wait_send()
            for k in range(n - 1):

                @pl.when(place < n - 1 - k)
                def _(k=k, j=j):
                    sum_copy(0, k, j).wait_send()

                @pl.when(place > k)
                def _(k=k, j=j):
                    sum_copy(1, k, j).wait_send()

        if gather:
            for block in range(n):
                pair_copy(block, 1 - core, j).wait_recv()
                pair_copy(block, core, j).wait_send()
            for k in range(n - 1):

                @pl.when((place < n - 1) & (place >= k))
                def _(k=k, j=j):
                    row_copy(0, k, j).wait_send()

                @pl.when((place > 0) & (place + k <= n - 1))
                def _(k=k, j=j):
                    row_copy(1, k, j).wait_send()

        if n_join:
            join_copy(j // chunks, 1 - core, j % chunks).wait_recv()
            join_copy(j // chunks, core, j % chunks).wait_send()


def line_call(
    n,
    collective,
    finish,
    part,
    ins,
    gather=False,
    joins=(),
    rests=(),
    chunks=LINE_CHUNKS,
    groups=(),
    weights=(),
    grads=(),
    extra=None,
):
    parts = () if part is None else part if isinstance(part, tuple) else (part,)
    reduce = len(parts) > 0
    giving = len(grads) > 0
    row_count, model_width = ins[0].shape
    vmem = pl.BlockSpec(memory_space=pltpu.VMEM)
    outs = []
    if gather:
        outs.append(jax.ShapeDtypeStruct((n, 2, row_count, model_width), jnp.bfloat16))
    outs += [jax.ShapeDtypeStruct((2, row_count, model_width), kind) for kind in joins]
    outs += list(rests)
    out_specs = [vmem] * len(outs)
    for members in groups if not giving else ():
        rows = weights[0].shape[0] * n * lax.axis_size("fsdp")
        width = sum(weights[a].shape[1] for a in members) // n
        outs.append(jax.ShapeDtypeStruct((rows, width), jnp.bfloat16))
        out_specs.append(pl.BlockSpec(memory_space=pl.ANY))
    dma = pltpu.SemaphoreType.DMA
    if giving:
        owned = grads[0].shape[0] // (n * lax.axis_size("fsdp"))
        for width in weights:
            outs.append(jax.ShapeDtypeStruct((owned, width * n), jnp.float32))
            out_specs.append(vmem)
    if extra is not None:
        outs.append(jax.ShapeDtypeStruct(extra.shape, jnp.float32))
        out_specs.append(vmem)
    total_chunks = chunks * max(len(parts), 1)
    sum_rows = row_count * max(len(parts), 1)
    scratch = []
    if reduce:
        slot = pltpu.VMEM((2, n - 1, sum_rows, model_width), jnp.bfloat16)
        scratch += [pltpu.VMEM((n, sum_rows, model_width), jnp.bfloat16), slot, slot]
        scratch += [pltpu.VMEM((row_count // chunks, model_width), jnp.float32)]
        tally = (2, n - 1, total_chunks)
        scratch += [dma((total_chunks,)), dma((total_chunks,)), dma(tally), dma(tally)]
    if gather:
        scratch += [dma((2, n - 1, chunks)), dma((2, n - 1, chunks)), dma((n, chunks)), dma((n, chunks))]
    if joins:
        scratch += [dma((len(joins), chunks)), dma((len(joins), chunks))]
    if groups and not giving:
        arrays = len(weights)
        pieces = (2, len(groups), n)
        scratch += [dma((arrays,)), dma((arrays, n - 1)), dma((arrays, n - 1))]
        scratch += [dma(pieces), dma(pieces), dma(pieces[1:]), dma(pieces[1:])]
    if giving:
        for grad in grads:
            piece = (owned, grad.shape[1])
            for lead in ((n, 2), (n,), (n,), (n - 1,), (n - 1,)):
                scratch.append(pltpu.VMEM(lead + piece, jnp.bfloat16))
        count = len(groups)
        scratch += [dma((count, n, 2)), dma((count, n, 2)), dma((count, n)), dma((count, n))]
        scratch += [dma((count, n - 1)), dma((count, n - 1))]
    if extra is not None:
        stack = pltpu.VMEM((3,) + extra.shape, jnp.float32)
        scratch += [stack, stack, pltpu.VMEM((n,) + extra.shape, jnp.float32)]
        scratch += [dma((3,)), dma((3,)), dma((n - 1,)), dma((n - 1,))]
    operands = list(parts) + list(ins) + (list(grads) if giving else list(weights))
    operands += [] if extra is None else [extra]
    moved = row_count * model_width * 2 * n * (2 * reduce + 2 * gather)
    return pl.pallas_call(
        functools.partial(
            line_body,
            n,
            chunks,
            len(parts),
            gather,
            len(ins),
            len(joins),
            len(rests),
            groups,
            giving,
            extra is not None,
            finish,
        ),
        out_shape=tuple(outs),
        in_specs=[vmem] * len(operands),
        out_specs=tuple(out_specs),
        scratch_shapes=scratch,
        compiler_params=pltpu.CompilerParams(
            collective_id=collective, has_side_effects=True, vmem_limit_bytes=56 << 20
        ),
        cost_estimate=pl.CostEstimate(
            flops=moved, bytes_accessed=20 * moved, transcendentals=0
        ),
        name="line_%d" % collective,
    )(*operands)


def finish_gather(j, rows, total, ins, rest):
    values = ins[0][rows, :].astype(jnp.float32)
    return (values * rms_scale(values) * ins[1][...]).astype(jnp.bfloat16)


def finish_attention(j, rows, total, ins, rest):
    residual = ins[0][rows, :].astype(jnp.float32) + total
    rest[0][rows, :] = residual
    return (residual * rms_scale(residual) * ins[1][...]).astype(jnp.bfloat16)


def gain_rows(j, rest, terms):
    sums = jnp.sum(terms, axis=0, keepdims=True)
    rest[...] = sums if j == 0 else rest[...] + sums


def finish_mlp_back(j, rows, total, ins, rest):
    residual = ins[0][rows, :]
    scale = rms_scale(residual)
    hat = residual * scale
    grad = ins[1][rows, :].astype(jnp.float32) + norm_back(total, hat, scale, ins[2][...])
    rest[0][rows, :] = grad
    gain_rows(j, rest[1], total * hat)
    return grad.astype(jnp.bfloat16)


def finish_ends(j, rows, total, ins, rest):
    if j >= LINE_CHUNKS:
        return (ins[3][rows, :] + total).astype(jnp.bfloat16)
    values = ins[1][rows, :].astype(jnp.float32)
    scale = rms_scale(values)
    hat = values * scale
    gain_rows(j, rest[0], total * hat)
    return ins[0][rows, :] + norm_back(total, hat, scale, ins[2][...])


def permuted_tokens(rows):
    n = lax.axis_size("context")
    place = lax.axis_index("context")
    core = lax.axis_index("tensor")
    shape = rows.shape
    near = jnp.zeros((n,) + shape, rows.dtype)
    for s in range(n):
        ring = [(i, (i + s) % n) for i in range(n)]
        came = lax.ppermute(rows, "context", ring) if s else rows
        near = lax.dynamic_update_slice(near, came[None], (lax.rem(place + n - s, n), 0, 0))
    far = lax.ppermute(near, "tensor", [(0, 1), (1, 0)])
    both = jnp.zeros((n, 2) + shape, rows.dtype)
    both = lax.dynamic_update_slice(both, near[:, None], (0, core, 0, 0))
    both = lax.dynamic_update_slice(both, far[:, None], (0, 1 - core, 0, 0))
    return both.reshape(n * 2 * shape[0], shape[1])


def token_half(block, index, parts):
    rows = block.shape[0] // parts
    return lax.dynamic_slice_in_dim(block, index * rows, rows, axis=0)


def line_shards(
    tokens,
    cotangent,
    norm_gain_attn,
    norm_gain_mlp,
    head_gains,
    query_weight,
    key_matrix,
    value_matrix,
    output_weight,
    gate_weight,
    up_weight,
    down_weight,
):
    seq_count, local_len, model_width = tokens.shape
    parts = lax.axis_size("context")
    cores = lax.axis_size("tensor")
    core = lax.axis_index("tensor")
    full_len = local_len * parts
    q_cols = query_weight.shape[1] // parts
    kv_cols = key_matrix.shape[1] // parts
    h_cols = gate_weight.shape[1] // parts
    q_heads = q_cols // HEAD_DIM
    kv_heads = kv_cols // HEAD_DIM
    head_group = q_heads // kv_heads
    score_scale = 1.0 / math.sqrt(HEAD_DIM)
    positions = jnp.arange(full_len, dtype=jnp.int32)
    cosine_table, sine_table = rope_tables(positions, HEAD_DIM)
    cosine_table = cosine_table[:, None, :]
    sine_table = sine_table[:, None, :]
    visible = positions[None, :] <= positions[:, None]
    gain_attn = norm_gain_attn.astype(jnp.float32)[None]
    gain_mlp = norm_gain_mlp.astype(jnp.float32)[None]
    gain_heads = head_gains.astype(jnp.float32)

    def line_parts(left, right):
        product = column_product(left, right).astype(jnp.bfloat16)
        return product.reshape(parts, cores, half_len, model_width)

    own_cot = token_half(cotangent.reshape(local_len, model_width), core, cores)
    inputs = token_half(tokens.reshape(local_len, model_width), core, cores)
    half_len = local_len // cores
    rows_f32 = jax.ShapeDtypeStruct((half_len, model_width), jnp.float32)
    sums_f32 = jax.ShapeDtypeStruct((1, model_width), jnp.float32)
    normed_attn, in_weights, out_weights = line_call(
        parts,
        1,
        finish_gather,
        None,
        (inputs, gain_attn),
        gather=True,
        groups=((0, 1, 2), (3,)),
        weights=(query_weight, key_matrix, value_matrix, output_weight),
    )
    normed_attn = normed_attn.reshape(full_len, model_width)
    grad_out = permuted_tokens(own_cot)

    raw = jnp.dot(normed_attn, in_weights, preferred_element_type=jnp.float32)
    query_split = raw[:, :q_cols].reshape(full_len, q_heads, HEAD_DIM)
    query_scale = rms_scale(query_split)
    query_hat = query_split * query_scale
    queries = rotate(query_hat * gain_heads[0], cosine_table, sine_table).astype(jnp.bfloat16)
    key_split = raw[:, q_cols : q_cols + kv_cols].reshape(full_len, kv_heads, HEAD_DIM)
    key_scale = rms_scale(key_split)
    key_hat = key_split * key_scale
    keys = rotate(key_hat * gain_heads[1], cosine_table, sine_table).astype(jnp.bfloat16)
    values = raw[:, q_cols + kv_cols :].astype(jnp.bfloat16).reshape(full_len, kv_heads, HEAD_DIM)
    queries = queries.reshape(full_len, kv_heads, head_group, HEAD_DIM)

    scores = (
        jnp.einsum("ikgd,jkd->kgij", queries, keys, preferred_element_type=jnp.float32)
        * score_scale
    )
    weights = jnp.where(visible, jnp.exp(scores), 0.0)
    probs = weights / jnp.sum(weights, axis=-1, keepdims=True)
    probs_low = probs.astype(jnp.bfloat16)
    attended = (
        jnp.einsum("kgij,jkd->ikgd", probs_low, values, preferred_element_type=jnp.float32)
        .astype(jnp.bfloat16)
        .reshape(full_len, q_cols)
    )
    normed_mlp, residual, mlp_in, mlp_down = line_call(
        parts,
        2,
        finish_attention,
        line_parts(attended, out_weights),
        (inputs, gain_mlp),
        gather=True,
        rests=(rows_f32,),
        groups=((0, 1), (2,)),
        weights=(gate_weight, up_weight, down_weight),
    )
    normed_mlp = normed_mlp.reshape(full_len, model_width)

    both = jnp.dot(normed_mlp, mlp_in, preferred_element_type=jnp.float32)
    gate_act = both[:, :h_cols]
    upward = both[:, h_cols:]
    sig_gate = jax.nn.sigmoid(gate_act)
    activated = gate_act * sig_gate
    hidden = (activated * upward).astype(jnp.bfloat16)
    grad_hidden = jnp.dot(grad_out, mlp_down, preferred_element_type=jnp.float32)
    derivative = sig_gate * (1.0 + gate_act * (1.0 - sig_gate))
    grad_gate = (grad_hidden * upward * derivative).astype(jnp.bfloat16)
    grad_up = (grad_hidden * activated).astype(jnp.bfloat16)
    grad_both = jnp.concatenate([grad_gate, grad_up], axis=1)
    grad_in = row_product(normed_mlp, grad_both).astype(jnp.bfloat16)
    grad_down = row_product(grad_out, hidden).astype(jnp.bfloat16)
    grad_branch, grad_residual, gain_mlp_part, gate_grad, up_grad, down_grad = line_call(
        parts,
        3,
        finish_mlp_back,
        line_parts(grad_both, mlp_in),
        (residual, own_cot, gain_mlp),
        gather=True,
        rests=(rows_f32, sums_f32),
        groups=((0, 1), (2,)),
        weights=(h_cols, h_cols, h_cols),
        grads=(grad_in, grad_down),
    )
    grad_branch = grad_branch.reshape(full_len, model_width)
    grad_attended = (
        jnp.dot(grad_branch, out_weights, preferred_element_type=jnp.float32)
        .astype(jnp.bfloat16)
        .reshape(full_len, kv_heads, head_group, HEAD_DIM)
    )
    grad_probs = jnp.einsum(
        "ikgd,jkd->kgij", grad_attended, values, preferred_element_type=jnp.float32
    )
    delta = jnp.sum(probs * grad_probs, axis=-1, keepdims=True)
    grad_scores = (probs * (grad_probs - delta)).astype(jnp.bfloat16)
    grad_queries = (
        jnp.einsum("kgij,jkd->ikgd", grad_scores, keys, preferred_element_type=jnp.float32)
        * score_scale
    ).reshape(full_len, q_heads, HEAD_DIM)
    grad_keys = (
        jnp.einsum("kgij,ikgd->jkd", grad_scores, queries, preferred_element_type=jnp.float32)
        * score_scale
    )
    grad_values = jnp.einsum(
        "kgij,ikgd->jkd", probs_low, grad_attended, preferred_element_type=jnp.float32
    )
    grad_query_hat = unrotate(grad_queries, cosine_table, sine_table)
    grad_key_hat = unrotate(grad_keys, cosine_table, sine_table)
    heads_part = jnp.stack(
        [
            jnp.sum(grad_query_hat * query_hat, axis=(0, 1)),
            jnp.sum(grad_key_hat * key_hat, axis=(0, 1)),
        ]
    )
    grad_raw = jnp.concatenate(
        [
            norm_back(grad_query_hat, query_hat, query_scale, gain_heads[0]).reshape(
                full_len, q_cols
            ),
            norm_back(grad_key_hat, key_hat, key_scale, gain_heads[1]).reshape(full_len, kv_cols),
            grad_values.reshape(full_len, kv_cols),
        ],
        axis=1,
    ).astype(jnp.bfloat16)
    attn_in_grad = row_product(normed_attn, grad_raw).astype(jnp.bfloat16)
    attn_out_grad = row_product(grad_branch, attended).astype(jnp.bfloat16)
    gains = jnp.concatenate(
        [
            jnp.zeros((1, model_width), jnp.float32),
            gain_mlp_part,
            jnp.pad(heads_part.reshape(1, -1), ((0, 0), (0, model_width - heads_part.size))),
            jnp.zeros((5, model_width), jnp.float32),
        ],
        axis=0,
    )
    grad_tokens, out, _, query_grad, key_grad, value_grad, output_grad, totals = line_call(
        parts,
        4,
        finish_ends,
        (line_parts(grad_raw, in_weights), line_parts(hidden, mlp_down)),
        (grad_residual, inputs, gain_attn, residual),
        joins=(jnp.float32, jnp.bfloat16),
        rests=(sums_f32,),
        groups=((0, 1, 2), (3,)),
        weights=(q_cols, kv_cols, kv_cols, q_cols),
        grads=(attn_in_grad, attn_out_grad),
        extra=gains,
    )
    return (
        out.reshape(tokens.shape),
        grad_tokens.reshape(tokens.shape),
        totals[0],
        totals[1],
        totals[2, : heads_part.size].reshape(heads_part.shape),
        query_grad,
        key_grad,
        value_grad,
        output_grad,
        gate_grad,
        up_grad,
        down_grad,
    )


def layer(*operands):
    tokens, key_matrix, gate_weight = operands[0], operands[6], operands[9]
    parts = lax.axis_size("context")
    cores = lax.axis_size("tensor")
    fits = (
        tokens.shape[0] == 1
        and key_matrix.shape[1] % (parts * HEAD_DIM) == 0
        and gate_weight.shape[1] % (parts * HEAD_DIM) == 0
        and tokens.shape[1] % (cores * LINE_CHUNKS * 16) == 0
        and cores == 2
        and lax.axis_size("fsdp") == 4
    )
    return line_shards(*operands) if fits else shards(*operands)


def solution(mesh):
    return jax.shard_map(
        layer,
        mesh=mesh,
        in_specs=(
            P("fsdp", "context", None),
            P("fsdp", "context", None),
            P(),
            P(),
            P(),
            P(("fsdp", "context"), "tensor"),
            P(("fsdp", "context"), "tensor"),
            P(("fsdp", "context"), "tensor"),
            P(("fsdp", "context"), "tensor"),
            P(("fsdp", "context"), "tensor"),
            P(("fsdp", "context"), "tensor"),
            P(("fsdp", "context"), "tensor"),
        ),
        out_specs=(
            P("fsdp", "context", None),
            P("fsdp", "context", None),
            P(),
            P(),
            P(),
            P(("fsdp", "context"), "tensor"),
            P(("fsdp", "context"), "tensor"),
            P(("fsdp", "context"), "tensor"),
            P(("fsdp", "context"), "tensor"),
            P(("fsdp", "context"), "tensor"),
            P(("fsdp", "context"), "tensor"),
            P(("fsdp", "context"), "tensor"),
        ),
        check_vma=False,
    )
```

```python
import functools
import math

import jax
import jax.numpy as jnp
from jax import lax
from jax.experimental import pallas as pl
from jax.experimental.pallas import tpu as pltpu
from jax.sharding import PartitionSpec as P


HEAD_DIM = 128


EPS = 1e-06
THETA = 1000000.0


def rms_scale(values):
    return lax.rsqrt(jnp.mean(values * values, axis=-1, keepdims=True) + EPS)


def rope_tables(positions, head_size):
    halves = head_size // 2
    inverse = THETA ** (-(jnp.arange(halves, dtype=jnp.float32) * 2.0) / head_size)
    angle = positions[:, None].astype(jnp.float32) * inverse[None, :]
    return (jnp.cos(angle), jnp.sin(angle))


def rotate(values, cosine_table, sine_table):
    halves = values.shape[-1] // 2
    leading = values[..., :halves]
    trailing = values[..., halves:]
    return jnp.concatenate(
        [
            leading * cosine_table - trailing * sine_table,
            trailing * cosine_table + leading * sine_table,
        ],
        axis=-1,
    )


def unrotate(values, cosine_table, sine_table):
    halves = values.shape[-1] // 2
    leading = values[..., :halves]
    trailing = values[..., halves:]
    return jnp.concatenate(
        [
            leading * cosine_table + trailing * sine_table,
            trailing * cosine_table - leading * sine_table,
        ],
        axis=-1,
    )


def norm_back(grad_normed, normed_hat, scale_factor, gain):
    scaled = grad_normed * gain
    return scale_factor * (
        scaled - normed_hat * jnp.mean(normed_hat * scaled, axis=-1, keepdims=True)
    )


def row_product(left, right):
    return lax.dot_general(
        left, right, (((0,), (0,)), ((), ())), preferred_element_type=jnp.float32
    )


def column_product(left, right):
    return lax.dot_general(
        left, right, (((1,), (1,)), ((), ())), preferred_element_type=jnp.float32
    )


def blank(row_total, col_total):
    return jnp.zeros((row_total, col_total), jnp.float32)


def placing(left):

    def place_rows(total, piece, start):
        return column_product(left, piece)

    return place_rows


def adding(left):

    def add_rows(total, piece, start):
        return jnp.dot(left, piece, preferred_element_type=jnp.float32)

    return add_rows


def tensor_total(partial_sum):
    return lax.psum(partial_sum, "tensor")


def owner_rows(term_fn, row_total):
    return lax.psum_scatter(
        term_fn(jnp.int32(0), lax.axis_size(("fsdp", "context")) * row_total),
        ("fsdp", "context"),
        scatter_dimension=0,
        tiled=True,
    )


def shards(
    tokens,
    cotangent,
    norm_gain_attn,
    norm_gain_mlp,
    head_gains,
    query_weight,
    key_matrix,
    value_matrix,
    output_weight,
    gate_weight,
    up_weight,
    down_weight,
):
    seq_count, local_len, model_width = tokens.shape
    row_count = seq_count * local_len
    owned_rows = query_weight.shape[0]
    query_cols = query_weight.shape[1]
    kv_cols = key_matrix.shape[1]
    hidden_cols = gate_weight.shape[1]
    query_heads = query_cols // HEAD_DIM
    kv_heads = kv_cols // HEAD_DIM
    head_group = query_heads // kv_heads
    score_scale = 1.0 / math.sqrt(HEAD_DIM)
    full_len = local_len * lax.axis_size("context")
    query_pos = lax.axis_index("context") * local_len + jnp.arange(local_len, dtype=jnp.int32)
    key_pos = jnp.arange(full_len, dtype=jnp.int32)
    cosine_table, sine_table = rope_tables(query_pos, HEAD_DIM)
    cosine_table = cosine_table[:, None, :]
    sine_table = sine_table[:, None, :]
    visible = key_pos[None, :] <= query_pos[:, None]
    inputs = tokens.reshape(row_count, model_width).astype(jnp.float32)
    grad_out = cotangent.reshape(row_count, model_width)
    gain_attn = norm_gain_attn.astype(jnp.float32)
    gain_mlp = norm_gain_mlp.astype(jnp.float32)
    gain_heads = head_gains.astype(jnp.float32)

    def attn_rows(fold_fn, initial):
        return fold_fn(
            initial,
            (
                lax.all_gather(query_weight, ("fsdp", "context"), axis=0, tiled=True),
                lax.all_gather(key_matrix, ("fsdp", "context"), axis=0, tiled=True),
                lax.all_gather(value_matrix, ("fsdp", "context"), axis=0, tiled=True),
            ),
            jnp.int32(0),
        )

    def attn_out_rows(fold_fn, initial):
        return fold_fn(
            initial,
            lax.all_gather(output_weight, ("fsdp", "context"), axis=0, tiled=True),
            jnp.int32(0),
        )

    def mlp_rows(fold_fn, initial):
        return fold_fn(
            initial,
            (
                lax.all_gather(gate_weight, ("fsdp", "context"), axis=0, tiled=True),
                lax.all_gather(up_weight, ("fsdp", "context"), axis=0, tiled=True),
            ),
            jnp.int32(0),
        )

    def down_rows(fold_fn, initial):
        return fold_fn(
            initial,
            lax.all_gather(down_weight, ("fsdp", "context"), axis=0, tiled=True),
            jnp.int32(0),
        )

    scale_attn = rms_scale(inputs)
    hat_attn = inputs * scale_attn
    normed_attn = (hat_attn * gain_attn).astype(jnp.bfloat16)

    def project_in(totals, pieces, start):
        return (
            jnp.dot(normed_attn, pieces[0], preferred_element_type=jnp.float32),
            jnp.dot(normed_attn, pieces[1], preferred_element_type=jnp.float32),
            jnp.dot(normed_attn, pieces[2], preferred_element_type=jnp.float32),
        )

    query_raw, key_unrotated, value_raw = attn_rows(
        project_in,
        (blank(row_count, query_cols), blank(row_count, kv_cols), blank(row_count, kv_cols)),
    )
    query_split = query_raw.reshape(seq_count, local_len, query_heads, HEAD_DIM)
    query_scale = rms_scale(query_split)
    query_hat = query_split * query_scale
    query_rows = rotate(query_hat * gain_heads[0], cosine_table, sine_table).astype(jnp.bfloat16)
    key_split = key_unrotated.reshape(seq_count, local_len, kv_heads, HEAD_DIM)
    key_scale = rms_scale(key_split)
    key_hat = key_split * key_scale
    keys_local = rotate(key_hat * gain_heads[1], cosine_table, sine_table).astype(jnp.bfloat16)
    values_local = value_raw.astype(jnp.bfloat16)
    keys_all, value_rows_gathered = (
        lax.all_gather(
            keys_local.reshape(seq_count, local_len, kv_cols), "context", axis=1, tiled=True
        ),
        lax.all_gather(
            values_local.reshape(seq_count, local_len, kv_cols), "context", axis=1, tiled=True
        ),
    )
    query_blocks = query_rows.reshape(
        seq_count, local_len, kv_heads, head_group, HEAD_DIM
    ).transpose(2, 0, 1, 3, 4)
    key_blocks = keys_all.reshape(seq_count, full_len, kv_heads, HEAD_DIM).transpose(2, 0, 1, 3)
    value_blocks = value_rows_gathered.reshape(seq_count, full_len, kv_heads, HEAD_DIM).transpose(
        2, 0, 1, 3
    )

    def attend(operands):
        query_block, key_block, value_block = operands
        scores = (
            jnp.einsum("bigd,bjd->bgij", query_block, key_block, preferred_element_type=jnp.float32)
            * score_scale
        )
        weights = jnp.where(visible, jnp.exp(scores), 0.0)
        totals = jnp.sum(weights, axis=-1)
        probs_low = (weights / totals[..., None]).astype(jnp.bfloat16)
        mixed_heads = jnp.einsum(
            "bgij,bjd->bigd", probs_low, value_block, preferred_element_type=jnp.float32
        )
        return (mixed_heads.astype(jnp.bfloat16), jnp.log(totals))

    mixed_all, log_totals = lax.map(attend, (query_blocks, key_blocks, value_blocks))
    attended = mixed_all.transpose(1, 2, 0, 3, 4).reshape(row_count, query_cols)
    attn_part = attn_out_rows(placing(attended), blank(row_count, model_width))
    residual = inputs + tensor_total(attn_part)
    scale_mlp = rms_scale(residual)
    hat_mlp = residual * scale_mlp
    normed_mlp = (hat_mlp * gain_mlp).astype(jnp.bfloat16)

    def project_mlp(totals, pieces, start):
        return (
            jnp.dot(normed_mlp, pieces[0], preferred_element_type=jnp.float32),
            jnp.dot(normed_mlp, pieces[1], preferred_element_type=jnp.float32),
        )

    gate_act, upward = mlp_rows(
        project_mlp, (blank(row_count, hidden_cols), blank(row_count, hidden_cols))
    )
    sig_gate = jax.nn.sigmoid(gate_act)
    activated = gate_act * sig_gate
    hidden = (activated * upward).astype(jnp.bfloat16)
    mlp_part = down_rows(placing(hidden), blank(row_count, model_width))
    result = residual + tensor_total(mlp_part)
    out = result.astype(jnp.bfloat16).reshape(seq_count, local_len, model_width)
    grad_hidden = down_rows(adding(grad_out), blank(row_count, hidden_cols))
    derivative = sig_gate * (1.0 + gate_act * (1.0 - sig_gate))
    grad_gate = (grad_hidden * upward * derivative).astype(jnp.bfloat16)
    grad_up = (grad_hidden * activated).astype(jnp.bfloat16)

    def gate_back(total, pieces, start):
        part_sum = column_product(grad_gate, pieces[0]) + column_product(grad_up, pieces[1])
        return part_sum

    grad_normed_mlp = tensor_total(mlp_rows(gate_back, blank(row_count, model_width)))

    def mlp_terms(start, span_rows):
        return jnp.concatenate(
            [
                row_product(normed_mlp, grad_gate),
                row_product(normed_mlp, grad_up),
                row_product(grad_out, hidden),
            ],
            axis=1,
        )

    mlp_grads = owner_rows(mlp_terms, owned_rows)
    grad_gain_mlp = jnp.sum(grad_normed_mlp * hat_mlp, axis=0)
    grad_residual = grad_out.astype(jnp.float32) + norm_back(
        grad_normed_mlp, hat_mlp, scale_mlp, gain_mlp
    )
    grad_branch = grad_residual.astype(jnp.bfloat16)
    grad_attended = attn_out_rows(adding(grad_branch), blank(row_count, query_cols))
    grad_attended_low = grad_attended.astype(jnp.bfloat16)
    grad_blocks = grad_attended_low.reshape(
        seq_count, local_len, kv_heads, head_group, HEAD_DIM
    ).transpose(2, 0, 1, 3, 4)

    def attend_back(operands):
        query_block, key_block, value_block, grad_block, log_total = operands
        scores = (
            jnp.einsum("bigd,bjd->bgij", query_block, key_block, preferred_element_type=jnp.float32)
            * score_scale
        )
        probs = jnp.where(visible, jnp.exp(scores - log_total[..., None]), 0.0)
        probs_low = probs.astype(jnp.bfloat16)
        grad_probs = jnp.einsum(
            "bigd,bjd->bgij", grad_block, value_block, preferred_element_type=jnp.float32
        )
        delta = jnp.sum(probs * grad_probs, axis=-1, keepdims=True)
        grad_scores = (probs * (grad_probs - delta)).astype(jnp.bfloat16)
        grad_query = (
            jnp.einsum("bgij,bjd->bigd", grad_scores, key_block, preferred_element_type=jnp.float32)
            * score_scale
        )
        grad_key = (
            jnp.einsum(
                "bgij,bigd->bjd", grad_scores, query_block, preferred_element_type=jnp.float32
            )
            * score_scale
        )
        grad_value = jnp.einsum(
            "bgij,bigd->bjd", probs_low, grad_block, preferred_element_type=jnp.float32
        )
        return (grad_query, grad_key, grad_value, delta[..., 0])

    grad_query_all, grad_key_all, grad_value_all, _ = lax.map(
        attend_back, (query_blocks, key_blocks, value_blocks, grad_blocks, log_totals)
    )
    grad_key_full = grad_key_all.transpose(1, 2, 0, 3).reshape(seq_count, full_len, kv_cols)
    grad_value_full = grad_value_all.transpose(1, 2, 0, 3).reshape(seq_count, full_len, kv_cols)
    grad_key_own, grad_value_own = (
        lax.psum_scatter(
            grad_key_full.astype(jnp.bfloat16), "context", scatter_dimension=1, tiled=True
        ).astype(jnp.float32),
        lax.psum_scatter(
            grad_value_full.astype(jnp.bfloat16), "context", scatter_dimension=1, tiled=True
        ).astype(jnp.float32),
    )
    grad_query_rot = grad_query_all.transpose(1, 2, 0, 3, 4).reshape(
        seq_count, local_len, query_heads, HEAD_DIM
    )
    grad_query_hat = unrotate(grad_query_rot, cosine_table, sine_table)
    grad_key_hat = unrotate(
        grad_key_own.reshape(seq_count, local_len, kv_heads, HEAD_DIM), cosine_table, sine_table
    )
    grad_gain_query = jnp.sum(grad_query_hat * query_hat, axis=(0, 1, 2))
    grad_gain_key = jnp.sum(grad_key_hat * key_hat, axis=(0, 1, 2))
    grad_query_raw = (
        norm_back(grad_query_hat, query_hat, query_scale, gain_heads[0])
        .reshape(row_count, query_cols)
        .astype(jnp.bfloat16)
    )
    grad_key_raw = (
        norm_back(grad_key_hat, key_hat, key_scale, gain_heads[1])
        .reshape(row_count, kv_cols)
        .astype(jnp.bfloat16)
    )
    grad_value_low = grad_value_own.reshape(row_count, kv_cols).astype(jnp.bfloat16)

    def attn_back(total, pieces, start):
        part_sum = (
            column_product(grad_query_raw, pieces[0])
            + column_product(grad_key_raw, pieces[1])
            + column_product(grad_value_low, pieces[2])
        )
        return part_sum

    grad_normed_part = attn_rows(attn_back, blank(row_count, model_width))
    grad_normed_attn, grad_heads_gain = (
        lax.psum(grad_normed_part.astype(jnp.bfloat16), "tensor").astype(jnp.float32),
        lax.psum(jnp.stack([grad_gain_query, grad_gain_key]).astype(jnp.bfloat16), "tensor").astype(
            jnp.float32
        ),
    )

    def attn_terms(start, span_rows):
        return jnp.concatenate(
            [
                row_product(normed_attn, grad_query_raw),
                row_product(normed_attn, grad_key_raw),
                row_product(normed_attn, grad_value_low),
                row_product(grad_branch, attended),
            ],
            axis=1,
        )

    attn_grads = owner_rows(attn_terms, owned_rows)
    grad_gain_attn = jnp.sum(grad_normed_attn * hat_attn, axis=0)
    grad_tokens = grad_residual + norm_back(grad_normed_attn, hat_attn, scale_attn, gain_attn)
    total_attn, total_mlp, total_heads = lax.psum(
        (grad_gain_attn, grad_gain_mlp, grad_heads_gain), ("fsdp", "context")
    )
    query_grad = attn_grads[:, :query_cols]
    key_grad = attn_grads[:, query_cols : query_cols + kv_cols]
    value_grad = attn_grads[:, query_cols + kv_cols : query_cols + 2 * kv_cols]
    output_grad = attn_grads[:, query_cols + 2 * kv_cols :]
    gate_grad = mlp_grads[:, :hidden_cols]
    up_grad = mlp_grads[:, hidden_cols : 2 * hidden_cols]
    down_grad = mlp_grads[:, 2 * hidden_cols :]
    return (
        out,
        grad_tokens.reshape(seq_count, local_len, model_width),
        total_attn,
        total_mlp,
        total_heads,
        query_grad,
        key_grad,
        value_grad,
        output_grad,
        gate_grad,
        up_grad,
        down_grad,
    )


LINE_CHUNKS = 8
LINE_LAG = 2
LINE_START_TURNS = 1
LINE_FROM_TURN = 1
LINE_GIVE_TURN = 6
MESH = pl.DeviceIdType.MESH


def line_copy(src, dst, send, recv, device):
    return pltpu.make_async_remote_copy(
        src_ref=src,
        dst_ref=dst,
        send_sem=send,
        recv_sem=recv,
        device_id=device,
        device_id_type=MESH,
    )


def line_barrier(n, place, core, fetching):
    barrier = pltpu.get_barrier_semaphore()

    def greet(device):
        pl.semaphore_signal(barrier, inc=1, device_id=device, device_id_type=MESH)

    greet({"tensor": 1 - core})
    if fetching:
        group = lax.axis_index("fsdp")
        greet({"fsdp": jnp.bitwise_xor(group, 1)})
        greet({"fsdp": jnp.bitwise_xor(group, 2)})
        for shift in range(1, n):
            greet({"context": lax.rem(place + shift, n)})
        pl.semaphore_wait(barrier, n + 2)
        return

    @pl.when(place > 0)
    def _():
        greet({"context": place - 1})

    @pl.when(place < n - 1)
    def _():
        greet({"context": place + 1})

    ends = jnp.where(place > 0, 1, 0) + jnp.where(place < n - 1, 1, 0)
    pl.semaphore_wait(barrier, ends + 1)


def nearest(n):
    return [sorted(range(n), key=lambda q: (abs(q - p), q)) for p in range(n)]


def ranked(n, place):
    table = nearest(n)
    return [sum(jnp.where(place == p, table[p][k], 0) for p in range(n)) for k in range(n)]


def fetch_steps(n, place, groups, weights, outs, sems, turns, start_turns, from_turn):
    own_send, line_send, line_recv, near_send, near_recv, far_send, far_recv = sems
    group = lax.axis_index("fsdp")
    rows = weights[0].shape[0]
    neighbours = ({"fsdp": jnp.bitwise_xor(group, 1)}, {"fsdp": jnp.bitwise_xor(group, 2)})
    spans = []
    for g, members in enumerate(groups):
        start = 0
        for a in members:
            width = weights[a].shape[1] // n
            spans.append((a, g, start, width))
            start += width

    def block(out, of_group, at):
        return out.at[pl.ds(pl.multiple_of((of_group * n + at) * rows, rows), rows)]

    order = ranked(n, place)

    def columns(a, at, width):
        return weights[a].at[:, pl.ds(pl.multiple_of(at * width, 128), width)]

    def own_copy(a, g, start, width):
        return pltpu.make_async_copy(
            columns(a, place, width),
            block(outs[g], group, place).at[:, pl.ds(start, width)],
            own_send.at[a],
        )

    def line_move(a, g, start, width, s):
        return line_copy(
            columns(a, order[s], width),
            block(outs[g], group, place).at[:, pl.ds(start, width)],
            line_send.at[a, s],
            line_recv.at[a, place],
            {"context": order[s]},
        )

    def line_arrival(a, g, start, width, s):
        return line_copy(
            columns(a, place, width),
            block(outs[g], group, order[s]).at[:, pl.ds(start, width)],
            line_send.at[a, s],
            line_recv.at[a, order[s]],
            {"context": order[s]},
        )

    def near_copy(way, g, s, of_group):
        piece = block(outs[g], of_group, order[s])
        return line_copy(
            piece, piece, near_send.at[way, g, s], near_recv.at[way, g, s], neighbours[way]
        )

    def far_copy(half, g, s, of_group):
        start = (of_group * n + order[s]) * rows + half * (rows // 2)
        piece = outs[g].at[pl.ds(pl.multiple_of(start, rows // 2), rows // 2)]
        return line_copy(
            piece, piece, far_send.at[half, g, s], far_recv.at[half, g, s], neighbours[1 - half]
        )

    def own_start():
        for span in spans:
            own_copy(*span).start()

    def line_start(span, s):
        return lambda: line_move(*span, s).start()

    def spread(g, s):
        def step():
            for span in spans:
                if span[1] == g:
                    if s == 0:
                        own_copy(*span).wait()
                    else:
                        line_arrival(*span, s).wait_recv()
            near_copy(0, g, s, group).start()
            near_copy(1, g, s, group).start()

        return step

    def pass_on(g, s):
        def step():
            for half in (0, 1):
                source = jnp.bitwise_xor(group, half + 1)
                near_copy(half, g, s, source).wait_recv()
                far_copy(half, g, s, source).start()

        return step

    def settle():
        for g in range(len(groups)):
            for s in range(n):
                for half in (0, 1):
                    far_copy(half, g, s, jnp.bitwise_xor(group, 3)).wait_recv()
                    far_copy(half, g, s, group).wait_send()
                    near_copy(half, g, s, group).wait_send()
        for span in spans:
            for s in range(1, n):
                line_move(*span, s).wait_send()

    issue = [(span, s) for s in range(1, n) for span in spans]
    at_turn = {(span[0], s): i * start_turns // len(issue) for i, (span, s) in enumerate(issue)}
    plan = [[] for _ in range(turns)]
    for span, s in issue:
        plan[at_turn[span[0], s]].append(line_start(span, s))
    table = nearest(n)
    moves = []
    for s in range(n):
        latest = max(table[table[p][s]].index(p) for p in range(n))
        for g in range(len(groups)):
            ready = max(at_turn[a, latest] for a in groups[g]) + 1 if s else 0
            moves.append((ready, spread(g, s)))
        moves += [(0, pass_on(g, s)) for g in range(len(groups))]
    turn = 0
    for i, (ready, step) in enumerate(moves):
        late = max(0, i - len(groups))
        even = from_turn + late * (turns - from_turn) // (len(moves) - len(groups)) if late else 0
        turn = min(max(turn, ready, even), turns - 1)
        plan[turn].append(step)
    return own_start, plan, settle


def piece_rows(count, body):
    @pl.loop(0, count // 16)
    def _(r):
        body(pl.ds(pl.multiple_of(r * 16, 16), 16))


def give_steps(n, place, groups, grads, outs, bufs, sems, turns, from_turn, deliver):
    first_send, first_recv, second_send, second_recv, line_send, line_recv = sems
    group = lax.axis_index("fsdp")
    rows = outs[0].shape[-2]

    half_rows = rows // 2

    far = ranked(n, place)[::-1]

    def part(g, of_group, s, half):
        block = of_group * n + far[s]
        start = pl.multiple_of(block * rows + half * half_rows, half_rows)
        return grads[g].at[pl.ds(start, half_rows)]

    def first_copy(g, s, half, k):
        target = jnp.bitwise_xor(group, half + 1 if k == 0 else 3)
        return line_copy(
            part(g, target, s, half),
            bufs[g]["first"].at[s, half, k],
            first_send.at[g, s, half, k],
            first_recv.at[g, s, half, k],
            {"fsdp": jnp.bitwise_xor(group, half + 1)},
        )

    def second_copy(g, s, half):
        return line_copy(
            bufs[g]["second_out"].at[s, half],
            bufs[g]["second"].at[s, half],
            second_send.at[g, s, half],
            second_recv.at[g, s, half],
            {"fsdp": jnp.bitwise_xor(group, 2 - half)},
        )

    def line_moves(g, s, arrival=False):
        start = 0
        for a in groups[g]:
            width = outs[a].shape[1] // n
            quarter = far[s] if arrival else place
            ref = outs[a].at[:, pl.ds(pl.multiple_of(quarter * width, 128), width)]
            out = bufs[g]["line_out"].at[min(s, n - 2), :, pl.ds(start, width)]
            yield line_copy(
                ref if arrival else out,
                ref,
                line_send.at[a, s],
                line_recv.at[a, quarter],
                {"context": far[s]},
            )
            start += width

    def store(g, at, values):
        start = 0
        for a in groups[g]:
            width = outs[a].shape[1] // n
            cols = pl.ds(pl.multiple_of(place * width, 128), width)
            outs[a][at, cols] = values[:, start : start + width].astype(jnp.bfloat16)
            start += width

    def send_first(g, s):
        for k in (1, 0):
            for half in (0, 1):
                first_copy(g, s, half, k).start()

    def begin():
        for i in range(2 * len(groups)):
            g, s = order[i]
            send_first(g, s)

    def across(i):
        g, s = order[i]

        def step():
            for half in (0, 1):
                first_copy(g, s, half, 1).wait_recv()
                own = part(g, jnp.bitwise_xor(group, 2 - half), s, half)
                came = bufs[g]["first"].at[s, half, 1]
                out = bufs[g]["second_out"].at[s, half]

                def add(at, own=own, came=came, out=out):
                    out[at, :] = (
                        own[at, :].astype(jnp.float32) + came[at, :].astype(jnp.float32)
                    ).astype(jnp.bfloat16)

                piece_rows(half_rows, add)
                second_copy(g, s, half).start()
            if i + 2 * len(groups) < len(order):
                send_first(*order[i + 2 * len(groups)])

        return step

    def total(g, s):
        def step():
            for half in (0, 1):
                first_copy(g, s, half, 0).wait_recv()
                second_copy(g, s, half).wait_recv()
                own = part(g, group, s, half)
                one = bufs[g]["first"].at[s, half, 0]
                two = bufs[g]["second"].at[s, half]

                def add(at, own=own, one=one, two=two, half=half):
                    value = own[at, :].astype(jnp.float32) + one[at, :].astype(jnp.float32)
                    value = value + two[at, :].astype(jnp.float32)
                    to = pl.ds(pl.multiple_of(at.start + half * half_rows, 16), 16)
                    if not deliver:
                        width = value.shape[1]
                        start = sum(grads[h].shape[1] for h in range(g))
                        outs[0][far[s], to, start : start + width] = value.astype(jnp.bfloat16)
                    elif s == n - 1:
                        store(g, to, value)
                    else:
                        bufs[g]["line_out"][s, to, :] = value.astype(jnp.bfloat16)

                piece_rows(half_rows, add)
            if deliver and s < n - 1:
                for move in line_moves(g, s):
                    move.start()

        return step

    def settle():
        for g, s in order:
            for half in (0, 1):
                first_copy(g, s, half, 0).wait_send()
                first_copy(g, s, half, 1).wait_send()
                second_copy(g, s, half).wait_send()
            if deliver and s < n - 1:
                for move in line_moves(g, s):
                    move.wait_send()
                for move in line_moves(g, s, arrival=True):
                    move.wait_recv()

    count = len(groups)
    order = [(g, s) for s in range(n) for g in range(count)]
    steps = []
    for i in range(len(order) + count):
        if i < len(order):
            steps.append(across(i))
        if 0 <= i - count < len(order):
            steps.append(total(*order[i - count]))
    plan = [[] for _ in range(turns)]
    for i, step in enumerate(steps):
        plan[from_turn + i * (turns - from_turn) // len(steps)].append(step)
    return begin, plan, settle


def line_body(n, chunks, n_part, gather, n_in, n_join, n_rest, groups, giving, deliver, extra, finish, *refs):
    refs = list(refs)
    take = lambda count: [refs.pop(0) for _ in range(count)]
    reduce = n_part > 0
    fetching = bool(groups) and not giving
    arrays = sum(len(members) for members in groups)
    parts = take(n_part)
    ins = take(n_in)
    weights = take(arrays) if fetching else []
    grads = take(len(groups)) if giving else []
    others = take(1)[0] if extra else None
    gathered = take(1)[0] if gather else None
    joined = take(n_join)
    rest = take(n_rest)
    fetched = take(len(groups)) if fetching else []
    given = take(arrays if deliver else 1) if giving else []
    gains_out = take(1)[0] if extra else None
    if reduce:
        across, sums_in, sums_out, summed = take(4)
        cross_send, cross_recv, sum_send, sum_recv = take(4)
    if gather:
        row_send, row_recv, pair_send, pair_recv = take(4)
    if n_join:
        join_send, join_recv = take(2)
    fetch_sems = take(7) if fetching else None
    if giving:
        names = ("first", "second_out", "second", "line_out")[: 4 if deliver else 3]
        give_bufs = [dict(zip(names, take(len(names)))) for _ in groups]
        give_sems = take(6)
    if extra:
        gain_own, gain_came, gain_line, gain_send, gain_recv, gain_line_send, gain_line_recv = take(7)

    place = lax.axis_index("context")
    core = lax.axis_index("tensor")
    other = {"tensor": 1 - core}
    step_rows = (ins[0].shape[0]) // chunks

    def rows(j):
        return pl.ds(j * step_rows, step_rows)

    line_barrier(n, place, core, bool(groups))
    lag = LINE_LAG if reduce else 0
    turns = chunks * max(n_part, 1) + lag + n
    plan = [[] for _ in range(turns)]
    if fetching:
        start_turns = min(LINE_START_TURNS, chunks) if reduce else 1
        from_turn = LINE_FROM_TURN if reduce else 1
        own_start, plan, settle = fetch_steps(
            n, place, groups, weights, fetched, fetch_sems, turns, start_turns, from_turn
        )
    if fetching:
        own_start()
    if giving:
        begin, plan, settle = give_steps(
            n, place, groups, grads, given, give_bufs, give_sems, turns, LINE_GIVE_TURN, deliver
        )
        begin()

    def cross(j):
        return line_copy(
            parts[j // chunks].at[:, 1 - core, rows(j % chunks)],
            across.at[:, rows(j)],
            cross_send.at[j],
            cross_recv.at[j],
            other,
        )

    def sum_copy(way, k, j):
        return line_copy(
            sums_out.at[way, k, rows(j)],
            sums_in.at[way, k, rows(j)],
            sum_send.at[way, k, j],
            sum_recv.at[way, k, j],
            {"context": place + 1 - 2 * way},
        )

    def own_term(target, j):
        return parts[j // chunks][target, core, rows(j % chunks), :].astype(jnp.float32) + across[
            target, rows(j), :
        ].astype(jnp.float32)

    def send_sums(way, j):
        first = place == (n - 1) * way
        for k in range(n - 1):
            target = jnp.where(way == 0, n - 1 - k, k)
            passes = jnp.where(way == 0, target - place, place - target) > 0

            @pl.when(passes & first)
            def _(k=k, target=target):
                sums_out[way, k, rows(j), :] = own_term(target, j).astype(jnp.bfloat16)
                sum_copy(way, k, j).start()

            @pl.when(passes & jnp.logical_not(first))
            def _(k=k, target=target):
                sum_copy(way, k, j).wait_recv()
                sums_out[way, k, rows(j), :] = (
                    own_term(target, j) + sums_in[way, k, rows(j), :].astype(jnp.float32)
                ).astype(jnp.bfloat16)
                sum_copy(way, k, j).start()

    def row_copy(way, k, j):
        block = place - k if way == 0 else place + k
        device = {"context": place + 1 if way == 0 else place - 1}
        ref = gathered.at[block, core, rows(j)]
        return line_copy(ref, ref, row_send.at[way, k, j], row_recv.at[way, k, j], device)

    def row_arrival(way, k, j):
        block = place - 1 - k if way == 0 else place + 1 + k
        ref = gathered.at[block, core, rows(j)]
        return line_copy(
            ref, ref, row_send.at[way, k, j], row_recv.at[way, k, j], other
        )

    def pair_copy(block, half, j):
        ref = gathered.at[block, half, rows(j)]
        return line_copy(ref, ref, pair_send.at[block, j], pair_recv.at[block, j], other)

    def finish_rows(j):
        total = None
        if reduce:

            summed[...] = own_term(place, j)

            @pl.when(place > 0)
            def _():
                sum_copy(0, n - 1 - place, j).wait_recv()
                summed[...] += sums_in[0, n - 1 - place, rows(j), :].astype(jnp.float32)

            @pl.when(place < n - 1)
            def _():
                sum_copy(1, place, j).wait_recv()
                summed[...] += sums_in[1, place, rows(j), :].astype(jnp.float32)

            total = summed[...]
        made = finish(j, rows(j % chunks), total, ins, rest)
        made = made if isinstance(made, tuple) else (made,)
        made = list(made)
        if gather and j < chunks:
            gathered[place, core, rows(j), :] = made.pop(0)

            @pl.when(place < n - 1)
            def _():
                row_copy(0, 0, j).start()

            @pl.when(place > 0)
            def _():
                row_copy(1, 0, j).start()

            pair_copy(place, core, j).start()
        if made:
            i = j // chunks - gather
            joined[i][core, rows(j % chunks), :] = made.pop(0)
            join_copy(i, core, j % chunks).start()

    def join_copy(i, half, j):
        ref = joined[i].at[half, rows(j)]
        return line_copy(ref, ref, join_send.at[i, j], join_recv.at[i, j], other)

    def pass_rows(k, j):
        for way in (0, 1):
            block = place - 1 - k if way == 0 else place + 1 + k
            here = block >= 0 if way == 0 else block <= n - 1
            onward = place < n - 1 if way == 0 else place > 0

            @pl.when(here)
            def _(way=way, block=block):
                row_arrival(way, k, j).wait_recv()

            if k + 1 <= n - 2:

                @pl.when(here & onward)
                def _(way=way):
                    row_copy(way, k + 1, j).start()

            @pl.when(here)
            def _(way=way, block=block):
                pair_copy(block, core, j).start()

    all_chunks = chunks * max(n_part, 1)
    if reduce:
        for j in range(all_chunks):
            cross(j).start()

    def gains_plan():
        group = lax.axis_index("fsdp")
        hops = (
            other,
            {"fsdp": jnp.bitwise_xor(group, 1)},
            {"fsdp": jnp.bitwise_xor(group, 2)},
        )

        def hop(h):
            return line_copy(
                gain_own.at[h], gain_came.at[h], gain_send.at[h], gain_recv.at[h], hops[h]
            )

        def line_hop(s):
            return line_copy(
                gain_line.at[place],
                gain_line.at[place],
                gain_line_send.at[s - 1],
                gain_line_recv.at[s - 1],
                {"context": lax.rem(place + s, n)},
            )

        def line_hop_in(s):
            ref = gain_line.at[lax.rem(place + n - s, n)]
            return line_copy(
                ref, ref, gain_line_send.at[s - 1], gain_line_recv.at[s - 1], other
            )

        def first():
            gain_own[0] = others[...]
            gain_own[0, 0:1, :] = rest[0][...]
            hop(0).start()

        def next_hop(h):
            def step():
                hop(h).wait_recv()
                value = gain_own[h] + gain_came[h]
                if h < 2:
                    gain_own[h + 1] = value
                    hop(h + 1).start()
                else:
                    gain_line[place] = value
                    for s in range(1, n):
                        line_hop(s).start()

            return step

        def last():
            for s in range(1, n):
                line_hop_in(s).wait_recv()
            value = gain_line[0]
            for p in range(1, n):
                value = value + gain_line[p]
            gains_out[...] = value
            for h in range(3):
                hop(h).wait_send()
            for s in range(1, n):
                line_hop(s).wait_send()

        return [first, next_hop(0), next_hop(1), next_hop(2), last]

    near = jnp.where(place < n // 2, 0, 1)
    gain_steps = gains_plan() if extra else []
    for i in range(turns):
        for step in plan[i]:
            step()
        if reduce and i < all_chunks:
            cross(i).wait_recv()
            send_sums(near, i)
        if reduce and 0 <= i - 1 < all_chunks:
            send_sums(1 - near, i - 1)
        if 0 <= i - lag < all_chunks:
            finish_rows(i - lag)
        if extra and i - lag >= chunks and gain_steps:
            gain_steps.pop(0)()
        if gather:
            for k in range(n - 1):
                if 0 <= i - lag - 1 - k < chunks:
                    pass_rows(k, i - lag - 1 - k)

    for step in gain_steps:
        step()
    if groups:
        settle()
    for j in range(all_chunks):
        if reduce:
            cross(j).wait_send()
            for k in range(n - 1):

                @pl.when(place < n - 1 - k)
                def _(k=k, j=j):
                    sum_copy(0, k, j).wait_send()

                @pl.when(place > k)
                def _(k=k, j=j):
                    sum_copy(1, k, j).wait_send()

        if gather and j < chunks:
            for block in range(n):
                pair_copy(block, 1 - core, j).wait_recv()
                pair_copy(block, core, j).wait_send()
            for k in range(n - 1):

                @pl.when((place < n - 1) & (place >= k))
                def _(k=k, j=j):
                    row_copy(0, k, j).wait_send()

                @pl.when((place > 0) & (place + k <= n - 1))
                def _(k=k, j=j):
                    row_copy(1, k, j).wait_send()

        if n_join and j // chunks >= gather:
            join_copy(j // chunks - gather, 1 - core, j % chunks).wait_recv()
            join_copy(j // chunks - gather, core, j % chunks).wait_send()


def line_call(
    n,
    collective,
    finish,
    part,
    ins,
    gather=False,
    joins=(),
    rests=(),
    chunks=LINE_CHUNKS,
    groups=(),
    weights=(),
    grads=(),
    deliver=True,
    extra=None,
):
    parts = () if part is None else part if isinstance(part, tuple) else (part,)
    reduce = len(parts) > 0
    giving = len(grads) > 0
    row_count, model_width = ins[0].shape
    vmem = pl.BlockSpec(memory_space=pltpu.VMEM)
    outs = []
    if gather:
        outs.append(jax.ShapeDtypeStruct((n, 2, row_count, model_width), jnp.bfloat16))
    outs += [jax.ShapeDtypeStruct((2, row_count, model_width), kind) for kind in joins]
    outs += list(rests)
    out_specs = [vmem] * len(outs)
    for members in groups if not giving else ():
        rows = weights[0].shape[0] * n * lax.axis_size("fsdp")
        width = sum(weights[a].shape[1] for a in members) // n
        outs.append(jax.ShapeDtypeStruct((rows, width), jnp.bfloat16))
        out_specs.append(pl.BlockSpec(memory_space=pl.ANY))
    dma = pltpu.SemaphoreType.DMA
    if giving:
        owned = grads[0].shape[0] // (n * lax.axis_size("fsdp"))
        shapes = [(owned, width * n) for width in weights]
        if not deliver:
            shapes = [(n, owned, sum(grad.shape[1] for grad in grads))]
        for shape in shapes:
            outs.append(jax.ShapeDtypeStruct(shape, jnp.bfloat16))
            out_specs.append(vmem)
    if extra is not None:
        outs.append(jax.ShapeDtypeStruct(extra.shape, jnp.float32))
        out_specs.append(vmem)
    total_chunks = chunks * max(len(parts), 1)
    sum_rows = row_count * max(len(parts), 1)
    scratch = []
    if reduce:
        slot = pltpu.VMEM((2, n - 1, sum_rows, model_width), jnp.bfloat16)
        scratch += [pltpu.VMEM((n, sum_rows, model_width), jnp.bfloat16), slot, slot]
        scratch += [pltpu.VMEM((row_count // chunks, model_width), jnp.float32)]
        tally = (2, n - 1, total_chunks)
        scratch += [dma((total_chunks,)), dma((total_chunks,)), dma(tally), dma(tally)]
    if gather:
        scratch += [dma((2, n - 1, chunks)), dma((2, n - 1, chunks)), dma((n, chunks)), dma((n, chunks))]
    if joins:
        scratch += [dma((len(joins), chunks)), dma((len(joins), chunks))]
    if groups and not giving:
        arrays = len(weights)
        pieces = (2, len(groups), n)
        scratch += [dma((arrays,)), dma((arrays, n)), dma((arrays, n))]
        scratch += [dma(pieces), dma(pieces), dma(pieces), dma(pieces)]
    if giving:
        for grad in grads:
            halves = (owned // 2, grad.shape[1])
            for lead in ((n, 2, 2), (n, 2), (n, 2)):
                scratch.append(pltpu.VMEM(lead + halves, jnp.bfloat16))
            if deliver:
                scratch.append(pltpu.VMEM((n - 1, owned, grad.shape[1]), jnp.bfloat16))
        count = len(groups)
        scratch += [dma((count, n, 2, 2)), dma((count, n, 2, 2))]
        scratch += [dma((count, n, 2)), dma((count, n, 2))]
        scratch += [dma((len(weights), n)), dma((len(weights), n))]
    if extra is not None:
        stack = pltpu.VMEM((3,) + extra.shape, jnp.float32)
        scratch += [stack, stack, pltpu.VMEM((n,) + extra.shape, jnp.float32)]
        scratch += [dma((3,)), dma((3,)), dma((n - 1,)), dma((n - 1,))]
    operands = list(parts) + list(ins) + (list(grads) if giving else list(weights))
    operands += [] if extra is None else [extra]
    moved = row_count * model_width * 2 * n * (2 * reduce + 2 * gather)
    return pl.pallas_call(
        functools.partial(
            line_body,
            n,
            chunks,
            len(parts),
            gather,
            len(ins),
            len(joins),
            len(rests),
            groups,
            giving,
            deliver,
            extra is not None,
            finish,
        ),
        out_shape=tuple(outs),
        in_specs=[vmem] * len(operands),
        out_specs=tuple(out_specs),
        scratch_shapes=scratch,
        compiler_params=pltpu.CompilerParams(
            collective_id=collective, has_side_effects=True, vmem_limit_bytes=56 << 20
        ),
        cost_estimate=pl.CostEstimate(
            flops=moved, bytes_accessed=20 * moved, transcendentals=0
        ),
    )(*operands)


def finish_gather(j, rows, total, ins, rest):
    values = ins[0][rows, :].astype(jnp.float32)
    return (values * rms_scale(values) * ins[1][...]).astype(jnp.bfloat16)


def finish_attention(j, rows, total, ins, rest):
    residual = ins[0][rows, :].astype(jnp.float32) + total
    rest[0][rows, :] = residual
    return (residual * rms_scale(residual) * ins[1][...]).astype(jnp.bfloat16)


def gain_rows(j, rest, terms):
    sums = jnp.sum(terms, axis=0, keepdims=True)
    rest[...] = sums if j == 0 else rest[...] + sums


def finish_mlp_back(j, rows, total, ins, rest):
    residual = ins[0][rows, :]
    if j >= LINE_CHUNKS:
        return (residual + total).astype(jnp.bfloat16)
    scale = rms_scale(residual)
    hat = residual * scale
    grad = ins[1][rows, :].astype(jnp.float32) + norm_back(total, hat, scale, ins[2][...])
    rest[0][rows, :] = grad
    gain_rows(j, rest[1], total * hat)
    return grad.astype(jnp.bfloat16)


def finish_tokens(j, rows, total, ins, rest):
    values = ins[1][rows, :].astype(jnp.float32)
    scale = rms_scale(values)
    hat = values * scale
    gain_rows(j, rest[0], total * hat)
    return ins[0][rows, :] + norm_back(total, hat, scale, ins[2][...])


def permuted_tokens(rows):
    n = lax.axis_size("context")
    place = lax.axis_index("context")
    core = lax.axis_index("tensor")
    shape = rows.shape
    near = jnp.zeros((n,) + shape, rows.dtype)
    for s in range(n):
        ring = [(i, (i + s) % n) for i in range(n)]
        came = lax.ppermute(rows, "context", ring) if s else rows
        near = lax.dynamic_update_slice(near, came[None], (lax.rem(place + n - s, n), 0, 0))
    far = lax.ppermute(near, "tensor", [(0, 1), (1, 0)])
    both = jnp.zeros((n, 2) + shape, rows.dtype)
    both = lax.dynamic_update_slice(both, near[:, None], (0, core, 0, 0))
    both = lax.dynamic_update_slice(both, far[:, None], (0, 1 - core, 0, 0))
    return both.reshape(n * 2 * shape[0], shape[1])


def widen_body(h_cols, out, tokens, mlp, *refs):
    attn, results = refs[:4], refs[4:]
    results[0][...] = out[...]
    results[1][...] = tokens[...]
    for a in range(4):
        results[2 + a][...] = attn[a][...].astype(jnp.float32)
    for a in range(3):
        results[6 + a][...] = mlp[0, :, a * h_cols : (a + 1) * h_cols].astype(jnp.float32)


def widen(parts, h_cols, out, tokens, mlp, *attn):
    rows = mlp.shape[1]
    width = out.shape[-1]
    out, tokens = out.reshape(-1, width), tokens.reshape(-1, width)
    token_rows = pl.BlockSpec((out.shape[0] // parts, width), lambda i: (i, 0))
    quarters = [pl.BlockSpec((rows, a.shape[1] // parts), lambda i: (0, i)) for a in attn]
    hidden = pl.BlockSpec((rows, h_cols), lambda i: (0, i))
    results = [jax.ShapeDtypeStruct(a.shape, a.dtype) for a in (out, tokens)]
    results += [jax.ShapeDtypeStruct(a.shape, jnp.float32) for a in attn]
    results += [jax.ShapeDtypeStruct((rows, h_cols * parts), jnp.float32)] * 3
    return pl.pallas_call(
        functools.partial(widen_body, h_cols),
        grid=(parts,),
        in_specs=[token_rows, token_rows, pl.BlockSpec((1,) + mlp.shape[1:], lambda i: (i, 0, 0))]
        + quarters,
        out_specs=tuple([token_rows, token_rows] + quarters + [hidden] * 3),
        out_shape=tuple(results),
        name="widen",
    )(out, tokens, mlp, *attn)


def token_half(block, index, parts):
    rows = block.shape[0] // parts
    return lax.dynamic_slice_in_dim(block, index * rows, rows, axis=0)


def line_shards(
    tokens,
    cotangent,
    norm_gain_attn,
    norm_gain_mlp,
    head_gains,
    query_weight,
    key_matrix,
    value_matrix,
    output_weight,
    gate_weight,
    up_weight,
    down_weight,
):
    _, local_len, model_width = tokens.shape
    parts = lax.axis_size("context")
    cores = lax.axis_size("tensor")
    core = lax.axis_index("tensor")
    full_len = local_len * parts
    q_cols = query_weight.shape[1] // parts
    kv_cols = key_matrix.shape[1] // parts
    h_cols = gate_weight.shape[1] // parts
    q_heads = q_cols // HEAD_DIM
    kv_heads = kv_cols // HEAD_DIM
    head_group = q_heads // kv_heads
    score_scale = 1.0 / math.sqrt(HEAD_DIM)
    positions = jnp.arange(full_len, dtype=jnp.int32)
    cosine_table, sine_table = rope_tables(positions, HEAD_DIM)
    cosine_table = cosine_table[:, None, :]
    sine_table = sine_table[:, None, :]
    visible = positions[None, :] <= positions[:, None]
    gain_attn = norm_gain_attn.astype(jnp.float32)[None]
    gain_mlp = norm_gain_mlp.astype(jnp.float32)[None]
    gain_heads = head_gains.astype(jnp.float32)

    def line_parts(left, right):
        product = column_product(left, right).astype(jnp.bfloat16)
        return product.reshape(parts, cores, half_len, model_width)

    own_cot = token_half(cotangent.reshape(local_len, model_width), core, cores)
    inputs = token_half(tokens.reshape(local_len, model_width), core, cores)
    half_len = local_len // cores
    rows_f32 = jax.ShapeDtypeStruct((half_len, model_width), jnp.float32)
    sums_f32 = jax.ShapeDtypeStruct((1, model_width), jnp.float32)
    normed_attn, in_weights, out_weights = line_call(
        parts,
        1,
        finish_gather,
        None,
        (inputs, gain_attn),
        gather=True,
        groups=((0, 1, 2), (3,)),
        weights=(query_weight, key_matrix, value_matrix, output_weight),
    )
    normed_attn = normed_attn.reshape(full_len, model_width)
    own_cot, normed_attn = lax.optimization_barrier((own_cot, normed_attn))
    grad_out = permuted_tokens(own_cot)

    raw = jnp.dot(normed_attn, in_weights, preferred_element_type=jnp.float32)
    query_split = raw[:, :q_cols].reshape(full_len, q_heads, HEAD_DIM)
    query_scale = rms_scale(query_split)
    query_hat = query_split * query_scale
    queries = rotate(query_hat * gain_heads[0], cosine_table, sine_table).astype(jnp.bfloat16)
    key_split = raw[:, q_cols : q_cols + kv_cols].reshape(full_len, kv_heads, HEAD_DIM)
    key_scale = rms_scale(key_split)
    key_hat = key_split * key_scale
    keys = rotate(key_hat * gain_heads[1], cosine_table, sine_table).astype(jnp.bfloat16)
    values = raw[:, q_cols + kv_cols :].astype(jnp.bfloat16).reshape(full_len, kv_heads, HEAD_DIM)
    queries = queries.reshape(full_len, kv_heads, head_group, HEAD_DIM)

    scores = (
        jnp.einsum("ikgd,jkd->kgij", queries, keys, preferred_element_type=jnp.float32)
        * score_scale
    )
    weights = jnp.where(visible, jnp.exp(scores), 0.0)
    probs = weights / jnp.sum(weights, axis=-1, keepdims=True)
    probs_low = probs.astype(jnp.bfloat16)
    attended = (
        jnp.einsum("kgij,jkd->ikgd", probs_low, values, preferred_element_type=jnp.float32)
        .astype(jnp.bfloat16)
        .reshape(full_len, q_cols)
    )
    normed_mlp, residual, mlp_in, mlp_down = line_call(
        parts,
        2,
        finish_attention,
        line_parts(attended, out_weights),
        (inputs, gain_mlp),
        gather=True,
        rests=(rows_f32,),
        groups=((0, 1), (2,)),
        weights=(gate_weight, up_weight, down_weight),
    )
    normed_mlp = normed_mlp.reshape(full_len, model_width)

    both = jnp.dot(normed_mlp, mlp_in, preferred_element_type=jnp.float32)
    gate_act = both[:, :h_cols]
    upward = both[:, h_cols:]
    sig_gate = jax.nn.sigmoid(gate_act)
    activated = gate_act * sig_gate
    hidden = (activated * upward).astype(jnp.bfloat16)
    grad_hidden = jnp.dot(grad_out, mlp_down, preferred_element_type=jnp.float32)
    derivative = sig_gate * (1.0 + gate_act * (1.0 - sig_gate))
    grad_gate = (grad_hidden * upward * derivative).astype(jnp.bfloat16)
    grad_up = (grad_hidden * activated).astype(jnp.bfloat16)
    grad_both = jnp.concatenate([grad_gate, grad_up], axis=1)
    grad_in = row_product(normed_mlp, grad_both).astype(jnp.bfloat16)
    grad_down = row_product(grad_out, hidden).astype(jnp.bfloat16)
    grad_branch, out, grad_residual, gain_mlp_part, mlp_grads = line_call(
        parts,
        3,
        finish_mlp_back,
        (line_parts(grad_both, mlp_in), line_parts(hidden, mlp_down)),
        (residual, own_cot, gain_mlp),
        gather=True,
        joins=(jnp.bfloat16,),
        rests=(rows_f32, sums_f32),
        groups=((0, 1), (2,)),
        weights=(h_cols, h_cols, h_cols),
        grads=(grad_in, grad_down),
        deliver=False,
    )
    mlp_grads = lax.all_to_all(mlp_grads, "context", split_axis=0, concat_axis=0, tiled=True)
    grad_branch = grad_branch.reshape(full_len, model_width)
    grad_attended = jnp.dot(grad_branch, out_weights, preferred_element_type=jnp.float32)
    grad_attended = grad_attended.astype(jnp.bfloat16)
    grad_attended = grad_attended.reshape(full_len, kv_heads, head_group, HEAD_DIM)
    grad_probs = jnp.einsum(
        "ikgd,jkd->kgij", grad_attended, values, preferred_element_type=jnp.float32
    )
    delta = jnp.sum(probs * grad_probs, axis=-1, keepdims=True)
    grad_scores = (probs * (grad_probs - delta)).astype(jnp.bfloat16)
    grad_queries = (
        jnp.einsum("kgij,jkd->ikgd", grad_scores, keys, preferred_element_type=jnp.float32)
        * score_scale
    ).reshape(full_len, q_heads, HEAD_DIM)
    grad_keys = (
        jnp.einsum("kgij,ikgd->jkd", grad_scores, queries, preferred_element_type=jnp.float32)
        * score_scale
    )
    grad_values = jnp.einsum(
        "kgij,ikgd->jkd", probs_low, grad_attended, preferred_element_type=jnp.float32
    )
    grad_query_hat = unrotate(grad_queries, cosine_table, sine_table)
    grad_key_hat = unrotate(grad_keys, cosine_table, sine_table)
    heads_part = jnp.stack(
        [
            jnp.sum(grad_query_hat * query_hat, axis=(0, 1)),
            jnp.sum(grad_key_hat * key_hat, axis=(0, 1)),
        ]
    )
    grad_raw = jnp.concatenate(
        [
            norm_back(grad_query_hat, query_hat, query_scale, gain_heads[0]).reshape(
                full_len, q_cols
            ),
            norm_back(grad_key_hat, key_hat, key_scale, gain_heads[1]).reshape(full_len, kv_cols),
            grad_values.reshape(full_len, kv_cols),
        ],
        axis=1,
    ).astype(jnp.bfloat16)
    attn_in_grad = row_product(normed_attn, grad_raw).astype(jnp.bfloat16)
    attn_out_grad = row_product(grad_branch, attended).astype(jnp.bfloat16)
    gains = jnp.concatenate(
        [
            jnp.zeros((1, model_width), jnp.float32),
            gain_mlp_part,
            jnp.pad(heads_part.reshape(1, -1), ((0, 0), (0, model_width - heads_part.size))),
            jnp.zeros((5, model_width), jnp.float32),
        ],
        axis=0,
    )
    grad_tokens, _, query_grad, key_grad, value_grad, output_grad, totals = line_call(
        parts,
        4,
        finish_tokens,
        line_parts(grad_raw, in_weights),
        (grad_residual, inputs, gain_attn),
        joins=(jnp.float32,),
        rests=(sums_f32,),
        groups=((0, 1, 2), (3,)),
        weights=(q_cols, kv_cols, kv_cols, q_cols),
        grads=(attn_in_grad, attn_out_grad),
        extra=gains,
    )
    ready = (out, grad_tokens, mlp_grads, query_grad, key_grad, value_grad, output_grad)
    out, grad_tokens, *weight_grads = widen(parts, h_cols, *ready)
    return (
        out.reshape(tokens.shape),
        grad_tokens.reshape(tokens.shape),
        totals[0],
        totals[1],
        totals[2, : heads_part.size].reshape(heads_part.shape),
        *weight_grads,
    )


def layer(*operands):
    tokens, key_matrix, gate_weight = operands[0], operands[6], operands[9]
    parts = lax.axis_size("context")
    cores = lax.axis_size("tensor")
    fits = (
        tokens.shape[0] == 1
        and key_matrix.shape[1] % (parts * HEAD_DIM) == 0
        and gate_weight.shape[1] % (parts * HEAD_DIM) == 0
        and tokens.shape[1] % (cores * LINE_CHUNKS * 16) == 0
        and cores == 2
        and lax.axis_size("fsdp") == 4
    )
    return line_shards(*operands) if fits else shards(*operands)


def solution(mesh):
    return jax.shard_map(
        layer,
        mesh=mesh,
        in_specs=(
            P("fsdp", "context", None),
            P("fsdp", "context", None),
            P(),
            P(),
            P(),
            P(("fsdp", "context"), "tensor"),
            P(("fsdp", "context"), "tensor"),
            P(("fsdp", "context"), "tensor"),
            P(("fsdp", "context"), "tensor"),
            P(("fsdp", "context"), "tensor"),
            P(("fsdp", "context"), "tensor"),
            P(("fsdp", "context"), "tensor"),
        ),
        out_specs=(
            P("fsdp", "context", None),
            P("fsdp", "context", None),
            P(),
            P(),
            P(),
            P(("fsdp", "context"), "tensor"),
            P(("fsdp", "context"), "tensor"),
            P(("fsdp", "context"), "tensor"),
            P(("fsdp", "context"), "tensor"),
            P(("fsdp", "context"), "tensor"),
            P(("fsdp", "context"), "tensor"),
            P(("fsdp", "context"), "tensor"),
        ),
        check_vma=False,
    )
```

```python
import functools
import math

import jax
import jax.numpy as jnp
from jax import lax
from jax.experimental import pallas as pl
from jax.experimental.pallas import tpu as pltpu
from jax.sharding import PartitionSpec as P


HEAD_DIM = 128


EPS = 1e-06
THETA = 1000000.0


def rms_scale(values):
    return lax.rsqrt(jnp.mean(values * values, axis=-1, keepdims=True) + EPS)


def rope_tables(positions, head_size):
    halves = head_size // 2
    inverse = THETA ** (-(jnp.arange(halves, dtype=jnp.float32) * 2.0) / head_size)
    angle = positions[:, None].astype(jnp.float32) * inverse[None, :]
    return (jnp.cos(angle), jnp.sin(angle))


def rotate(values, cosine_table, sine_table):
    halves = values.shape[-1] // 2
    leading = values[..., :halves]
    trailing = values[..., halves:]
    return jnp.concatenate(
        [
            leading * cosine_table - trailing * sine_table,
            trailing * cosine_table + leading * sine_table,
        ],
        axis=-1,
    )


def unrotate(values, cosine_table, sine_table):
    halves = values.shape[-1] // 2
    leading = values[..., :halves]
    trailing = values[..., halves:]
    return jnp.concatenate(
        [
            leading * cosine_table + trailing * sine_table,
            trailing * cosine_table - leading * sine_table,
        ],
        axis=-1,
    )


def norm_back(grad_normed, normed_hat, scale_factor, gain):
    scaled = grad_normed * gain
    return scale_factor * (
        scaled - normed_hat * jnp.mean(normed_hat * scaled, axis=-1, keepdims=True)
    )


def row_product(left, right):
    return lax.dot_general(
        left, right, (((0,), (0,)), ((), ())), preferred_element_type=jnp.float32
    )


def column_product(left, right):
    return lax.dot_general(
        left, right, (((1,), (1,)), ((), ())), preferred_element_type=jnp.float32
    )


def blank(row_total, col_total):
    return jnp.zeros((row_total, col_total), jnp.float32)


def placing(left):

    def place_rows(total, piece, start):
        return column_product(left, piece)

    return place_rows


def adding(left):

    def add_rows(total, piece, start):
        return jnp.dot(left, piece, preferred_element_type=jnp.float32)

    return add_rows


def tensor_total(partial_sum):
    return lax.psum(partial_sum, "tensor")


def owner_rows(term_fn, row_total):
    return lax.psum_scatter(
        term_fn(jnp.int32(0), lax.axis_size(("fsdp", "context")) * row_total),
        ("fsdp", "context"),
        scatter_dimension=0,
        tiled=True,
    )


def shards(
    tokens,
    cotangent,
    norm_gain_attn,
    norm_gain_mlp,
    head_gains,
    query_weight,
    key_matrix,
    value_matrix,
    output_weight,
    gate_weight,
    up_weight,
    down_weight,
):
    seq_count, local_len, model_width = tokens.shape
    row_count = seq_count * local_len
    owned_rows = query_weight.shape[0]
    query_cols = query_weight.shape[1]
    kv_cols = key_matrix.shape[1]
    hidden_cols = gate_weight.shape[1]
    query_heads = query_cols // HEAD_DIM
    kv_heads = kv_cols // HEAD_DIM
    head_group = query_heads // kv_heads
    score_scale = 1.0 / math.sqrt(HEAD_DIM)
    full_len = local_len * lax.axis_size("context")
    query_pos = lax.axis_index("context") * local_len + jnp.arange(local_len, dtype=jnp.int32)
    key_pos = jnp.arange(full_len, dtype=jnp.int32)
    cosine_table, sine_table = rope_tables(query_pos, HEAD_DIM)
    cosine_table = cosine_table[:, None, :]
    sine_table = sine_table[:, None, :]
    visible = key_pos[None, :] <= query_pos[:, None]
    inputs = tokens.reshape(row_count, model_width).astype(jnp.float32)
    grad_out = cotangent.reshape(row_count, model_width)
    gain_attn = norm_gain_attn.astype(jnp.float32)
    gain_mlp = norm_gain_mlp.astype(jnp.float32)
    gain_heads = head_gains.astype(jnp.float32)

    def attn_rows(fold_fn, initial):
        return fold_fn(
            initial,
            (
                lax.all_gather(query_weight, ("fsdp", "context"), axis=0, tiled=True),
                lax.all_gather(key_matrix, ("fsdp", "context"), axis=0, tiled=True),
                lax.all_gather(value_matrix, ("fsdp", "context"), axis=0, tiled=True),
            ),
            jnp.int32(0),
        )

    def attn_out_rows(fold_fn, initial):
        return fold_fn(
            initial,
            lax.all_gather(output_weight, ("fsdp", "context"), axis=0, tiled=True),
            jnp.int32(0),
        )

    def mlp_rows(fold_fn, initial):
        return fold_fn(
            initial,
            (
                lax.all_gather(gate_weight, ("fsdp", "context"), axis=0, tiled=True),
                lax.all_gather(up_weight, ("fsdp", "context"), axis=0, tiled=True),
            ),
            jnp.int32(0),
        )

    def down_rows(fold_fn, initial):
        return fold_fn(
            initial,
            lax.all_gather(down_weight, ("fsdp", "context"), axis=0, tiled=True),
            jnp.int32(0),
        )

    scale_attn = rms_scale(inputs)
    hat_attn = inputs * scale_attn
    normed_attn = (hat_attn * gain_attn).astype(jnp.bfloat16)

    def project_in(totals, pieces, start):
        return (
            jnp.dot(normed_attn, pieces[0], preferred_element_type=jnp.float32),
            jnp.dot(normed_attn, pieces[1], preferred_element_type=jnp.float32),
            jnp.dot(normed_attn, pieces[2], preferred_element_type=jnp.float32),
        )

    query_raw, key_unrotated, value_raw = attn_rows(
        project_in,
        (blank(row_count, query_cols), blank(row_count, kv_cols), blank(row_count, kv_cols)),
    )
    query_split = query_raw.reshape(seq_count, local_len, query_heads, HEAD_DIM)
    query_scale = rms_scale(query_split)
    query_hat = query_split * query_scale
    query_rows = rotate(query_hat * gain_heads[0], cosine_table, sine_table).astype(jnp.bfloat16)
    key_split = key_unrotated.reshape(seq_count, local_len, kv_heads, HEAD_DIM)
    key_scale = rms_scale(key_split)
    key_hat = key_split * key_scale
    keys_local = rotate(key_hat * gain_heads[1], cosine_table, sine_table).astype(jnp.bfloat16)
    values_local = value_raw.astype(jnp.bfloat16)
    keys_all, value_rows_gathered = (
        lax.all_gather(
            keys_local.reshape(seq_count, local_len, kv_cols), "context", axis=1, tiled=True
        ),
        lax.all_gather(
            values_local.reshape(seq_count, local_len, kv_cols), "context", axis=1, tiled=True
        ),
    )
    query_blocks = query_rows.reshape(
        seq_count, local_len, kv_heads, head_group, HEAD_DIM
    ).transpose(2, 0, 1, 3, 4)
    key_blocks = keys_all.reshape(seq_count, full_len, kv_heads, HEAD_DIM).transpose(2, 0, 1, 3)
    value_blocks = value_rows_gathered.reshape(seq_count, full_len, kv_heads, HEAD_DIM).transpose(
        2, 0, 1, 3
    )

    def attend(operands):
        query_block, key_block, value_block = operands
        scores = (
            jnp.einsum("bigd,bjd->bgij", query_block, key_block, preferred_element_type=jnp.float32)
            * score_scale
        )
        weights = jnp.where(visible, jnp.exp(scores), 0.0)
        totals = jnp.sum(weights, axis=-1)
        probs_low = (weights / totals[..., None]).astype(jnp.bfloat16)
        mixed_heads = jnp.einsum(
            "bgij,bjd->bigd", probs_low, value_block, preferred_element_type=jnp.float32
        )
        return (mixed_heads.astype(jnp.bfloat16), jnp.log(totals))

    mixed_all, log_totals = lax.map(attend, (query_blocks, key_blocks, value_blocks))
    attended = mixed_all.transpose(1, 2, 0, 3, 4).reshape(row_count, query_cols)
    attn_part = attn_out_rows(placing(attended), blank(row_count, model_width))
    residual = inputs + tensor_total(attn_part)
    scale_mlp = rms_scale(residual)
    hat_mlp = residual * scale_mlp
    normed_mlp = (hat_mlp * gain_mlp).astype(jnp.bfloat16)

    def project_mlp(totals, pieces, start):
        return (
            jnp.dot(normed_mlp, pieces[0], preferred_element_type=jnp.float32),
            jnp.dot(normed_mlp, pieces[1], preferred_element_type=jnp.float32),
        )

    gate_act, upward = mlp_rows(
        project_mlp, (blank(row_count, hidden_cols), blank(row_count, hidden_cols))
    )
    sig_gate = jax.nn.sigmoid(gate_act)
    activated = gate_act * sig_gate
    hidden = (activated * upward).astype(jnp.bfloat16)
    mlp_part = down_rows(placing(hidden), blank(row_count, model_width))
    result = residual + tensor_total(mlp_part)
    out = result.astype(jnp.bfloat16).reshape(seq_count, local_len, model_width)
    grad_hidden = down_rows(adding(grad_out), blank(row_count, hidden_cols))
    derivative = sig_gate * (1.0 + gate_act * (1.0 - sig_gate))
    grad_gate = (grad_hidden * upward * derivative).astype(jnp.bfloat16)
    grad_up = (grad_hidden * activated).astype(jnp.bfloat16)

    def gate_back(total, pieces, start):
        part_sum = column_product(grad_gate, pieces[0]) + column_product(grad_up, pieces[1])
        return part_sum

    grad_normed_mlp = tensor_total(mlp_rows(gate_back, blank(row_count, model_width)))

    def mlp_terms(start, span_rows):
        return jnp.concatenate(
            [
                row_product(normed_mlp, grad_gate),
                row_product(normed_mlp, grad_up),
                row_product(grad_out, hidden),
            ],
            axis=1,
        )

    mlp_grads = owner_rows(mlp_terms, owned_rows)
    grad_gain_mlp = jnp.sum(grad_normed_mlp * hat_mlp, axis=0)
    grad_residual = grad_out.astype(jnp.float32) + norm_back(
        grad_normed_mlp, hat_mlp, scale_mlp, gain_mlp
    )
    grad_branch = grad_residual.astype(jnp.bfloat16)
    grad_attended = attn_out_rows(adding(grad_branch), blank(row_count, query_cols))
    grad_attended_low = grad_attended.astype(jnp.bfloat16)
    grad_blocks = grad_attended_low.reshape(
        seq_count, local_len, kv_heads, head_group, HEAD_DIM
    ).transpose(2, 0, 1, 3, 4)

    def attend_back(operands):
        query_block, key_block, value_block, grad_block, log_total = operands
        scores = (
            jnp.einsum("bigd,bjd->bgij", query_block, key_block, preferred_element_type=jnp.float32)
            * score_scale
        )
        probs = jnp.where(visible, jnp.exp(scores - log_total[..., None]), 0.0)
        probs_low = probs.astype(jnp.bfloat16)
        grad_probs = jnp.einsum(
            "bigd,bjd->bgij", grad_block, value_block, preferred_element_type=jnp.float32
        )
        delta = jnp.sum(probs * grad_probs, axis=-1, keepdims=True)
        grad_scores = (probs * (grad_probs - delta)).astype(jnp.bfloat16)
        grad_query = (
            jnp.einsum("bgij,bjd->bigd", grad_scores, key_block, preferred_element_type=jnp.float32)
            * score_scale
        )
        grad_key = (
            jnp.einsum(
                "bgij,bigd->bjd", grad_scores, query_block, preferred_element_type=jnp.float32
            )
            * score_scale
        )
        grad_value = jnp.einsum(
            "bgij,bigd->bjd", probs_low, grad_block, preferred_element_type=jnp.float32
        )
        return (grad_query, grad_key, grad_value, delta[..., 0])

    grad_query_all, grad_key_all, grad_value_all, _ = lax.map(
        attend_back, (query_blocks, key_blocks, value_blocks, grad_blocks, log_totals)
    )
    grad_key_full = grad_key_all.transpose(1, 2, 0, 3).reshape(seq_count, full_len, kv_cols)
    grad_value_full = grad_value_all.transpose(1, 2, 0, 3).reshape(seq_count, full_len, kv_cols)
    grad_key_own, grad_value_own = (
        lax.psum_scatter(
            grad_key_full.astype(jnp.bfloat16), "context", scatter_dimension=1, tiled=True
        ).astype(jnp.float32),
        lax.psum_scatter(
            grad_value_full.astype(jnp.bfloat16), "context", scatter_dimension=1, tiled=True
        ).astype(jnp.float32),
    )
    grad_query_rot = grad_query_all.transpose(1, 2, 0, 3, 4).reshape(
        seq_count, local_len, query_heads, HEAD_DIM
    )
    grad_query_hat = unrotate(grad_query_rot, cosine_table, sine_table)
    grad_key_hat = unrotate(
        grad_key_own.reshape(seq_count, local_len, kv_heads, HEAD_DIM), cosine_table, sine_table
    )
    grad_gain_query = jnp.sum(grad_query_hat * query_hat, axis=(0, 1, 2))
    grad_gain_key = jnp.sum(grad_key_hat * key_hat, axis=(0, 1, 2))
    grad_query_raw = (
        norm_back(grad_query_hat, query_hat, query_scale, gain_heads[0])
        .reshape(row_count, query_cols)
        .astype(jnp.bfloat16)
    )
    grad_key_raw = (
        norm_back(grad_key_hat, key_hat, key_scale, gain_heads[1])
        .reshape(row_count, kv_cols)
        .astype(jnp.bfloat16)
    )
    grad_value_low = grad_value_own.reshape(row_count, kv_cols).astype(jnp.bfloat16)

    def attn_back(total, pieces, start):
        part_sum = (
            column_product(grad_query_raw, pieces[0])
            + column_product(grad_key_raw, pieces[1])
            + column_product(grad_value_low, pieces[2])
        )
        return part_sum

    grad_normed_part = attn_rows(attn_back, blank(row_count, model_width))
    grad_normed_attn, grad_heads_gain = (
        lax.psum(grad_normed_part.astype(jnp.bfloat16), "tensor").astype(jnp.float32),
        lax.psum(jnp.stack([grad_gain_query, grad_gain_key]).astype(jnp.bfloat16), "tensor").astype(
            jnp.float32
        ),
    )

    def attn_terms(start, span_rows):
        return jnp.concatenate(
            [
                row_product(normed_attn, grad_query_raw),
                row_product(normed_attn, grad_key_raw),
                row_product(normed_attn, grad_value_low),
                row_product(grad_branch, attended),
            ],
            axis=1,
        )

    attn_grads = owner_rows(attn_terms, owned_rows)
    grad_gain_attn = jnp.sum(grad_normed_attn * hat_attn, axis=0)
    grad_tokens = grad_residual + norm_back(grad_normed_attn, hat_attn, scale_attn, gain_attn)
    total_attn, total_mlp, total_heads = lax.psum(
        (grad_gain_attn, grad_gain_mlp, grad_heads_gain), ("fsdp", "context")
    )
    query_grad = attn_grads[:, :query_cols]
    key_grad = attn_grads[:, query_cols : query_cols + kv_cols]
    value_grad = attn_grads[:, query_cols + kv_cols : query_cols + 2 * kv_cols]
    output_grad = attn_grads[:, query_cols + 2 * kv_cols :]
    gate_grad = mlp_grads[:, :hidden_cols]
    up_grad = mlp_grads[:, hidden_cols : 2 * hidden_cols]
    down_grad = mlp_grads[:, 2 * hidden_cols :]
    return (
        out,
        grad_tokens.reshape(seq_count, local_len, model_width),
        total_attn,
        total_mlp,
        total_heads,
        query_grad,
        key_grad,
        value_grad,
        output_grad,
        gate_grad,
        up_grad,
        down_grad,
    )


LINE_CHUNKS = 8
LINE_LAG = 2
LINE_START_TURNS = 1
LINE_FROM_TURN = 1
LINE_PLAIN_FROM = 0
LINE_PLAIN_LAG = 1
LINE_PLAIN_STEP = 1
LINE_GIVE_TURN = 6
MESH = pl.DeviceIdType.MESH


def line_copy(src, dst, send, recv, device):
    return pltpu.make_async_remote_copy(
        src_ref=src,
        dst_ref=dst,
        send_sem=send,
        recv_sem=recv,
        device_id=device,
        device_id_type=MESH,
    )


def line_barrier(n, place, core, fetching):
    barrier = pltpu.get_barrier_semaphore()

    def greet(device):
        pl.semaphore_signal(barrier, inc=1, device_id=device, device_id_type=MESH)

    greet({"tensor": 1 - core})
    if fetching:
        group = lax.axis_index("fsdp")
        greet({"fsdp": jnp.bitwise_xor(group, 1)})
        greet({"fsdp": jnp.bitwise_xor(group, 2)})
        for shift in range(1, n):
            greet({"context": lax.rem(place + shift, n)})
        pl.semaphore_wait(barrier, n + 2)
        return

    @pl.when(place > 0)
    def _():
        greet({"context": place - 1})

    @pl.when(place < n - 1)
    def _():
        greet({"context": place + 1})

    ends = jnp.where(place > 0, 1, 0) + jnp.where(place < n - 1, 1, 0)
    pl.semaphore_wait(barrier, ends + 1)


def nearest(n):
    return [sorted(range(n), key=lambda q: (abs(q - p), q)) for p in range(n)]


def ranked(n, place):
    table = nearest(n)
    return [sum(jnp.where(place == p, table[p][k], 0) for p in range(n)) for k in range(n)]


def fetch_steps(n, place, groups, weights, outs, sems, turns, start_turns, from_turn):
    own_send, line_send, line_recv, near_send, near_recv, far_send, far_recv = sems
    group = lax.axis_index("fsdp")
    rows = weights[0].shape[0]
    neighbours = ({"fsdp": jnp.bitwise_xor(group, 1)}, {"fsdp": jnp.bitwise_xor(group, 2)})
    spans = []
    for g, members in enumerate(groups):
        start = 0
        for a in members:
            width = weights[a].shape[1] // n
            spans.append((a, g, start, width))
            start += width

    def block(out, of_group, at):
        return out.at[pl.ds(pl.multiple_of((of_group * n + at) * rows, rows), rows)]

    order = ranked(n, place)

    def columns(a, at, width):
        return weights[a].at[:, pl.ds(pl.multiple_of(at * width, 128), width)]

    def own_copy(a, g, start, width):
        return pltpu.make_async_copy(
            columns(a, place, width),
            block(outs[g], group, place).at[:, pl.ds(start, width)],
            own_send.at[a],
        )

    def line_move(a, g, start, width, s):
        return line_copy(
            columns(a, order[s], width),
            block(outs[g], group, place).at[:, pl.ds(start, width)],
            line_send.at[a, s],
            line_recv.at[a, place],
            {"context": order[s]},
        )

    def line_arrival(a, g, start, width, s):
        return line_copy(
            columns(a, place, width),
            block(outs[g], group, order[s]).at[:, pl.ds(start, width)],
            line_send.at[a, s],
            line_recv.at[a, order[s]],
            {"context": order[s]},
        )

    def near_copy(way, g, s, of_group):
        piece = block(outs[g], of_group, order[s])
        return line_copy(
            piece, piece, near_send.at[way, g, s], near_recv.at[way, g, s], neighbours[way]
        )

    def far_copy(half, g, s, of_group):
        start = (of_group * n + order[s]) * rows + half * (rows // 2)
        piece = outs[g].at[pl.ds(pl.multiple_of(start, rows // 2), rows // 2)]
        return line_copy(
            piece, piece, far_send.at[half, g, s], far_recv.at[half, g, s], neighbours[1 - half]
        )

    def own_start():
        for span in spans:
            own_copy(*span).start()

    def line_start(span, s):
        return lambda: line_move(*span, s).start()

    def spread(g, s):
        def step():
            for span in spans:
                if span[1] == g:
                    if s == 0:
                        own_copy(*span).wait()
                    else:
                        line_arrival(*span, s).wait_recv()
            near_copy(0, g, s, group).start()
            near_copy(1, g, s, group).start()

        return step

    def pass_on(g, s):
        def step():
            for half in (0, 1):
                source = jnp.bitwise_xor(group, half + 1)
                near_copy(half, g, s, source).wait_recv()
                far_copy(half, g, s, source).start()

        return step

    def settle():
        for g in range(len(groups)):
            for s in range(n):
                for half in (0, 1):
                    far_copy(half, g, s, jnp.bitwise_xor(group, 3)).wait_recv()
                    far_copy(half, g, s, group).wait_send()
                    near_copy(half, g, s, group).wait_send()
        for span in spans:
            for s in range(1, n):
                line_move(*span, s).wait_send()

    issue = [(span, s) for s in range(1, n) for span in spans]
    at_turn = {(span[0], s): i * start_turns // len(issue) for i, (span, s) in enumerate(issue)}
    plan = [[] for _ in range(turns)]
    for span, s in issue:
        plan[at_turn[span[0], s]].append(line_start(span, s))
    table = nearest(n)
    moves = []
    for s in range(n):
        latest = max(table[table[p][s]].index(p) for p in range(n))
        for g in range(len(groups)):
            ready = max(at_turn[a, latest] for a in groups[g]) + 1 if s else 0
            moves.append((ready, spread(g, s)))
        moves += [(0, pass_on(g, s)) for g in range(len(groups))]
    turn = 0
    for i, (ready, step) in enumerate(moves):
        late = max(0, i - len(groups))
        even = from_turn + late * (turns - from_turn) // (len(moves) - len(groups)) if late else 0
        turn = min(max(turn, ready, even), turns - 1)
        plan[turn].append(step)
    return own_start, plan, settle


def piece_rows(count, body):
    @pl.loop(0, count // 16)
    def _(r):
        body(pl.ds(pl.multiple_of(r * 16, 16), 16))


def give_steps(n, place, groups, grads, outs, bufs, sems, turns, from_turn, deliver):
    first_send, first_recv, second_send, second_recv, line_send, line_recv, mine_sem = sems
    group = lax.axis_index("fsdp")
    rows = outs[0].shape[-2]

    half_rows = rows // 2

    far = ranked(n, place)[::-1]

    def part(g, of_group, s, half):
        block = of_group * n + far[s]
        start = pl.multiple_of(block * rows + half * half_rows, half_rows)
        return grads[g].at[pl.ds(start, half_rows)]

    def mine_copy(g, s, half, k):
        target = group if k == 0 else jnp.bitwise_xor(group, 2 - half)
        return pltpu.make_async_copy(
            part(g, target, s, half), bufs[g]["mine"].at[s, half, k], mine_sem.at[g, s, half, k]
        )

    def first_copy(g, s, half, k):
        target = jnp.bitwise_xor(group, half + 1 if k == 0 else 3)
        return line_copy(
            part(g, target, s, half),
            bufs[g]["first"].at[s, half, k],
            first_send.at[g, s, half, k],
            first_recv.at[g, s, half, k],
            {"fsdp": jnp.bitwise_xor(group, half + 1)},
        )

    def second_copy(g, s, half):
        return line_copy(
            bufs[g]["second_out"].at[s, half],
            bufs[g]["second"].at[s, half],
            second_send.at[g, s, half],
            second_recv.at[g, s, half],
            {"fsdp": jnp.bitwise_xor(group, 2 - half)},
        )

    def line_moves(g, s, arrival=False):
        start = 0
        for a in groups[g]:
            width = outs[a].shape[1] // n
            quarter = far[s] if arrival else place
            ref = outs[a].at[:, pl.ds(pl.multiple_of(quarter * width, 128), width)]
            out = bufs[g]["line_out"].at[min(s, n - 2), :, pl.ds(start, width)]
            yield line_copy(
                ref if arrival else out,
                ref,
                line_send.at[a, s],
                line_recv.at[a, quarter],
                {"context": far[s]},
            )
            start += width

    def store(g, at, values):
        start = 0
        for a in groups[g]:
            width = outs[a].shape[1] // n
            cols = pl.ds(pl.multiple_of(place * width, 128), width)
            outs[a][at, cols] = values[:, start : start + width].astype(jnp.bfloat16)
            start += width

    def send_first(g, s):
        for k in (1, 0):
            for half in (0, 1):
                first_copy(g, s, half, k).start()
                mine_copy(g, s, half, k).start()

    def begin():
        for i in range(2 * len(groups)):
            g, s = order[i]
            send_first(g, s)

    def across(i):
        g, s = order[i]

        def step():
            for half in (0, 1):
                first_copy(g, s, half, 1).wait_recv()
                mine_copy(g, s, half, 1).wait()
                own = bufs[g]["mine"].at[s, half, 1]
                came = bufs[g]["first"].at[s, half, 1]
                out = bufs[g]["second_out"].at[s, half]

                def add(at, own=own, came=came, out=out):
                    out[at, :] = (
                        own[at, :].astype(jnp.float32) + came[at, :].astype(jnp.float32)
                    ).astype(jnp.bfloat16)

                piece_rows(half_rows, add)
                second_copy(g, s, half).start()
            if i + 2 * len(groups) < len(order):
                send_first(*order[i + 2 * len(groups)])

        return step

    def total(g, s):
        def step():
            for half in (0, 1):
                first_copy(g, s, half, 0).wait_recv()
                second_copy(g, s, half).wait_recv()
                mine_copy(g, s, half, 0).wait()
                own = bufs[g]["mine"].at[s, half, 0]
                one = bufs[g]["first"].at[s, half, 0]
                two = bufs[g]["second"].at[s, half]

                def add(at, own=own, one=one, two=two, half=half):
                    value = own[at, :].astype(jnp.float32) + one[at, :].astype(jnp.float32)
                    value = value + two[at, :].astype(jnp.float32)
                    to = pl.ds(pl.multiple_of(at.start + half * half_rows, 16), 16)
                    if not deliver:
                        width = value.shape[1]
                        start = sum(grads[h].shape[1] for h in range(g))
                        outs[0][far[s], to, start : start + width] = value.astype(jnp.bfloat16)
                    elif s == n - 1:
                        store(g, to, value)
                    else:
                        bufs[g]["line_out"][s, to, :] = value.astype(jnp.bfloat16)

                piece_rows(half_rows, add)
            if deliver and s < n - 1:
                for move in line_moves(g, s):
                    move.start()

        return step

    def settle():
        for g, s in order:
            for half in (0, 1):
                first_copy(g, s, half, 0).wait_send()
                first_copy(g, s, half, 1).wait_send()
                second_copy(g, s, half).wait_send()
            if deliver and s < n - 1:
                for move in line_moves(g, s):
                    move.wait_send()
                for move in line_moves(g, s, arrival=True):
                    move.wait_recv()

    count = len(groups)
    order = [(g, s) for s in range(n) for g in range(count)]
    steps = []
    for i in range(len(order) + count):
        if i < len(order):
            steps.append(across(i))
        if 0 <= i - count < len(order):
            steps.append(total(*order[i - count]))
    plan = [[] for _ in range(turns)]
    for i, step in enumerate(steps):
        plan[from_turn + i * (turns - from_turn) // len(steps)].append(step)
    return begin, plan, settle


def spread_steps(n, pieces, out, sems, turns, from_turn):
    own_send, near_send, near_recv, far_send, far_recv = sems
    group = lax.axis_index("fsdp")
    rows = pieces.shape[1]
    neighbours = ({"fsdp": jnp.bitwise_xor(group, 1)}, {"fsdp": jnp.bitwise_xor(group, 2)})

    def block(of_group, k, half=None):
        start = (of_group * n + k) * rows
        if half is None:
            return out.at[pl.ds(pl.multiple_of(start, rows), rows)]
        return out.at[pl.ds(pl.multiple_of(start + half * (rows // 2), rows // 2), rows // 2)]

    def own_copy(k):
        return pltpu.make_async_copy(pieces.at[k], block(group, k), own_send.at[k])

    def near_copy(way, k, of_group):
        return line_copy(
            pieces.at[k],
            block(of_group, k),
            near_send.at[way, k],
            near_recv.at[way, k],
            neighbours[way],
        )

    def far_copy(half, k, of_group):
        ref = block(of_group, k, half)
        return line_copy(
            ref, ref, far_send.at[half, k], far_recv.at[half, k], neighbours[1 - half]
        )

    def begin():
        for k in range(n):
            for way in (0, 1):
                near_copy(way, k, group).start()
            own_copy(k).start()

    def pass_on(k):
        def step():
            for half in (0, 1):
                source = jnp.bitwise_xor(group, half + 1)
                near_copy(half, k, source).wait_recv()
                far_copy(half, k, source).start()

        return step

    def settle():
        for k in range(n):
            own_copy(k).wait()
            for half in (0, 1):
                far_copy(half, k, jnp.bitwise_xor(group, 3)).wait_recv()
                far_copy(half, k, group).wait_send()
                near_copy(half, k, group).wait_send()

    plan = [[] for _ in range(turns)]
    for k in range(n):
        plan[from_turn + k * (turns - from_turn) // n].append(pass_on(k))
    return begin, plan, settle


def line_body(n, chunks, n_part, gather, spreading, n_in, n_join, n_rest, groups, giving, deliver, extra, finish, *refs):
    refs = list(refs)
    take = lambda count: [refs.pop(0) for _ in range(count)]
    reduce = n_part > 0
    fetching = bool(groups) and not giving
    arrays = sum(len(members) for members in groups)
    parts = take(n_part)
    ins = take(n_in)
    weights = take(arrays) if fetching else []
    grads = take(len(groups)) if giving else []
    others = take(1)[0] if extra else None
    pieces = take(1)[0] if spreading else None
    gathered_all = take(gather)
    joined = take(n_join)
    rest = take(n_rest)
    fetched = take(len(groups)) if fetching else []
    spread_out = take(1)[0] if spreading else None
    given = take(arrays if deliver else 1) if giving else []
    gains_out = take(1)[0] if extra else None
    if reduce:
        own, own_sem, across, sums_in, sums_out, summed = take(6)
        cross_send, cross_recv, sum_send, sum_recv = take(4)
    if gather:
        row_send, row_recv, pair_send, pair_recv = take(4)
    if n_join:
        join_send, join_recv = take(2)
    fetch_sems = take(7) if fetching else None
    spread_sems = take(5) if spreading else None
    if giving:
        names = ("mine", "first", "second_out", "second", "line_out")[: 5 if deliver else 4]
        give_bufs = [dict(zip(names, take(len(names)))) for _ in groups]
        give_sems = take(7)
    if extra:
        gain_own, gain_came, gain_line, gain_send, gain_recv, gain_line_send, gain_line_recv = take(7)

    place = lax.axis_index("context")
    core = lax.axis_index("tensor")
    other = {"tensor": 1 - core}
    step_rows = (ins[0].shape[0]) // chunks

    def rows(j):
        return pl.ds(j * step_rows, step_rows)

    line_barrier(n, place, core, bool(groups) or spreading)
    lag = LINE_LAG if reduce else 0
    turns = chunks * max(n_part, 1) + lag + n
    plan = [[] for _ in range(turns)]
    if fetching:
        start_turns = min(LINE_START_TURNS, chunks) if reduce else 1
        from_turn = LINE_FROM_TURN if reduce else 1
        own_start, plan, settle = fetch_steps(
            n, place, groups, weights, fetched, fetch_sems, turns, start_turns, from_turn
        )
    if fetching:
        own_start()
    if spreading:
        begin, plan, settle = spread_steps(
            n, pieces, spread_out, spread_sems, turns, LINE_FROM_TURN
        )
        begin()
    if giving:
        begin, plan, settle = give_steps(
            n, place, groups, grads, given, give_bufs, give_sems, turns, LINE_GIVE_TURN, deliver
        )
        begin()

    def cross(j):
        return line_copy(
            parts[j // chunks].at[:, 1 - core, rows(j % chunks)],
            across.at[:, rows(j)],
            cross_send.at[j],
            cross_recv.at[j],
            other,
        )

    def own_copy(j):
        return pltpu.make_async_copy(
            parts[j // chunks].at[:, core, rows(j % chunks)], own.at[:, rows(j)], own_sem.at[j]
        )

    def sum_copy(way, k, j):
        return line_copy(
            sums_out.at[way, k, rows(j)],
            sums_in.at[way, k, rows(j)],
            sum_send.at[way, k, j],
            sum_recv.at[way, k, j],
            {"context": place + 1 - 2 * way},
        )

    def own_term(target, j):
        return own[target, rows(j), :].astype(jnp.float32) + across[
            target, rows(j), :
        ].astype(jnp.float32)

    def send_sums(way, j):
        first = place == (n - 1) * way

        @pl.loop(0, n - 1)
        def _(k):
            target = jnp.where(way == 0, n - 1 - k, k)
            passes = jnp.where(way == 0, target - place, place - target) > 0

            @pl.when(passes & jnp.logical_not(first))
            def _():
                sum_copy(way, k, j).wait_recv()

            @pl.when(passes)
            def _():
                came = sums_in[way, k, rows(j), :].astype(jnp.float32)
                value = own_term(target, j) + jnp.where(first, 0.0, came)
                sums_out[way, k, rows(j), :] = value.astype(jnp.bfloat16)
                sum_copy(way, k, j).start()

    def row_copy(way, k, j, w=0):
        block = place - k if way == 0 else place + k
        device = {"context": place + 1 if way == 0 else place - 1}
        ref = gathered_all[w].at[block, core, rows(j)]
        return line_copy(ref, ref, row_send.at[w, way, k, j], row_recv.at[w, way, k, j], device)

    def row_arrival(way, k, j, w=0):
        block = place - 1 - k if way == 0 else place + 1 + k
        ref = gathered_all[w].at[block, core, rows(j)]
        return line_copy(ref, ref, row_send.at[w, way, k, j], row_recv.at[w, way, k, j], other)

    def pair_copy(block, half, j, w=0):
        ref = gathered_all[w].at[block, half, rows(j)]
        return line_copy(ref, ref, pair_send.at[w, block, j], pair_recv.at[w, block, j], other)

    def send_rows(j, values, w=0):
        gathered_all[w][place, core, rows(j), :] = values

        @pl.when(place < n - 1)
        def _():
            row_copy(0, 0, j, w).start()

        @pl.when(place > 0)
        def _():
            row_copy(1, 0, j, w).start()

        pair_copy(place, core, j, w).start()

    def finish_rows(j):
        total = None
        if reduce:

            summed[...] = own_term(place, j)

            @pl.when(place > 0)
            def _():
                sum_copy(0, n - 1 - place, j).wait_recv()
                summed[...] += sums_in[0, n - 1 - place, rows(j), :].astype(jnp.float32)

            @pl.when(place < n - 1)
            def _():
                sum_copy(1, place, j).wait_recv()
                summed[...] += sums_in[1, place, rows(j), :].astype(jnp.float32)

            total = summed[...]
        made = finish(j, rows(j % chunks), total, ins, rest)
        made = made if isinstance(made, tuple) else (made,)
        made = list(made)
        if gather and j < chunks:
            send_rows(j, made.pop(0))
        if made:
            i = j // chunks - (gather > 0)
            joined[i][core, rows(j % chunks), :] = made.pop(0)
            join_copy(i, core, j % chunks).start()

    def join_copy(i, half, j):
        ref = joined[i].at[half, rows(j)]
        return line_copy(ref, ref, join_send.at[i, j], join_recv.at[i, j], other)

    def pass_rows(k, j, w=0):
        for way in (0, 1):
            block = place - 1 - k if way == 0 else place + 1 + k
            here = block >= 0 if way == 0 else block <= n - 1
            onward = place < n - 1 if way == 0 else place > 0

            @pl.when(here)
            def _(way=way, block=block):
                row_arrival(way, k, j, w).wait_recv()

            if k + 1 <= n - 2:

                @pl.when(here & onward)
                def _(way=way):
                    row_copy(way, k + 1, j, w).start()

            @pl.when(here)
            def _(way=way, block=block):
                pair_copy(block, core, j, w).start()

    all_chunks = chunks * max(n_part, 1)
    if reduce:
        for j in range(all_chunks):
            cross(j).start()
            own_copy(j).start()

    def gains_plan():
        group = lax.axis_index("fsdp")
        hops = (
            other,
            {"fsdp": jnp.bitwise_xor(group, 1)},
            {"fsdp": jnp.bitwise_xor(group, 2)},
        )

        def hop(h):
            return line_copy(
                gain_own.at[h], gain_came.at[h], gain_send.at[h], gain_recv.at[h], hops[h]
            )

        def line_hop(s):
            return line_copy(
                gain_line.at[place],
                gain_line.at[place],
                gain_line_send.at[s - 1],
                gain_line_recv.at[s - 1],
                {"context": lax.rem(place + s, n)},
            )

        def line_hop_in(s):
            ref = gain_line.at[lax.rem(place + n - s, n)]
            return line_copy(
                ref, ref, gain_line_send.at[s - 1], gain_line_recv.at[s - 1], other
            )

        def first():
            gain_own[0] = others[...]
            hop(0).start()

        def next_hop(h):
            def step():
                hop(h).wait_recv()
                value = gain_own[h] + gain_came[h]
                if h < 2:
                    gain_own[h + 1] = value
                    hop(h + 1).start()
                else:
                    gain_line[place] = value
                    for s in range(1, n):
                        line_hop(s).start()

            return step

        def last():
            for s in range(1, n):
                line_hop_in(s).wait_recv()
            value = gain_line[0]
            for p in range(1, n):
                value = value + gain_line[p]
            gains_out[...] = value
            for h in range(3):
                hop(h).wait_send()
            for s in range(1, n):
                line_hop(s).wait_send()

        return [first, next_hop(0), next_hop(1), next_hop(2), last]

    near = jnp.where(place < n // 2, 0, 1)
    gain_steps = gains_plan() if extra else []
    if not reduce:
        for j in range(chunks):
            finish_rows(j)
    for i in range(turns):
        for step in plan[i]:
            step()
        if gather > 1 and 0 <= i - LINE_PLAIN_FROM < chunks:
            j = i - LINE_PLAIN_FROM
            send_rows(j, ins[-1][rows(j), :], 1)
        if reduce and i < all_chunks:
            own_copy(i).wait()
            cross(i).wait_recv()
            send_sums(near, i)
        if reduce and 0 <= i - 1 < all_chunks:
            send_sums(1 - near, i - 1)
        if reduce and 0 <= i - lag < all_chunks:
            finish_rows(i - lag)
        if i > 0 and gain_steps:
            gain_steps.pop(0)()
        if gather:
            for k in range(n - 1):
                if 0 <= i - lag - 1 - k < chunks:
                    pass_rows(k, i - lag - 1 - k)
                if gather > 1 and 0 <= i - LINE_PLAIN_LAG - k * LINE_PLAIN_STEP < chunks:
                    pass_rows(k, i - LINE_PLAIN_LAG - k * LINE_PLAIN_STEP, 1)

    for step in gain_steps:
        step()
    if gather > 1:
        for i in range(turns, turns + LINE_PLAIN_LAG + (n - 2) * LINE_PLAIN_STEP):
            for k in range(n - 1):
                if 0 <= i - LINE_PLAIN_LAG - k * LINE_PLAIN_STEP < chunks:
                    pass_rows(k, i - LINE_PLAIN_LAG - k * LINE_PLAIN_STEP, 1)
    if groups or spreading:
        settle()
    for j in range(all_chunks):
        if reduce:
            cross(j).wait_send()
            for k in range(n - 1):

                @pl.when(place < n - 1 - k)
                def _(k=k, j=j):
                    sum_copy(0, k, j).wait_send()

                @pl.when(place > k)
                def _(k=k, j=j):
                    sum_copy(1, k, j).wait_send()

        for w in range(gather if j < chunks else 0):
            for block in range(n):
                pair_copy(block, 1 - core, j, w).wait_recv()
                pair_copy(block, core, j, w).wait_send()
            for k in range(n - 1):

                @pl.when((place < n - 1) & (place >= k))
                def _(k=k, j=j, w=w):
                    row_copy(0, k, j, w).wait_send()

                @pl.when((place > 0) & (place + k <= n - 1))
                def _(k=k, j=j, w=w):
                    row_copy(1, k, j, w).wait_send()

        i = j // chunks - (gather > 0)
        if n_join and i >= 0:
            join_copy(i, 1 - core, j % chunks).wait_recv()
            join_copy(i, core, j % chunks).wait_send()


def line_call(
    n,
    collective,
    finish,
    part,
    ins,
    gather=0,
    joins=(),
    rests=(),
    chunks=LINE_CHUNKS,
    groups=(),
    weights=(),
    grads=(),
    deliver=True,
    extra=None,
    pieces=None,
):
    parts = () if part is None else part if isinstance(part, tuple) else (part,)
    reduce = len(parts) > 0
    giving = len(grads) > 0
    row_count, model_width = ins[0].shape
    vmem = pl.BlockSpec(memory_space=pltpu.VMEM)
    outs = []
    for _ in range(gather):
        outs.append(jax.ShapeDtypeStruct((n, 2, row_count, model_width), jnp.bfloat16))
    outs += [jax.ShapeDtypeStruct((2, row_count, model_width), kind) for kind in joins]
    outs += list(rests)
    out_specs = [vmem] * len(outs)
    for members in groups if not giving else ():
        rows = weights[0].shape[0] * n * lax.axis_size("fsdp")
        width = sum(weights[a].shape[1] for a in members) // n
        outs.append(jax.ShapeDtypeStruct((rows, width), jnp.bfloat16))
        out_specs.append(pl.BlockSpec(memory_space=pl.ANY))
    dma = pltpu.SemaphoreType.DMA
    if pieces is not None:
        rows = pieces.shape[0] * pieces.shape[1] * lax.axis_size("fsdp")
        outs.append(jax.ShapeDtypeStruct((rows, pieces.shape[2]), jnp.bfloat16))
        out_specs.append(pl.BlockSpec(memory_space=pl.ANY))
    if giving:
        owned = grads[0].shape[0] // (n * lax.axis_size("fsdp"))
        shapes = [(owned, width * n) for width in weights]
        if not deliver:
            shapes = [(n, owned, sum(grad.shape[1] for grad in grads))]
        for shape in shapes:
            outs.append(jax.ShapeDtypeStruct(shape, jnp.bfloat16))
            out_specs.append(vmem)
    if extra is not None:
        outs.append(jax.ShapeDtypeStruct(extra.shape, jnp.float32))
        out_specs.append(vmem)
    total_chunks = chunks * max(len(parts), 1)
    sum_rows = row_count * max(len(parts), 1)
    scratch = []
    if reduce:
        slot = pltpu.VMEM((2, n - 1, sum_rows, model_width), jnp.bfloat16)
        scratch += [pltpu.VMEM((n, sum_rows, model_width), jnp.bfloat16), dma((total_chunks,))]
        scratch += [pltpu.VMEM((n, sum_rows, model_width), jnp.bfloat16), slot, slot]
        scratch += [pltpu.VMEM((row_count // chunks, model_width), jnp.float32)]
        tally = (2, n - 1, total_chunks)
        scratch += [dma((total_chunks,)), dma((total_chunks,)), dma(tally), dma(tally)]
    if gather:
        tally = (gather, 2, n - 1, chunks)
        scratch += [dma(tally), dma(tally), dma((gather, n, chunks)), dma((gather, n, chunks))]
    if joins:
        scratch += [dma((len(joins), chunks)), dma((len(joins), chunks))]
    if groups and not giving:
        arrays = len(weights)
        tally = (2, len(groups), n)
        scratch += [dma((arrays,)), dma((arrays, n)), dma((arrays, n))]
        scratch += [dma(tally), dma(tally), dma(tally), dma(tally)]
    if pieces is not None:
        scratch += [dma((n,))] + [dma((2, n))] * 4
    if giving:
        for grad in grads:
            halves = (owned // 2, grad.shape[1])
            for lead in ((n, 2, 2), (n, 2, 2), (n, 2), (n, 2)):
                scratch.append(pltpu.VMEM(lead + halves, jnp.bfloat16))
            if deliver:
                scratch.append(pltpu.VMEM((n - 1, owned, grad.shape[1]), jnp.bfloat16))
        count = len(groups)
        scratch += [dma((count, n, 2, 2)), dma((count, n, 2, 2))]
        scratch += [dma((count, n, 2)), dma((count, n, 2))]
        scratch += [dma((len(weights), n)), dma((len(weights), n)), dma((count, n, 2, 2))]
    if extra is not None:
        stack = pltpu.VMEM((3,) + extra.shape, jnp.float32)
        scratch += [stack, stack, pltpu.VMEM((n,) + extra.shape, jnp.float32)]
        scratch += [dma((3,)), dma((3,)), dma((n - 1,)), dma((n - 1,))]
    operands = list(parts) + list(ins) + (list(grads) if giving else list(weights))
    operands += [] if extra is None else [extra]
    operands += [] if pieces is None else [pieces]
    anywhere = [*parts, *grads]
    in_specs = [
        pl.BlockSpec(memory_space=pl.ANY) if any(a is b for b in anywhere) else vmem
        for a in operands
    ]
    moved = row_count * model_width * 2 * n * (2 * reduce + 2 * gather)
    return pl.pallas_call(
        functools.partial(
            line_body,
            n,
            chunks,
            len(parts),
            gather,
            pieces is not None,
            len(ins),
            len(joins),
            len(rests),
            groups,
            giving,
            deliver,
            extra is not None,
            finish,
        ),
        out_shape=tuple(outs),
        in_specs=in_specs,
        out_specs=tuple(out_specs),
        scratch_shapes=scratch,
        compiler_params=pltpu.CompilerParams(
            collective_id=collective, has_side_effects=True, vmem_limit_bytes=56 << 20
        ),
        cost_estimate=pl.CostEstimate(
            flops=moved, bytes_accessed=20 * moved, transcendentals=0
        ),
    )(*operands)


def finish_gather(j, rows, total, ins, rest):
    values = ins[0][rows, :].astype(jnp.float32)
    return (values * rms_scale(values) * ins[1][...]).astype(jnp.bfloat16)


def finish_attention(j, rows, total, ins, rest):
    residual = ins[0][rows, :].astype(jnp.float32) + total
    rest[0][rows, :] = residual
    return (residual * rms_scale(residual) * ins[1][...]).astype(jnp.bfloat16)


def gain_rows(j, rest, terms):
    sums = jnp.sum(terms, axis=0, keepdims=True)
    rest[...] = sums if j == 0 else rest[...] + sums


def finish_mlp_back(j, rows, total, ins, rest):
    residual = ins[0][rows, :]
    if j >= LINE_CHUNKS:
        return (residual + total).astype(jnp.bfloat16)
    scale = rms_scale(residual)
    hat = residual * scale
    grad = ins[1][rows, :].astype(jnp.float32) + norm_back(total, hat, scale, ins[2][...])
    rest[0][rows, :] = grad
    gain_rows(j, rest[1], total * hat)
    return grad.astype(jnp.bfloat16)


def finish_tokens(j, rows, total, ins, rest):
    values = ins[1][rows, :].astype(jnp.float32)
    scale = rms_scale(values)
    hat = values * scale
    return ins[0][rows, :] + norm_back(total, hat, scale, ins[2][...])


def permuted_tokens(rows):
    n = lax.axis_size("context")
    place = lax.axis_index("context")
    core = lax.axis_index("tensor")
    shape = rows.shape
    near = jnp.zeros((n,) + shape, rows.dtype)
    for s in range(n):
        ring = [(i, (i + s) % n) for i in range(n)]
        came = lax.ppermute(rows, "context", ring) if s else rows
        near = lax.dynamic_update_slice(near, came[None], (lax.rem(place + n - s, n), 0, 0))
    far = lax.ppermute(near, "tensor", [(0, 1), (1, 0)])
    both = jnp.zeros((n, 2) + shape, rows.dtype)
    both = lax.dynamic_update_slice(both, near[:, None], (0, core, 0, 0))
    both = lax.dynamic_update_slice(both, far[:, None], (0, 1 - core, 0, 0))
    return both.reshape(n * 2 * shape[0], shape[1])


def widen_body(h_cols, out, tokens, mlp, *refs):
    attn, results = refs[:4], refs[4:]
    results[0][...] = out[...]
    results[1][...] = tokens[...]
    for a in range(4):
        results[2 + a][...] = attn[a][...].astype(jnp.float32)
    for a in range(3):
        results[6 + a][...] = mlp[0, :, a * h_cols : (a + 1) * h_cols].astype(jnp.float32)


def widen(parts, h_cols, out, tokens, mlp, *attn):
    rows = mlp.shape[1]
    width = out.shape[-1]
    out, tokens = out.reshape(-1, width), tokens.reshape(-1, width)
    token_rows = pl.BlockSpec((out.shape[0] // parts, width), lambda i: (i, 0))
    quarters = [pl.BlockSpec((rows, a.shape[1] // parts), lambda i: (0, i)) for a in attn]
    hidden = pl.BlockSpec((rows, h_cols), lambda i: (0, i))
    results = [jax.ShapeDtypeStruct(a.shape, a.dtype) for a in (out, tokens)]
    results += [jax.ShapeDtypeStruct(a.shape, jnp.float32) for a in attn]
    results += [jax.ShapeDtypeStruct((rows, h_cols * parts), jnp.float32)] * 3
    return pl.pallas_call(
        functools.partial(widen_body, h_cols),
        grid=(parts,),
        in_specs=[token_rows, token_rows, pl.BlockSpec((1,) + mlp.shape[1:], lambda i: (i, 0, 0))]
        + quarters,
        out_specs=tuple([token_rows, token_rows] + quarters + [hidden] * 3),
        out_shape=tuple(results),
        name="widen",
    )(out, tokens, mlp, *attn)


def token_half(block, index, parts):
    rows = block.shape[0] // parts
    return lax.dynamic_slice_in_dim(block, index * rows, rows, axis=0)


def line_shards(
    tokens,
    cotangent,
    norm_gain_attn,
    norm_gain_mlp,
    head_gains,
    query_weight,
    key_matrix,
    value_matrix,
    output_weight,
    gate_weight,
    up_weight,
    down_weight,
):
    _, local_len, model_width = tokens.shape
    parts = lax.axis_size("context")
    cores = lax.axis_size("tensor")
    core = lax.axis_index("tensor")
    full_len = local_len * parts
    q_cols = query_weight.shape[1] // parts
    kv_cols = key_matrix.shape[1] // parts
    h_cols = gate_weight.shape[1] // parts
    q_heads = q_cols // HEAD_DIM
    kv_heads = kv_cols // HEAD_DIM
    head_group = q_heads // kv_heads
    score_scale = 1.0 / math.sqrt(HEAD_DIM)
    positions = jnp.arange(full_len, dtype=jnp.int32)
    cosine_table, sine_table = rope_tables(positions, HEAD_DIM)
    cosine_table = cosine_table[:, None, :]
    sine_table = sine_table[:, None, :]
    visible = positions[None, :] <= positions[:, None]
    gain_attn = norm_gain_attn.astype(jnp.float32)[None]
    gain_mlp = norm_gain_mlp.astype(jnp.float32)[None]
    gain_heads = head_gains.astype(jnp.float32)

    def line_parts(left, right):
        product = column_product(left, right).astype(jnp.bfloat16)
        return product.reshape(parts, cores, half_len, model_width)

    own_cot = token_half(cotangent.reshape(local_len, model_width), core, cores)
    inputs = token_half(tokens.reshape(local_len, model_width), core, cores)
    half_len = local_len // cores
    rows_f32 = jax.ShapeDtypeStruct((half_len, model_width), jnp.float32)
    sums_f32 = jax.ShapeDtypeStruct((1, model_width), jnp.float32)
    normed_attn, in_weights, out_weights = line_call(
        parts,
        1,
        finish_gather,
        None,
        (inputs, gain_attn),
        gather=1,
        groups=((0, 1, 2), (3,)),
        weights=(query_weight, key_matrix, value_matrix, output_weight),
    )
    normed_attn = normed_attn.reshape(full_len, model_width)
    own_cot, normed_attn = lax.optimization_barrier((own_cot, normed_attn))
    grad_out = permuted_tokens(own_cot)

    raw = jnp.dot(normed_attn, in_weights, preferred_element_type=jnp.float32)
    query_split = raw[:, :q_cols].reshape(full_len, q_heads, HEAD_DIM)
    query_scale = rms_scale(query_split)
    query_hat = query_split * query_scale
    queries = rotate(query_hat * gain_heads[0], cosine_table, sine_table).astype(jnp.bfloat16)
    key_split = raw[:, q_cols : q_cols + kv_cols].reshape(full_len, kv_heads, HEAD_DIM)
    key_scale = rms_scale(key_split)
    key_hat = key_split * key_scale
    keys = rotate(key_hat * gain_heads[1], cosine_table, sine_table).astype(jnp.bfloat16)
    values = raw[:, q_cols + kv_cols :].astype(jnp.bfloat16).reshape(full_len, kv_heads, HEAD_DIM)
    queries = queries.reshape(full_len, kv_heads, head_group, HEAD_DIM)

    scores = (
        jnp.einsum("ikgd,jkd->kgij", queries, keys, preferred_element_type=jnp.float32)
        * score_scale
    )
    weights = jnp.where(visible, jnp.exp(scores), 0.0)
    probs = weights / jnp.sum(weights, axis=-1, keepdims=True)
    probs_low = probs.astype(jnp.bfloat16)
    attended = (
        jnp.einsum("kgij,jkd->ikgd", probs_low, values, preferred_element_type=jnp.float32)
        .astype(jnp.bfloat16)
        .reshape(full_len, q_cols)
    )
    normed_mlp, residual, mlp_in, mlp_down = line_call(
        parts,
        2,
        finish_attention,
        line_parts(attended, out_weights),
        (inputs, gain_mlp),
        gather=1,
        rests=(rows_f32,),
        groups=((0, 1), (2,)),
        weights=(gate_weight, up_weight, down_weight),
    )
    normed_mlp = normed_mlp.reshape(full_len, model_width)

    both = jnp.dot(normed_mlp, mlp_in, preferred_element_type=jnp.float32)
    gate_act = both[:, :h_cols]
    upward = both[:, h_cols:]
    sig_gate = jax.nn.sigmoid(gate_act)
    activated = gate_act * sig_gate
    hidden = (activated * upward).astype(jnp.bfloat16)
    grad_hidden = jnp.dot(grad_out, mlp_down, preferred_element_type=jnp.float32)
    derivative = sig_gate * (1.0 + gate_act * (1.0 - sig_gate))
    grad_gate = (grad_hidden * upward * derivative).astype(jnp.bfloat16)
    grad_up = (grad_hidden * activated).astype(jnp.bfloat16)
    grad_both = jnp.concatenate([grad_gate, grad_up], axis=1)
    grad_in = row_product(normed_mlp, grad_both).astype(jnp.bfloat16)
    grad_down = row_product(grad_out, hidden).astype(jnp.bfloat16)
    grad_branch, out, grad_residual, gain_mlp_part, mlp_grads = line_call(
        parts,
        3,
        finish_mlp_back,
        (line_parts(grad_both, mlp_in), line_parts(hidden, mlp_down)),
        (residual, own_cot, gain_mlp),
        gather=1,
        joins=(jnp.bfloat16,),
        rests=(rows_f32, sums_f32),
        groups=((0, 1), (2,)),
        weights=(h_cols, h_cols, h_cols),
        grads=(grad_in, grad_down),
        deliver=False,
    )
    mlp_grads = lax.all_to_all(mlp_grads, "context", split_axis=0, concat_axis=0, tiled=True)
    grad_branch = grad_branch.reshape(full_len, model_width)
    grad_attended = jnp.dot(grad_branch, out_weights, preferred_element_type=jnp.float32)
    grad_attended = grad_attended.astype(jnp.bfloat16)
    grad_attended = grad_attended.reshape(full_len, kv_heads, head_group, HEAD_DIM)
    grad_probs = jnp.einsum(
        "ikgd,jkd->kgij", grad_attended, values, preferred_element_type=jnp.float32
    )
    delta = jnp.sum(probs * grad_probs, axis=-1, keepdims=True)
    grad_scores = (probs * (grad_probs - delta)).astype(jnp.bfloat16)
    grad_queries = (
        jnp.einsum("kgij,jkd->ikgd", grad_scores, keys, preferred_element_type=jnp.float32)
        * score_scale
    ).reshape(full_len, q_heads, HEAD_DIM)
    grad_keys = (
        jnp.einsum("kgij,ikgd->jkd", grad_scores, queries, preferred_element_type=jnp.float32)
        * score_scale
    )
    grad_values = jnp.einsum(
        "kgij,ikgd->jkd", probs_low, grad_attended, preferred_element_type=jnp.float32
    )
    grad_query_hat = unrotate(grad_queries, cosine_table, sine_table)
    grad_key_hat = unrotate(grad_keys, cosine_table, sine_table)
    heads_part = jnp.stack(
        [
            jnp.sum(grad_query_hat * query_hat, axis=(0, 1)),
            jnp.sum(grad_key_hat * key_hat, axis=(0, 1)),
        ]
    )
    grad_raw = jnp.concatenate(
        [
            norm_back(grad_query_hat, query_hat, query_scale, gain_heads[0]).reshape(
                full_len, q_cols
            ),
            norm_back(grad_key_hat, key_hat, key_scale, gain_heads[1]).reshape(full_len, kv_cols),
            grad_values.reshape(full_len, kv_cols),
        ],
        axis=1,
    ).astype(jnp.bfloat16)
    attn_in_grad = row_product(normed_attn, grad_raw).astype(jnp.bfloat16)
    attn_out_grad = row_product(grad_branch, attended).astype(jnp.bfloat16)
    gain_attn_part = (
        jnp.sum(attn_in_grad.astype(jnp.float32) * in_weights.astype(jnp.float32), axis=1)[None]
        / gain_attn
    )
    gains = jnp.concatenate(
        [
            gain_attn_part,
            gain_mlp_part,
            jnp.pad(heads_part.reshape(1, -1), ((0, 0), (0, model_width - heads_part.size))),
            jnp.zeros((5, model_width), jnp.float32),
        ],
        axis=0,
    )
    grad_tokens, query_grad, key_grad, value_grad, output_grad, totals = line_call(
        parts,
        4,
        finish_tokens,
        line_parts(grad_raw, in_weights),
        (grad_residual, inputs, gain_attn),
        joins=(jnp.float32,),
        groups=((0, 1, 2), (3,)),
        weights=(q_cols, kv_cols, kv_cols, q_cols),
        grads=(attn_in_grad, attn_out_grad),
        extra=gains,
    )
    ready = (out, grad_tokens, mlp_grads, query_grad, key_grad, value_grad, output_grad)
    out, grad_tokens, *weight_grads = widen(parts, h_cols, *ready)
    return (
        out.reshape(tokens.shape),
        grad_tokens.reshape(tokens.shape),
        totals[0],
        totals[1],
        totals[2, : heads_part.size].reshape(heads_part.shape),
        *weight_grads,
    )


def layer(*operands):
    tokens, key_matrix, gate_weight = operands[0], operands[6], operands[9]
    parts = lax.axis_size("context")
    cores = lax.axis_size("tensor")
    fits = (
        tokens.shape[0] == 1
        and key_matrix.shape[1] % (parts * HEAD_DIM) == 0
        and gate_weight.shape[1] % (parts * HEAD_DIM) == 0
        and tokens.shape[1] % (cores * LINE_CHUNKS * 16) == 0
        and cores == 2
        and lax.axis_size("fsdp") == 4
    )
    return line_shards(*operands) if fits else shards(*operands)


def solution(mesh):
    return jax.shard_map(
        layer,
        mesh=mesh,
        in_specs=(
            P("fsdp", "context", None),
            P("fsdp", "context", None),
            P(),
            P(),
            P(),
            P(("fsdp", "context"), "tensor"),
            P(("fsdp", "context"), "tensor"),
            P(("fsdp", "context"), "tensor"),
            P(("fsdp", "context"), "tensor"),
            P(("fsdp", "context"), "tensor"),
            P(("fsdp", "context"), "tensor"),
            P(("fsdp", "context"), "tensor"),
        ),
        out_specs=(
            P("fsdp", "context", None),
            P("fsdp", "context", None),
            P(),
            P(),
            P(),
            P(("fsdp", "context"), "tensor"),
            P(("fsdp", "context"), "tensor"),
            P(("fsdp", "context"), "tensor"),
            P(("fsdp", "context"), "tensor"),
            P(("fsdp", "context"), "tensor"),
            P(("fsdp", "context"), "tensor"),
            P(("fsdp", "context"), "tensor"),
        ),
        check_vma=False,
    )
```

```python
import functools
import math

import jax
import jax.numpy as jnp
from jax import lax
from jax.experimental import pallas as pl
from jax.experimental.pallas import tpu as pltpu
from jax.sharding import PartitionSpec as P


HEAD_DIM = 128


EPS = 1e-06
THETA = 1000000.0


def rms_scale(values):
    return lax.rsqrt(jnp.mean(values * values, axis=-1, keepdims=True) + EPS)


def rope_tables(positions, head_size):
    halves = head_size // 2
    inverse = THETA ** (-(jnp.arange(halves, dtype=jnp.float32) * 2.0) / head_size)
    angle = positions[:, None].astype(jnp.float32) * inverse[None, :]
    return (jnp.cos(angle), jnp.sin(angle))


def rotate(values, cosine_table, sine_table):
    halves = values.shape[-1] // 2
    leading = values[..., :halves]
    trailing = values[..., halves:]
    return jnp.concatenate(
        [
            leading * cosine_table - trailing * sine_table,
            trailing * cosine_table + leading * sine_table,
        ],
        axis=-1,
    )


def unrotate(values, cosine_table, sine_table):
    halves = values.shape[-1] // 2
    leading = values[..., :halves]
    trailing = values[..., halves:]
    return jnp.concatenate(
        [
            leading * cosine_table + trailing * sine_table,
            trailing * cosine_table - leading * sine_table,
        ],
        axis=-1,
    )


def norm_back(grad_normed, normed_hat, scale_factor, gain):
    scaled = grad_normed * gain
    return scale_factor * (
        scaled - normed_hat * jnp.mean(normed_hat * scaled, axis=-1, keepdims=True)
    )


def row_product(left, right):
    return lax.dot_general(
        left, right, (((0,), (0,)), ((), ())), preferred_element_type=jnp.float32
    )


def column_product(left, right):
    return lax.dot_general(
        left, right, (((1,), (1,)), ((), ())), preferred_element_type=jnp.float32
    )


def blank(row_total, col_total):
    return jnp.zeros((row_total, col_total), jnp.float32)


def placing(left):

    def place_rows(total, piece, start):
        return column_product(left, piece)

    return place_rows


def adding(left):

    def add_rows(total, piece, start):
        return jnp.dot(left, piece, preferred_element_type=jnp.float32)

    return add_rows


def tensor_total(partial_sum):
    return lax.psum(partial_sum, "tensor")


def owner_rows(term_fn, row_total):
    return lax.psum_scatter(
        term_fn(jnp.int32(0), lax.axis_size(("fsdp", "context")) * row_total),
        ("fsdp", "context"),
        scatter_dimension=0,
        tiled=True,
    )


def shards(
    tokens,
    cotangent,
    norm_gain_attn,
    norm_gain_mlp,
    head_gains,
    query_weight,
    key_matrix,
    value_matrix,
    output_weight,
    gate_weight,
    up_weight,
    down_weight,
):
    seq_count, local_len, model_width = tokens.shape
    row_count = seq_count * local_len
    owned_rows = query_weight.shape[0]
    query_cols = query_weight.shape[1]
    kv_cols = key_matrix.shape[1]
    hidden_cols = gate_weight.shape[1]
    query_heads = query_cols // HEAD_DIM
    kv_heads = kv_cols // HEAD_DIM
    head_group = query_heads // kv_heads
    score_scale = 1.0 / math.sqrt(HEAD_DIM)
    full_len = local_len * lax.axis_size("context")
    query_pos = lax.axis_index("context") * local_len + jnp.arange(local_len, dtype=jnp.int32)
    key_pos = jnp.arange(full_len, dtype=jnp.int32)
    cosine_table, sine_table = rope_tables(query_pos, HEAD_DIM)
    cosine_table = cosine_table[:, None, :]
    sine_table = sine_table[:, None, :]
    visible = key_pos[None, :] <= query_pos[:, None]
    inputs = tokens.reshape(row_count, model_width).astype(jnp.float32)
    grad_out = cotangent.reshape(row_count, model_width)
    gain_attn = norm_gain_attn.astype(jnp.float32)
    gain_mlp = norm_gain_mlp.astype(jnp.float32)
    gain_heads = head_gains.astype(jnp.float32)

    def attn_rows(fold_fn, initial):
        return fold_fn(
            initial,
            (
                lax.all_gather(query_weight, ("fsdp", "context"), axis=0, tiled=True),
                lax.all_gather(key_matrix, ("fsdp", "context"), axis=0, tiled=True),
                lax.all_gather(value_matrix, ("fsdp", "context"), axis=0, tiled=True),
            ),
            jnp.int32(0),
        )

    def attn_out_rows(fold_fn, initial):
        return fold_fn(
            initial,
            lax.all_gather(output_weight, ("fsdp", "context"), axis=0, tiled=True),
            jnp.int32(0),
        )

    def mlp_rows(fold_fn, initial):
        return fold_fn(
            initial,
            (
                lax.all_gather(gate_weight, ("fsdp", "context"), axis=0, tiled=True),
                lax.all_gather(up_weight, ("fsdp", "context"), axis=0, tiled=True),
            ),
            jnp.int32(0),
        )

    def down_rows(fold_fn, initial):
        return fold_fn(
            initial,
            lax.all_gather(down_weight, ("fsdp", "context"), axis=0, tiled=True),
            jnp.int32(0),
        )

    scale_attn = rms_scale(inputs)
    hat_attn = inputs * scale_attn
    normed_attn = (hat_attn * gain_attn).astype(jnp.bfloat16)

    def project_in(totals, pieces, start):
        return (
            jnp.dot(normed_attn, pieces[0], preferred_element_type=jnp.float32),
            jnp.dot(normed_attn, pieces[1], preferred_element_type=jnp.float32),
            jnp.dot(normed_attn, pieces[2], preferred_element_type=jnp.float32),
        )

    query_raw, key_unrotated, value_raw = attn_rows(
        project_in,
        (blank(row_count, query_cols), blank(row_count, kv_cols), blank(row_count, kv_cols)),
    )
    query_split = query_raw.reshape(seq_count, local_len, query_heads, HEAD_DIM)
    query_scale = rms_scale(query_split)
    query_hat = query_split * query_scale
    query_rows = rotate(query_hat * gain_heads[0], cosine_table, sine_table).astype(jnp.bfloat16)
    key_split = key_unrotated.reshape(seq_count, local_len, kv_heads, HEAD_DIM)
    key_scale = rms_scale(key_split)
    key_hat = key_split * key_scale
    keys_local = rotate(key_hat * gain_heads[1], cosine_table, sine_table).astype(jnp.bfloat16)
    values_local = value_raw.astype(jnp.bfloat16)
    keys_all, value_rows_gathered = (
        lax.all_gather(
            keys_local.reshape(seq_count, local_len, kv_cols), "context", axis=1, tiled=True
        ),
        lax.all_gather(
            values_local.reshape(seq_count, local_len, kv_cols), "context", axis=1, tiled=True
        ),
    )
    query_blocks = query_rows.reshape(
        seq_count, local_len, kv_heads, head_group, HEAD_DIM
    ).transpose(2, 0, 1, 3, 4)
    key_blocks = keys_all.reshape(seq_count, full_len, kv_heads, HEAD_DIM).transpose(2, 0, 1, 3)
    value_blocks = value_rows_gathered.reshape(seq_count, full_len, kv_heads, HEAD_DIM).transpose(
        2, 0, 1, 3
    )

    def attend(operands):
        query_block, key_block, value_block = operands
        scores = (
            jnp.einsum("bigd,bjd->bgij", query_block, key_block, preferred_element_type=jnp.float32)
            * score_scale
        )
        weights = jnp.where(visible, jnp.exp(scores), 0.0)
        totals = jnp.sum(weights, axis=-1)
        probs_low = (weights / totals[..., None]).astype(jnp.bfloat16)
        mixed_heads = jnp.einsum(
            "bgij,bjd->bigd", probs_low, value_block, preferred_element_type=jnp.float32
        )
        return (mixed_heads.astype(jnp.bfloat16), jnp.log(totals))

    mixed_all, log_totals = lax.map(attend, (query_blocks, key_blocks, value_blocks))
    attended = mixed_all.transpose(1, 2, 0, 3, 4).reshape(row_count, query_cols)
    attn_part = attn_out_rows(placing(attended), blank(row_count, model_width))
    residual = inputs + tensor_total(attn_part)
    scale_mlp = rms_scale(residual)
    hat_mlp = residual * scale_mlp
    normed_mlp = (hat_mlp * gain_mlp).astype(jnp.bfloat16)

    def project_mlp(totals, pieces, start):
        return (
            jnp.dot(normed_mlp, pieces[0], preferred_element_type=jnp.float32),
            jnp.dot(normed_mlp, pieces[1], preferred_element_type=jnp.float32),
        )

    gate_act, upward = mlp_rows(
        project_mlp, (blank(row_count, hidden_cols), blank(row_count, hidden_cols))
    )
    sig_gate = jax.nn.sigmoid(gate_act)
    activated = gate_act * sig_gate
    hidden = (activated * upward).astype(jnp.bfloat16)
    mlp_part = down_rows(placing(hidden), blank(row_count, model_width))
    result = residual + tensor_total(mlp_part)
    out = result.astype(jnp.bfloat16).reshape(seq_count, local_len, model_width)
    grad_hidden = down_rows(adding(grad_out), blank(row_count, hidden_cols))
    derivative = sig_gate * (1.0 + gate_act * (1.0 - sig_gate))
    grad_gate = (grad_hidden * upward * derivative).astype(jnp.bfloat16)
    grad_up = (grad_hidden * activated).astype(jnp.bfloat16)

    def gate_back(total, pieces, start):
        part_sum = column_product(grad_gate, pieces[0]) + column_product(grad_up, pieces[1])
        return part_sum

    grad_normed_mlp = tensor_total(mlp_rows(gate_back, blank(row_count, model_width)))

    def mlp_terms(start, span_rows):
        return jnp.concatenate(
            [
                row_product(normed_mlp, grad_gate),
                row_product(normed_mlp, grad_up),
                row_product(grad_out, hidden),
            ],
            axis=1,
        )

    mlp_grads = owner_rows(mlp_terms, owned_rows)
    grad_gain_mlp = jnp.sum(grad_normed_mlp * hat_mlp, axis=0)
    grad_residual = grad_out.astype(jnp.float32) + norm_back(
        grad_normed_mlp, hat_mlp, scale_mlp, gain_mlp
    )
    grad_branch = grad_residual.astype(jnp.bfloat16)
    grad_attended = attn_out_rows(adding(grad_branch), blank(row_count, query_cols))
    grad_attended_low = grad_attended.astype(jnp.bfloat16)
    grad_blocks = grad_attended_low.reshape(
        seq_count, local_len, kv_heads, head_group, HEAD_DIM
    ).transpose(2, 0, 1, 3, 4)

    def attend_back(operands):
        query_block, key_block, value_block, grad_block, log_total = operands
        scores = (
            jnp.einsum("bigd,bjd->bgij", query_block, key_block, preferred_element_type=jnp.float32)
            * score_scale
        )
        probs = jnp.where(visible, jnp.exp(scores - log_total[..., None]), 0.0)
        probs_low = probs.astype(jnp.bfloat16)
        grad_probs = jnp.einsum(
            "bigd,bjd->bgij", grad_block, value_block, preferred_element_type=jnp.float32
        )
        delta = jnp.sum(probs * grad_probs, axis=-1, keepdims=True)
        grad_scores = (probs * (grad_probs - delta)).astype(jnp.bfloat16)
        grad_query = (
            jnp.einsum("bgij,bjd->bigd", grad_scores, key_block, preferred_element_type=jnp.float32)
            * score_scale
        )
        grad_key = (
            jnp.einsum(
                "bgij,bigd->bjd", grad_scores, query_block, preferred_element_type=jnp.float32
            )
            * score_scale
        )
        grad_value = jnp.einsum(
            "bgij,bigd->bjd", probs_low, grad_block, preferred_element_type=jnp.float32
        )
        return (grad_query, grad_key, grad_value, delta[..., 0])

    grad_query_all, grad_key_all, grad_value_all, _ = lax.map(
        attend_back, (query_blocks, key_blocks, value_blocks, grad_blocks, log_totals)
    )
    grad_key_full = grad_key_all.transpose(1, 2, 0, 3).reshape(seq_count, full_len, kv_cols)
    grad_value_full = grad_value_all.transpose(1, 2, 0, 3).reshape(seq_count, full_len, kv_cols)
    grad_key_own, grad_value_own = (
        lax.psum_scatter(
            grad_key_full.astype(jnp.bfloat16), "context", scatter_dimension=1, tiled=True
        ).astype(jnp.float32),
        lax.psum_scatter(
            grad_value_full.astype(jnp.bfloat16), "context", scatter_dimension=1, tiled=True
        ).astype(jnp.float32),
    )
    grad_query_rot = grad_query_all.transpose(1, 2, 0, 3, 4).reshape(
        seq_count, local_len, query_heads, HEAD_DIM
    )
    grad_query_hat = unrotate(grad_query_rot, cosine_table, sine_table)
    grad_key_hat = unrotate(
        grad_key_own.reshape(seq_count, local_len, kv_heads, HEAD_DIM), cosine_table, sine_table
    )
    grad_gain_query = jnp.sum(grad_query_hat * query_hat, axis=(0, 1, 2))
    grad_gain_key = jnp.sum(grad_key_hat * key_hat, axis=(0, 1, 2))
    grad_query_raw = (
        norm_back(grad_query_hat, query_hat, query_scale, gain_heads[0])
        .reshape(row_count, query_cols)
        .astype(jnp.bfloat16)
    )
    grad_key_raw = (
        norm_back(grad_key_hat, key_hat, key_scale, gain_heads[1])
        .reshape(row_count, kv_cols)
        .astype(jnp.bfloat16)
    )
    grad_value_low = grad_value_own.reshape(row_count, kv_cols).astype(jnp.bfloat16)

    def attn_back(total, pieces, start):
        part_sum = (
            column_product(grad_query_raw, pieces[0])
            + column_product(grad_key_raw, pieces[1])
            + column_product(grad_value_low, pieces[2])
        )
        return part_sum

    grad_normed_part = attn_rows(attn_back, blank(row_count, model_width))
    grad_normed_attn, grad_heads_gain = (
        lax.psum(grad_normed_part.astype(jnp.bfloat16), "tensor").astype(jnp.float32),
        lax.psum(jnp.stack([grad_gain_query, grad_gain_key]).astype(jnp.bfloat16), "tensor").astype(
            jnp.float32
        ),
    )

    def attn_terms(start, span_rows):
        return jnp.concatenate(
            [
                row_product(normed_attn, grad_query_raw),
                row_product(normed_attn, grad_key_raw),
                row_product(normed_attn, grad_value_low),
                row_product(grad_branch, attended),
            ],
            axis=1,
        )

    attn_grads = owner_rows(attn_terms, owned_rows)
    grad_gain_attn = jnp.sum(grad_normed_attn * hat_attn, axis=0)
    grad_tokens = grad_residual + norm_back(grad_normed_attn, hat_attn, scale_attn, gain_attn)
    total_attn, total_mlp, total_heads = lax.psum(
        (grad_gain_attn, grad_gain_mlp, grad_heads_gain), ("fsdp", "context")
    )
    query_grad = attn_grads[:, :query_cols]
    key_grad = attn_grads[:, query_cols : query_cols + kv_cols]
    value_grad = attn_grads[:, query_cols + kv_cols : query_cols + 2 * kv_cols]
    output_grad = attn_grads[:, query_cols + 2 * kv_cols :]
    gate_grad = mlp_grads[:, :hidden_cols]
    up_grad = mlp_grads[:, hidden_cols : 2 * hidden_cols]
    down_grad = mlp_grads[:, 2 * hidden_cols :]
    return (
        out,
        grad_tokens.reshape(seq_count, local_len, model_width),
        total_attn,
        total_mlp,
        total_heads,
        query_grad,
        key_grad,
        value_grad,
        output_grad,
        gate_grad,
        up_grad,
        down_grad,
    )


LINE_CHUNKS = 8
LINE_LAG = 2
LINE_START_TURNS = 1
LINE_FROM_TURN = 1
LINE_PLAIN_FROM = 0
LINE_PLAIN_LAG = 1
LINE_PLAIN_STEP = 1
LINE_GIVE_TURN = 6
MESH = pl.DeviceIdType.MESH


def line_copy(src, dst, send, recv, device):
    return pltpu.make_async_remote_copy(
        src_ref=src,
        dst_ref=dst,
        send_sem=send,
        recv_sem=recv,
        device_id=device,
        device_id_type=MESH,
    )


def line_barrier(n, place, core, fetching):
    barrier = pltpu.get_barrier_semaphore()

    def greet(device):
        pl.semaphore_signal(barrier, inc=1, device_id=device, device_id_type=MESH)

    greet({"tensor": 1 - core})
    if fetching:
        group = lax.axis_index("fsdp")
        greet({"fsdp": jnp.bitwise_xor(group, 1)})
        greet({"fsdp": jnp.bitwise_xor(group, 2)})
        for shift in range(1, n):
            greet({"context": lax.rem(place + shift, n)})
        pl.semaphore_wait(barrier, n + 2)
        return

    @pl.when(place > 0)
    def _():
        greet({"context": place - 1})

    @pl.when(place < n - 1)
    def _():
        greet({"context": place + 1})

    ends = jnp.where(place > 0, 1, 0) + jnp.where(place < n - 1, 1, 0)
    pl.semaphore_wait(barrier, ends + 1)


def nearest(n):
    return [sorted(range(n), key=lambda q: (abs(q - p), q)) for p in range(n)]


def ranked(n, place):
    table = nearest(n)
    return [sum(jnp.where(place == p, table[p][k], 0) for p in range(n)) for k in range(n)]


def fetch_steps(n, place, groups, weights, outs, sems, turns, start_turns, from_turn):
    own_send, line_send, line_recv, near_send, near_recv, far_send, far_recv = sems
    group = lax.axis_index("fsdp")
    rows = weights[0].shape[0]
    neighbours = ({"fsdp": jnp.bitwise_xor(group, 1)}, {"fsdp": jnp.bitwise_xor(group, 2)})
    spans = []
    for g, members in enumerate(groups):
        start = 0
        for a in members:
            width = weights[a].shape[1] // n
            spans.append((a, g, start, width))
            start += width

    def block(out, of_group, at):
        return out.at[pl.ds(pl.multiple_of((of_group * n + at) * rows, rows), rows)]

    order = ranked(n, place)

    def columns(a, at, width):
        return weights[a].at[:, pl.ds(pl.multiple_of(at * width, 128), width)]

    def own_copy(a, g, start, width):
        return pltpu.make_async_copy(
            columns(a, place, width),
            block(outs[g], group, place).at[:, pl.ds(start, width)],
            own_send.at[a],
        )

    def line_move(a, g, start, width, s):
        return line_copy(
            columns(a, order[s], width),
            block(outs[g], group, place).at[:, pl.ds(start, width)],
            line_send.at[a, s],
            line_recv.at[a, place],
            {"context": order[s]},
        )

    def line_arrival(a, g, start, width, s):
        return line_copy(
            columns(a, place, width),
            block(outs[g], group, order[s]).at[:, pl.ds(start, width)],
            line_send.at[a, s],
            line_recv.at[a, order[s]],
            {"context": order[s]},
        )

    def near_copy(way, g, s, of_group):
        piece = block(outs[g], of_group, order[s])
        return line_copy(
            piece, piece, near_send.at[way, g, s], near_recv.at[way, g, s], neighbours[way]
        )

    def far_copy(half, g, s, of_group):
        start = (of_group * n + order[s]) * rows + half * (rows // 2)
        piece = outs[g].at[pl.ds(pl.multiple_of(start, rows // 2), rows // 2)]
        return line_copy(
            piece, piece, far_send.at[half, g, s], far_recv.at[half, g, s], neighbours[1 - half]
        )

    def own_start():
        for span in spans:
            own_copy(*span).start()

    def line_start(span, s):
        return lambda: line_move(*span, s).start()

    def spread(g, s):
        def step():
            for span in spans:
                if span[1] == g:
                    if s == 0:
                        own_copy(*span).wait()
                    else:
                        line_arrival(*span, s).wait_recv()
            near_copy(0, g, s, group).start()
            near_copy(1, g, s, group).start()

        return step

    def pass_on(g, s):
        def step():
            for half in (0, 1):
                source = jnp.bitwise_xor(group, half + 1)
                near_copy(half, g, s, source).wait_recv()
                far_copy(half, g, s, source).start()

        return step

    def settle():
        for g in range(len(groups)):
            for s in range(n):
                for half in (0, 1):
                    far_copy(half, g, s, jnp.bitwise_xor(group, 3)).wait_recv()
                    far_copy(half, g, s, group).wait_send()
                    near_copy(half, g, s, group).wait_send()
        for span in spans:
            for s in range(1, n):
                line_move(*span, s).wait_send()

    issue = [(span, s) for s in range(1, n) for span in spans]
    at_turn = {(span[0], s): i * start_turns // len(issue) for i, (span, s) in enumerate(issue)}
    plan = [[] for _ in range(turns)]
    for span, s in issue:
        plan[at_turn[span[0], s]].append(line_start(span, s))
    table = nearest(n)
    moves = []
    for s in range(n):
        latest = max(table[table[p][s]].index(p) for p in range(n))
        for g in range(len(groups)):
            ready = max(at_turn[a, latest] for a in groups[g]) + 1 if s else 0
            moves.append((ready, spread(g, s)))
        moves += [(0, pass_on(g, s)) for g in range(len(groups))]
    turn = 0
    for i, (ready, step) in enumerate(moves):
        late = max(0, i - len(groups))
        even = from_turn + late * (turns - from_turn) // (len(moves) - len(groups)) if late else 0
        turn = min(max(turn, ready, even), turns - 1)
        plan[turn].append(step)
    return own_start, plan, settle


def piece_rows(count, body):
    @pl.loop(0, count // 16)
    def _(r):
        body(pl.ds(pl.multiple_of(r * 16, 16), 16))


def give_steps(n, place, groups, grads, outs, bufs, sems, turns, from_turn, deliver):
    first_send, first_recv, second_send, second_recv, line_send, line_recv, mine_sem = sems
    group = lax.axis_index("fsdp")
    rows = outs[0].shape[-2]

    half_rows = rows // 2

    far = ranked(n, place)[::-1]

    def part(g, of_group, s, half):
        block = of_group * n + far[s]
        start = pl.multiple_of(block * rows + half * half_rows, half_rows)
        return grads[g].at[pl.ds(start, half_rows)]

    def mine_copy(g, s, half, k):
        target = group if k == 0 else jnp.bitwise_xor(group, 2 - half)
        return pltpu.make_async_copy(
            part(g, target, s, half), bufs[g]["mine"].at[s, half, k], mine_sem.at[g, s, half, k]
        )

    def first_copy(g, s, half, k):
        target = jnp.bitwise_xor(group, half + 1 if k == 0 else 3)
        return line_copy(
            part(g, target, s, half),
            bufs[g]["first"].at[s, half, k],
            first_send.at[g, s, half, k],
            first_recv.at[g, s, half, k],
            {"fsdp": jnp.bitwise_xor(group, half + 1)},
        )

    def second_copy(g, s, half):
        return line_copy(
            bufs[g]["second_out"].at[s, half],
            bufs[g]["second"].at[s, half],
            second_send.at[g, s, half],
            second_recv.at[g, s, half],
            {"fsdp": jnp.bitwise_xor(group, 2 - half)},
        )

    def line_moves(g, s, arrival=False):
        start = 0
        for a in groups[g]:
            width = outs[a].shape[1] // n
            quarter = far[s] if arrival else place
            ref = outs[a].at[:, pl.ds(pl.multiple_of(quarter * width, 128), width)]
            out = bufs[g]["line_out"].at[min(s, n - 2), :, pl.ds(start, width)]
            yield line_copy(
                ref if arrival else out,
                ref,
                line_send.at[a, s],
                line_recv.at[a, quarter],
                {"context": far[s]},
            )
            start += width

    def store(g, at, values):
        start = 0
        for a in groups[g]:
            width = outs[a].shape[1] // n
            cols = pl.ds(pl.multiple_of(place * width, 128), width)
            outs[a][at, cols] = values[:, start : start + width].astype(jnp.bfloat16)
            start += width

    def send_first(g, s):
        for k in (1, 0):
            for half in (0, 1):
                first_copy(g, s, half, k).start()
                mine_copy(g, s, half, k).start()

    def begin():
        for i in range(2 * len(groups)):
            g, s = order[i]
            send_first(g, s)

    def across(i):
        g, s = order[i]

        def step():
            for half in (0, 1):
                first_copy(g, s, half, 1).wait_recv()
                mine_copy(g, s, half, 1).wait()
                own = bufs[g]["mine"].at[s, half, 1]
                came = bufs[g]["first"].at[s, half, 1]
                out = bufs[g]["second_out"].at[s, half]

                def add(at, own=own, came=came, out=out):
                    out[at, :] = (
                        own[at, :].astype(jnp.float32) + came[at, :].astype(jnp.float32)
                    ).astype(jnp.bfloat16)

                piece_rows(half_rows, add)
                second_copy(g, s, half).start()
            if i + 2 * len(groups) < len(order):
                send_first(*order[i + 2 * len(groups)])

        return step

    def total(g, s):
        def step():
            for half in (0, 1):
                first_copy(g, s, half, 0).wait_recv()
                second_copy(g, s, half).wait_recv()
                mine_copy(g, s, half, 0).wait()
                own = bufs[g]["mine"].at[s, half, 0]
                one = bufs[g]["first"].at[s, half, 0]
                two = bufs[g]["second"].at[s, half]

                def add(at, own=own, one=one, two=two, half=half):
                    value = own[at, :].astype(jnp.float32) + one[at, :].astype(jnp.float32)
                    value = value + two[at, :].astype(jnp.float32)
                    to = pl.ds(pl.multiple_of(at.start + half * half_rows, 16), 16)
                    if not deliver:
                        width = value.shape[1]
                        start = sum(grads[h].shape[1] for h in range(g))
                        outs[0][far[s], to, start : start + width] = value.astype(jnp.bfloat16)
                    elif s == n - 1:
                        store(g, to, value)
                    else:
                        bufs[g]["line_out"][s, to, :] = value.astype(jnp.bfloat16)

                piece_rows(half_rows, add)
            if deliver and s < n - 1:
                for move in line_moves(g, s):
                    move.start()

        return step

    def settle():
        for g, s in order:
            for half in (0, 1):
                first_copy(g, s, half, 0).wait_send()
                first_copy(g, s, half, 1).wait_send()
                second_copy(g, s, half).wait_send()
            if deliver and s < n - 1:
                for move in line_moves(g, s):
                    move.wait_send()
                for move in line_moves(g, s, arrival=True):
                    move.wait_recv()

    count = len(groups)
    order = [(g, s) for s in range(n) for g in range(count)]
    steps = []
    for i in range(len(order) + count):
        if i < len(order):
            steps.append(across(i))
        if 0 <= i - count < len(order):
            steps.append(total(*order[i - count]))
    plan = [[] for _ in range(turns)]
    for i, step in enumerate(steps):
        plan[from_turn + i * (turns - from_turn) // len(steps)].append(step)
    return begin, plan, settle


def spread_steps(n, pieces, out, sems, turns, from_turn):
    own_send, near_send, near_recv, far_send, far_recv = sems
    group = lax.axis_index("fsdp")
    rows = pieces.shape[1]
    neighbours = ({"fsdp": jnp.bitwise_xor(group, 1)}, {"fsdp": jnp.bitwise_xor(group, 2)})

    def block(of_group, k, half=None):
        start = (of_group * n + k) * rows
        if half is None:
            return out.at[pl.ds(pl.multiple_of(start, rows), rows)]
        return out.at[pl.ds(pl.multiple_of(start + half * (rows // 2), rows // 2), rows // 2)]

    def own_copy(k):
        return pltpu.make_async_copy(pieces.at[k], block(group, k), own_send.at[k])

    def near_copy(way, k, of_group):
        return line_copy(
            pieces.at[k],
            block(of_group, k),
            near_send.at[way, k],
            near_recv.at[way, k],
            neighbours[way],
        )

    def far_copy(half, k, of_group):
        ref = block(of_group, k, half)
        return line_copy(
            ref, ref, far_send.at[half, k], far_recv.at[half, k], neighbours[1 - half]
        )

    def begin():
        for k in range(n):
            for way in (0, 1):
                near_copy(way, k, group).start()
            own_copy(k).start()

    def pass_on(k):
        def step():
            for half in (0, 1):
                source = jnp.bitwise_xor(group, half + 1)
                near_copy(half, k, source).wait_recv()
                far_copy(half, k, source).start()

        return step

    def settle():
        for k in range(n):
            own_copy(k).wait()
            for half in (0, 1):
                far_copy(half, k, jnp.bitwise_xor(group, 3)).wait_recv()
                far_copy(half, k, group).wait_send()
                near_copy(half, k, group).wait_send()

    plan = [[] for _ in range(turns)]
    for k in range(n):
        plan[from_turn + k * (turns - from_turn) // n].append(pass_on(k))
    return begin, plan, settle


def line_body(n, chunks, n_part, gather, spreading, n_in, n_join, n_rest, groups, giving, deliver, extra, finish, *refs):
    refs = list(refs)
    take = lambda count: [refs.pop(0) for _ in range(count)]
    reduce = n_part > 0
    fetching = bool(groups) and not giving
    arrays = sum(len(members) for members in groups)
    parts = take(n_part)
    ins = take(n_in)
    weights = take(arrays) if fetching else []
    grads = take(len(groups)) if giving else []
    others = take(1)[0] if extra else None
    pieces = take(1)[0] if spreading else None
    gathered_all = take(gather)
    joined = take(n_join)
    rest = take(n_rest)
    fetched = take(len(groups)) if fetching else []
    spread_out = take(1)[0] if spreading else None
    given = take(arrays if deliver else 1) if giving else []
    gains_out = take(1)[0] if extra else None
    if reduce:
        own, own_sem, across, sums_in, sums_out, summed = take(6)
        cross_send, cross_recv, sum_send, sum_recv = take(4)
    if gather:
        row_send, row_recv, pair_send, pair_recv = take(4)
    if n_join:
        join_send, join_recv = take(2)
    fetch_sems = take(7) if fetching else None
    spread_sems = take(5) if spreading else None
    if giving:
        names = ("mine", "first", "second_out", "second", "line_out")[: 5 if deliver else 4]
        give_bufs = [dict(zip(names, take(len(names)))) for _ in groups]
        give_sems = take(7)
    if extra:
        gain_own, gain_came, gain_line, gain_send, gain_recv, gain_line_send, gain_line_recv = take(7)

    place = lax.axis_index("context")
    core = lax.axis_index("tensor")
    other = {"tensor": 1 - core}
    step_rows = (ins[0].shape[0]) // chunks

    def rows(j):
        return pl.ds(j * step_rows, step_rows)

    line_barrier(n, place, core, bool(groups) or spreading)
    lag = LINE_LAG if reduce else 0
    turns = chunks * max(n_part, 1) + lag + n
    plan = [[] for _ in range(turns)]
    if fetching:
        start_turns = min(LINE_START_TURNS, chunks) if reduce else 1
        from_turn = LINE_FROM_TURN if reduce else 1
        own_start, plan, settle = fetch_steps(
            n, place, groups, weights, fetched, fetch_sems, turns, start_turns, from_turn
        )
    if fetching:
        own_start()
    if spreading:
        begin, plan, settle = spread_steps(
            n, pieces, spread_out, spread_sems, turns, LINE_FROM_TURN
        )
        begin()
    if giving:
        begin, plan, settle = give_steps(
            n, place, groups, grads, given, give_bufs, give_sems, turns, LINE_GIVE_TURN, deliver
        )
        begin()

    def cross(j):
        return line_copy(
            parts[j // chunks].at[:, 1 - core, rows(j % chunks)],
            across.at[:, rows(j)],
            cross_send.at[j],
            cross_recv.at[j],
            other,
        )

    def own_copy(j):
        return pltpu.make_async_copy(
            parts[j // chunks].at[:, core, rows(j % chunks)], own.at[:, rows(j)], own_sem.at[j]
        )

    def sum_copy(way, k, j):
        return line_copy(
            sums_out.at[way, k, rows(j)],
            sums_in.at[way, k, rows(j)],
            sum_send.at[way, k, j],
            sum_recv.at[way, k, j],
            {"context": place + 1 - 2 * way},
        )

    def own_term(target, j):
        return own[target, rows(j), :].astype(jnp.float32) + across[
            target, rows(j), :
        ].astype(jnp.float32)

    def send_sums(way, j):
        first = place == (n - 1) * way

        @pl.loop(0, n - 1)
        def _(k):
            target = jnp.where(way == 0, n - 1 - k, k)
            passes = jnp.where(way == 0, target - place, place - target) > 0

            @pl.when(passes & jnp.logical_not(first))
            def _():
                sum_copy(way, k, j).wait_recv()

            @pl.when(passes)
            def _():
                came = sums_in[way, k, rows(j), :].astype(jnp.float32)
                value = own_term(target, j) + jnp.where(first, 0.0, came)
                sums_out[way, k, rows(j), :] = value.astype(jnp.bfloat16)
                sum_copy(way, k, j).start()

    def row_copy(way, k, j, w=0):
        block = place - k if way == 0 else place + k
        device = {"context": place + 1 if way == 0 else place - 1}
        ref = gathered_all[w].at[block, core, rows(j)]
        return line_copy(ref, ref, row_send.at[w, way, k, j], row_recv.at[w, way, k, j], device)

    def row_arrival(way, k, j, w=0):
        block = place - 1 - k if way == 0 else place + 1 + k
        ref = gathered_all[w].at[block, core, rows(j)]
        return line_copy(ref, ref, row_send.at[w, way, k, j], row_recv.at[w, way, k, j], other)

    def pair_copy(block, half, j, w=0):
        ref = gathered_all[w].at[block, half, rows(j)]
        return line_copy(ref, ref, pair_send.at[w, block, j], pair_recv.at[w, block, j], other)

    def send_rows(j, values, w=0):
        gathered_all[w][place, core, rows(j), :] = values

        @pl.when(place < n - 1)
        def _():
            row_copy(0, 0, j, w).start()

        @pl.when(place > 0)
        def _():
            row_copy(1, 0, j, w).start()

        pair_copy(place, core, j, w).start()

    def finish_rows(j):
        total = None
        if reduce:

            summed[...] = own_term(place, j)

            @pl.when(place > 0)
            def _():
                sum_copy(0, n - 1 - place, j).wait_recv()
                summed[...] += sums_in[0, n - 1 - place, rows(j), :].astype(jnp.float32)

            @pl.when(place < n - 1)
            def _():
                sum_copy(1, place, j).wait_recv()
                summed[...] += sums_in[1, place, rows(j), :].astype(jnp.float32)

            total = summed[...]
        made = finish(j, rows(j % chunks), total, ins, rest)
        made = made if isinstance(made, tuple) else (made,)
        made = list(made)
        if gather and j < chunks:
            send_rows(j, made.pop(0))
        if made:
            i = j // chunks - (gather > 0)
            joined[i][core, rows(j % chunks), :] = made.pop(0)
            join_copy(i, core, j % chunks).start()

    def join_copy(i, half, j):
        ref = joined[i].at[half, rows(j)]
        return line_copy(ref, ref, join_send.at[i, j], join_recv.at[i, j], other)

    def pass_rows(k, j, w=0):
        for way in (0, 1):
            block = place - 1 - k if way == 0 else place + 1 + k
            here = block >= 0 if way == 0 else block <= n - 1
            onward = place < n - 1 if way == 0 else place > 0

            @pl.when(here)
            def _(way=way, block=block):
                row_arrival(way, k, j, w).wait_recv()

            if k + 1 <= n - 2:

                @pl.when(here & onward)
                def _(way=way):
                    row_copy(way, k + 1, j, w).start()

            @pl.when(here)
            def _(way=way, block=block):
                pair_copy(block, core, j, w).start()

    all_chunks = chunks * max(n_part, 1)
    if reduce:
        for j in range(all_chunks):
            cross(j).start()
            own_copy(j).start()

    def gains_plan():
        group = lax.axis_index("fsdp")
        hops = (
            other,
            {"fsdp": jnp.bitwise_xor(group, 1)},
            {"fsdp": jnp.bitwise_xor(group, 2)},
        )

        def hop(h):
            return line_copy(
                gain_own.at[h], gain_came.at[h], gain_send.at[h], gain_recv.at[h], hops[h]
            )

        def line_hop(s):
            return line_copy(
                gain_line.at[place],
                gain_line.at[place],
                gain_line_send.at[s - 1],
                gain_line_recv.at[s - 1],
                {"context": lax.rem(place + s, n)},
            )

        def line_hop_in(s):
            ref = gain_line.at[lax.rem(place + n - s, n)]
            return line_copy(
                ref, ref, gain_line_send.at[s - 1], gain_line_recv.at[s - 1], other
            )

        def first():
            gain_own[0] = others[...]
            hop(0).start()

        def next_hop(h):
            def step():
                hop(h).wait_recv()
                value = gain_own[h] + gain_came[h]
                if h < 2:
                    gain_own[h + 1] = value
                    hop(h + 1).start()
                else:
                    gain_line[place] = value
                    for s in range(1, n):
                        line_hop(s).start()

            return step

        def last():
            for s in range(1, n):
                line_hop_in(s).wait_recv()
            value = gain_line[0]
            for p in range(1, n):
                value = value + gain_line[p]
            gains_out[...] = value
            for h in range(3):
                hop(h).wait_send()
            for s in range(1, n):
                line_hop(s).wait_send()

        return [first, next_hop(0), next_hop(1), next_hop(2), last]

    near = jnp.where(place < n // 2, 0, 1)
    gain_steps = gains_plan() if extra else []
    if not reduce:
        for j in range(chunks):
            finish_rows(j)
    for i in range(turns):
        for step in plan[i]:
            step()
        if gather > 1 and 0 <= i - LINE_PLAIN_FROM < chunks:
            j = i - LINE_PLAIN_FROM
            send_rows(j, ins[-1][rows(j), :], 1)
        if reduce and i < all_chunks:
            own_copy(i).wait()
            cross(i).wait_recv()
            send_sums(near, i)
        if reduce and 0 <= i - 1 < all_chunks:
            send_sums(1 - near, i - 1)
        if reduce and 0 <= i - lag < all_chunks:
            finish_rows(i - lag)
        if i > 0 and gain_steps:
            gain_steps.pop(0)()
        if gather:
            for k in range(n - 1):
                if 0 <= i - lag - 1 - k < chunks:
                    pass_rows(k, i - lag - 1 - k)
                if gather > 1 and 0 <= i - LINE_PLAIN_LAG - k * LINE_PLAIN_STEP < chunks:
                    pass_rows(k, i - LINE_PLAIN_LAG - k * LINE_PLAIN_STEP, 1)

    for step in gain_steps:
        step()
    if gather > 1:
        for i in range(turns, turns + LINE_PLAIN_LAG + (n - 2) * LINE_PLAIN_STEP):
            for k in range(n - 1):
                if 0 <= i - LINE_PLAIN_LAG - k * LINE_PLAIN_STEP < chunks:
                    pass_rows(k, i - LINE_PLAIN_LAG - k * LINE_PLAIN_STEP, 1)
    if groups or spreading:
        settle()
    for j in range(all_chunks):
        if reduce:
            cross(j).wait_send()
            for k in range(n - 1):

                @pl.when(place < n - 1 - k)
                def _(k=k, j=j):
                    sum_copy(0, k, j).wait_send()

                @pl.when(place > k)
                def _(k=k, j=j):
                    sum_copy(1, k, j).wait_send()

        for w in range(gather if j < chunks else 0):
            for block in range(n):
                pair_copy(block, 1 - core, j, w).wait_recv()
                pair_copy(block, core, j, w).wait_send()
            for k in range(n - 1):

                @pl.when((place < n - 1) & (place >= k))
                def _(k=k, j=j, w=w):
                    row_copy(0, k, j, w).wait_send()

                @pl.when((place > 0) & (place + k <= n - 1))
                def _(k=k, j=j, w=w):
                    row_copy(1, k, j, w).wait_send()

        i = j // chunks - (gather > 0)
        if n_join and i >= 0:
            join_copy(i, 1 - core, j % chunks).wait_recv()
            join_copy(i, core, j % chunks).wait_send()


def line_call(
    n,
    collective,
    finish,
    part,
    ins,
    gather=0,
    joins=(),
    rests=(),
    chunks=LINE_CHUNKS,
    groups=(),
    weights=(),
    grads=(),
    deliver=True,
    extra=None,
    pieces=None,
):
    parts = () if part is None else part if isinstance(part, tuple) else (part,)
    reduce = len(parts) > 0
    giving = len(grads) > 0
    row_count, model_width = ins[0].shape
    vmem = pl.BlockSpec(memory_space=pltpu.VMEM)
    outs = []
    for _ in range(gather):
        outs.append(jax.ShapeDtypeStruct((n, 2, row_count, model_width), jnp.bfloat16))
    outs += [jax.ShapeDtypeStruct((2, row_count, model_width), kind) for kind in joins]
    outs += list(rests)
    out_specs = [vmem] * len(outs)
    for members in groups if not giving else ():
        rows = weights[0].shape[0] * n * lax.axis_size("fsdp")
        width = sum(weights[a].shape[1] for a in members) // n
        outs.append(jax.ShapeDtypeStruct((rows, width), jnp.bfloat16))
        out_specs.append(pl.BlockSpec(memory_space=pl.ANY))
    dma = pltpu.SemaphoreType.DMA
    if pieces is not None:
        rows = pieces.shape[0] * pieces.shape[1] * lax.axis_size("fsdp")
        outs.append(jax.ShapeDtypeStruct((rows, pieces.shape[2]), jnp.bfloat16))
        out_specs.append(pl.BlockSpec(memory_space=pl.ANY))
    if giving:
        owned = grads[0].shape[0] // (n * lax.axis_size("fsdp"))
        shapes = [(owned, width * n) for width in weights]
        if not deliver:
            shapes = [(n, owned, sum(grad.shape[1] for grad in grads))]
        for shape in shapes:
            outs.append(jax.ShapeDtypeStruct(shape, jnp.bfloat16))
            out_specs.append(vmem)
    if extra is not None:
        outs.append(jax.ShapeDtypeStruct(extra.shape, jnp.float32))
        out_specs.append(vmem)
    total_chunks = chunks * max(len(parts), 1)
    sum_rows = row_count * max(len(parts), 1)
    scratch = []
    if reduce:
        slot = pltpu.VMEM((2, n - 1, sum_rows, model_width), jnp.bfloat16)
        scratch += [pltpu.VMEM((n, sum_rows, model_width), jnp.bfloat16), dma((total_chunks,))]
        scratch += [pltpu.VMEM((n, sum_rows, model_width), jnp.bfloat16), slot, slot]
        scratch += [pltpu.VMEM((row_count // chunks, model_width), jnp.float32)]
        tally = (2, n - 1, total_chunks)
        scratch += [dma((total_chunks,)), dma((total_chunks,)), dma(tally), dma(tally)]
    if gather:
        tally = (gather, 2, n - 1, chunks)
        scratch += [dma(tally), dma(tally), dma((gather, n, chunks)), dma((gather, n, chunks))]
    if joins:
        scratch += [dma((len(joins), chunks)), dma((len(joins), chunks))]
    if groups and not giving:
        arrays = len(weights)
        tally = (2, len(groups), n)
        scratch += [dma((arrays,)), dma((arrays, n)), dma((arrays, n))]
        scratch += [dma(tally), dma(tally), dma(tally), dma(tally)]
    if pieces is not None:
        scratch += [dma((n,))] + [dma((2, n))] * 4
    if giving:
        for grad in grads:
            halves = (owned // 2, grad.shape[1])
            for lead in ((n, 2, 2), (n, 2, 2), (n, 2), (n, 2)):
                scratch.append(pltpu.VMEM(lead + halves, jnp.bfloat16))
            if deliver:
                scratch.append(pltpu.VMEM((n - 1, owned, grad.shape[1]), jnp.bfloat16))
        count = len(groups)
        scratch += [dma((count, n, 2, 2)), dma((count, n, 2, 2))]
        scratch += [dma((count, n, 2)), dma((count, n, 2))]
        scratch += [dma((len(weights), n)), dma((len(weights), n)), dma((count, n, 2, 2))]
    if extra is not None:
        stack = pltpu.VMEM((3,) + extra.shape, jnp.float32)
        scratch += [stack, stack, pltpu.VMEM((n,) + extra.shape, jnp.float32)]
        scratch += [dma((3,)), dma((3,)), dma((n - 1,)), dma((n - 1,))]
    operands = list(parts) + list(ins) + (list(grads) if giving else list(weights))
    operands += [] if extra is None else [extra]
    operands += [] if pieces is None else [pieces]
    anywhere = [*parts, *grads]
    in_specs = [
        pl.BlockSpec(memory_space=pl.ANY) if any(a is b for b in anywhere) else vmem
        for a in operands
    ]
    moved = row_count * model_width * 2 * n * (2 * reduce + 2 * gather)
    return pl.pallas_call(
        functools.partial(
            line_body,
            n,
            chunks,
            len(parts),
            gather,
            pieces is not None,
            len(ins),
            len(joins),
            len(rests),
            groups,
            giving,
            deliver,
            extra is not None,
            finish,
        ),
        out_shape=tuple(outs),
        in_specs=in_specs,
        out_specs=tuple(out_specs),
        scratch_shapes=scratch,
        compiler_params=pltpu.CompilerParams(
            collective_id=collective, has_side_effects=True, vmem_limit_bytes=56 << 20
        ),
        cost_estimate=pl.CostEstimate(
            flops=moved, bytes_accessed=20 * moved, transcendentals=0
        ),
    )(*operands)


def finish_gather(j, rows, total, ins, rest):
    values = ins[0][rows, :].astype(jnp.float32)
    return (values * rms_scale(values) * ins[1][...]).astype(jnp.bfloat16)


def finish_attention(j, rows, total, ins, rest):
    residual = ins[0][rows, :].astype(jnp.float32) + total
    rest[0][rows, :] = residual
    return (residual * rms_scale(residual) * ins[1][...]).astype(jnp.bfloat16)


def gain_rows(j, rest, terms):
    sums = jnp.sum(terms, axis=0, keepdims=True)
    rest[...] = sums if j == 0 else rest[...] + sums


def finish_mlp_back(j, rows, total, ins, rest):
    residual = ins[0][rows, :]
    if j >= LINE_CHUNKS:
        return (residual + total).astype(jnp.bfloat16)
    scale = rms_scale(residual)
    hat = residual * scale
    grad = ins[1][rows, :].astype(jnp.float32) + norm_back(total, hat, scale, ins[2][...])
    rest[0][rows, :] = grad
    gain_rows(j, rest[1], total * hat)
    return grad.astype(jnp.bfloat16)


def finish_tokens(j, rows, total, ins, rest):
    values = ins[1][rows, :].astype(jnp.float32)
    scale = rms_scale(values)
    hat = values * scale
    return ins[0][rows, :] + norm_back(total, hat, scale, ins[2][...])


def permuted_tokens(rows):
    n = lax.axis_size("context")
    place = lax.axis_index("context")
    core = lax.axis_index("tensor")
    shape = rows.shape
    near = jnp.zeros((n,) + shape, rows.dtype)
    for s in range(n):
        ring = [(i, (i + s) % n) for i in range(n)]
        came = lax.ppermute(rows, "context", ring) if s else rows
        near = lax.dynamic_update_slice(near, came[None], (lax.rem(place + n - s, n), 0, 0))
    far = lax.ppermute(near, "tensor", [(0, 1), (1, 0)])
    both = jnp.zeros((n, 2) + shape, rows.dtype)
    both = lax.dynamic_update_slice(both, near[:, None], (0, core, 0, 0))
    both = lax.dynamic_update_slice(both, far[:, None], (0, 1 - core, 0, 0))
    return both.reshape(n * 2 * shape[0], shape[1])


BACK_BLOCK = 256


def attend_back_body(kv_heads, group, queries, keys, values, grads, d_queries, d_keys, d_values):
    length = queries.shape[0]
    scale = 1.0 / math.sqrt(HEAD_DIM)
    d_keys[...] = jnp.zeros_like(d_keys)
    d_values[...] = jnp.zeros_like(d_values)
    for h in range(kv_heads):
        own = slice(h * HEAD_DIM, (h + 1) * HEAD_DIM)
        for start in range(0, length, BACK_BLOCK):
            end = start + BACK_BLOCK
            shape = (BACK_BLOCK, end)
            at = lax.broadcasted_iota(jnp.int32, shape, 0) + start
            visible = lax.broadcasted_iota(jnp.int32, shape, 1) <= at
            key, value = keys[0:end, own], values[0:end, own]
            for m in range(h * group, (h + 1) * group):
                cols = slice(m * HEAD_DIM, (m + 1) * HEAD_DIM)
                query, grad = queries[start:end, cols], grads[start:end, cols]
                weights = jnp.where(visible, jnp.exp(column_product(query, key) * scale), 0.0)
                probs = weights / jnp.sum(weights, axis=1, keepdims=True)
                grad_probs = column_product(grad, value)
                delta = jnp.sum(probs * grad_probs, axis=1, keepdims=True)
                grad_scores = (probs * (grad_probs - delta)).astype(jnp.bfloat16)
                d_queries[start:end, cols] = (
                    jnp.dot(grad_scores, key, preferred_element_type=jnp.float32) * scale
                )
                d_keys[0:end, own] += row_product(grad_scores, query) * scale
                d_values[0:end, own] += row_product(probs.astype(jnp.bfloat16), grad)


def attend_back(kv_heads, group, queries, keys, values, grads):
    vmem = pl.BlockSpec(memory_space=pltpu.VMEM)
    shapes = [jax.ShapeDtypeStruct(a.shape, jnp.float32) for a in (queries, keys, values)]
    work = 5 * queries.shape[0] ** 2 * queries.shape[1]
    return pl.pallas_call(
        functools.partial(attend_back_body, kv_heads, group),
        out_shape=tuple(shapes),
        in_specs=[vmem] * 4,
        out_specs=(vmem,) * 3,
        compiler_params=pltpu.CompilerParams(vmem_limit_bytes=48 << 20),
        cost_estimate=pl.CostEstimate(flops=work, bytes_accessed=4 << 20, transcendentals=0),
        name="attend_back",
    )(queries, keys, values, grads)


def widen_body(h_cols, out, tokens, mlp, *refs):
    attn, results = refs[:4], refs[4:]
    results[0][...] = out[...]
    results[1][...] = tokens[...]
    for a in range(4):
        results[2 + a][...] = attn[a][...].astype(jnp.float32)
    for a in range(3):
        results[6 + a][...] = mlp[0, :, a * h_cols : (a + 1) * h_cols].astype(jnp.float32)


def widen(parts, h_cols, out, tokens, mlp, *attn):
    rows = mlp.shape[1]
    width = out.shape[-1]
    out, tokens = out.reshape(-1, width), tokens.reshape(-1, width)
    token_rows = pl.BlockSpec((out.shape[0] // parts, width), lambda i: (i, 0))
    quarters = [pl.BlockSpec((rows, a.shape[1] // parts), lambda i: (0, i)) for a in attn]
    hidden = pl.BlockSpec((rows, h_cols), lambda i: (0, i))
    results = [jax.ShapeDtypeStruct(a.shape, a.dtype) for a in (out, tokens)]
    results += [jax.ShapeDtypeStruct(a.shape, jnp.float32) for a in attn]
    results += [jax.ShapeDtypeStruct((rows, h_cols * parts), jnp.float32)] * 3
    return pl.pallas_call(
        functools.partial(widen_body, h_cols),
        grid=(parts,),
        in_specs=[token_rows, token_rows, pl.BlockSpec((1,) + mlp.shape[1:], lambda i: (i, 0, 0))]
        + quarters,
        out_specs=tuple([token_rows, token_rows] + quarters + [hidden] * 3),
        out_shape=tuple(results),
        name="widen",
    )(out, tokens, mlp, *attn)


def token_half(block, index, parts):
    rows = block.shape[0] // parts
    return lax.dynamic_slice_in_dim(block, index * rows, rows, axis=0)


def line_shards(
    tokens,
    cotangent,
    norm_gain_attn,
    norm_gain_mlp,
    head_gains,
    query_weight,
    key_matrix,
    value_matrix,
    output_weight,
    gate_weight,
    up_weight,
    down_weight,
):
    _, local_len, model_width = tokens.shape
    parts = lax.axis_size("context")
    cores = lax.axis_size("tensor")
    core = lax.axis_index("tensor")
    full_len = local_len * parts
    q_cols = query_weight.shape[1] // parts
    kv_cols = key_matrix.shape[1] // parts
    h_cols = gate_weight.shape[1] // parts
    q_heads = q_cols // HEAD_DIM
    kv_heads = kv_cols // HEAD_DIM
    head_group = q_heads // kv_heads
    score_scale = 1.0 / math.sqrt(HEAD_DIM)
    positions = jnp.arange(full_len, dtype=jnp.int32)
    cosine_table, sine_table = rope_tables(positions, HEAD_DIM)
    cosine_table = cosine_table[:, None, :]
    sine_table = sine_table[:, None, :]
    visible = positions[None, :] <= positions[:, None]
    gain_attn = norm_gain_attn.astype(jnp.float32)[None]
    gain_mlp = norm_gain_mlp.astype(jnp.float32)[None]
    gain_heads = head_gains.astype(jnp.float32)

    def line_parts(left, right):
        product = column_product(left, right).astype(jnp.bfloat16)
        return product.reshape(parts, cores, half_len, model_width)

    own_cot = token_half(cotangent.reshape(local_len, model_width), core, cores)
    inputs = token_half(tokens.reshape(local_len, model_width), core, cores)
    half_len = local_len // cores
    rows_f32 = jax.ShapeDtypeStruct((half_len, model_width), jnp.float32)
    sums_f32 = jax.ShapeDtypeStruct((1, model_width), jnp.float32)
    normed_attn, in_weights, out_weights = line_call(
        parts,
        1,
        finish_gather,
        None,
        (inputs, gain_attn),
        gather=1,
        groups=((0, 1, 2), (3,)),
        weights=(query_weight, key_matrix, value_matrix, output_weight),
    )
    normed_attn = normed_attn.reshape(full_len, model_width)
    own_cot, normed_attn = lax.optimization_barrier((own_cot, normed_attn))
    grad_out = permuted_tokens(own_cot)

    raw = jnp.dot(normed_attn, in_weights, preferred_element_type=jnp.float32)
    query_split = raw[:, :q_cols].reshape(full_len, q_heads, HEAD_DIM)
    query_scale = rms_scale(query_split)
    query_hat = query_split * query_scale
    queries = rotate(query_hat * gain_heads[0], cosine_table, sine_table).astype(jnp.bfloat16)
    key_split = raw[:, q_cols : q_cols + kv_cols].reshape(full_len, kv_heads, HEAD_DIM)
    key_scale = rms_scale(key_split)
    key_hat = key_split * key_scale
    keys = rotate(key_hat * gain_heads[1], cosine_table, sine_table).astype(jnp.bfloat16)
    values = raw[:, q_cols + kv_cols :].astype(jnp.bfloat16).reshape(full_len, kv_heads, HEAD_DIM)
    queries = queries.reshape(full_len, kv_heads, head_group, HEAD_DIM)

    scores = (
        jnp.einsum("ikgd,jkd->kgij", queries, keys, preferred_element_type=jnp.float32)
        * score_scale
    )
    weights = jnp.where(visible, jnp.exp(scores), 0.0)
    probs = weights / jnp.sum(weights, axis=-1, keepdims=True)
    probs_low = probs.astype(jnp.bfloat16)
    attended = (
        jnp.einsum("kgij,jkd->ikgd", probs_low, values, preferred_element_type=jnp.float32)
        .astype(jnp.bfloat16)
        .reshape(full_len, q_cols)
    )
    normed_mlp, residual, mlp_in, mlp_down = line_call(
        parts,
        2,
        finish_attention,
        line_parts(attended, out_weights),
        (inputs, gain_mlp),
        gather=1,
        rests=(rows_f32,),
        groups=((0, 1), (2,)),
        weights=(gate_weight, up_weight, down_weight),
    )
    normed_mlp = normed_mlp.reshape(full_len, model_width)

    both = jnp.dot(normed_mlp, mlp_in, preferred_element_type=jnp.float32)
    gate_act = both[:, :h_cols]
    upward = both[:, h_cols:]
    sig_gate = jax.nn.sigmoid(gate_act)
    activated = gate_act * sig_gate
    hidden = (activated * upward).astype(jnp.bfloat16)
    grad_hidden = jnp.dot(grad_out, mlp_down, preferred_element_type=jnp.float32)
    derivative = sig_gate * (1.0 + gate_act * (1.0 - sig_gate))
    grad_gate = (grad_hidden * upward * derivative).astype(jnp.bfloat16)
    grad_up = (grad_hidden * activated).astype(jnp.bfloat16)
    grad_both = jnp.concatenate([grad_gate, grad_up], axis=1)
    grad_in = row_product(normed_mlp, grad_both).astype(jnp.bfloat16)
    grad_down = row_product(grad_out, hidden).astype(jnp.bfloat16)
    grad_branch, out, grad_residual, gain_mlp_part, mlp_grads = line_call(
        parts,
        3,
        finish_mlp_back,
        (line_parts(grad_both, mlp_in), line_parts(hidden, mlp_down)),
        (residual, own_cot, gain_mlp),
        gather=1,
        joins=(jnp.bfloat16,),
        rests=(rows_f32, sums_f32),
        groups=((0, 1), (2,)),
        weights=(h_cols, h_cols, h_cols),
        grads=(grad_in, grad_down),
        deliver=False,
    )
    mlp_grads = lax.all_to_all(mlp_grads, "context", split_axis=0, concat_axis=0, tiled=True)
    grad_branch = grad_branch.reshape(full_len, model_width)
    grad_attended = jnp.dot(grad_branch, out_weights, preferred_element_type=jnp.float32)
    grad_attended = grad_attended.astype(jnp.bfloat16)
    grad_queries, grad_keys, grad_values = attend_back(
        kv_heads,
        head_group,
        queries.reshape(full_len, q_cols),
        keys.reshape(full_len, kv_cols),
        values.reshape(full_len, kv_cols),
        grad_attended,
    )
    grad_queries = grad_queries.reshape(full_len, q_heads, HEAD_DIM)
    grad_keys = grad_keys.reshape(full_len, kv_heads, HEAD_DIM)
    grad_query_hat = unrotate(grad_queries, cosine_table, sine_table)
    grad_key_hat = unrotate(grad_keys, cosine_table, sine_table)
    heads_part = jnp.stack(
        [
            jnp.sum(grad_query_hat * query_hat, axis=(0, 1)),
            jnp.sum(grad_key_hat * key_hat, axis=(0, 1)),
        ]
    )
    grad_raw = jnp.concatenate(
        [
            norm_back(grad_query_hat, query_hat, query_scale, gain_heads[0]).reshape(
                full_len, q_cols
            ),
            norm_back(grad_key_hat, key_hat, key_scale, gain_heads[1]).reshape(full_len, kv_cols),
            grad_values.reshape(full_len, kv_cols),
        ],
        axis=1,
    ).astype(jnp.bfloat16)
    attn_in_grad = row_product(normed_attn, grad_raw).astype(jnp.bfloat16)
    attn_out_grad = row_product(grad_branch, attended).astype(jnp.bfloat16)
    gain_attn_part = (
        jnp.sum(attn_in_grad.astype(jnp.float32) * in_weights.astype(jnp.float32), axis=1)[None]
        / gain_attn
    )
    gains = jnp.concatenate(
        [
            gain_attn_part,
            gain_mlp_part,
            jnp.pad(heads_part.reshape(1, -1), ((0, 0), (0, model_width - heads_part.size))),
            jnp.zeros((5, model_width), jnp.float32),
        ],
        axis=0,
    )
    grad_tokens, query_grad, key_grad, value_grad, output_grad, totals = line_call(
        parts,
        4,
        finish_tokens,
        line_parts(grad_raw, in_weights),
        (grad_residual, inputs, gain_attn),
        joins=(jnp.float32,),
        groups=((0, 1, 2), (3,)),
        weights=(q_cols, kv_cols, kv_cols, q_cols),
        grads=(attn_in_grad, attn_out_grad),
        extra=gains,
    )
    ready = (out, grad_tokens, mlp_grads, query_grad, key_grad, value_grad, output_grad)
    out, grad_tokens, *weight_grads = widen(parts, h_cols, *ready)
    return (
        out.reshape(tokens.shape),
        grad_tokens.reshape(tokens.shape),
        totals[0],
        totals[1],
        totals[2, : heads_part.size].reshape(heads_part.shape),
        *weight_grads,
    )


def layer(*operands):
    tokens, key_matrix, gate_weight = operands[0], operands[6], operands[9]
    parts = lax.axis_size("context")
    cores = lax.axis_size("tensor")
    fits = (
        tokens.shape[0] == 1
        and key_matrix.shape[1] % (parts * HEAD_DIM) == 0
        and gate_weight.shape[1] % (parts * HEAD_DIM) == 0
        and tokens.shape[1] % (cores * LINE_CHUNKS * 16) == 0
        and cores == 2
        and tokens.shape[1] * parts % BACK_BLOCK == 0
        and lax.axis_size("fsdp") == 4
    )
    return line_shards(*operands) if fits else shards(*operands)


def solution(mesh):
    return jax.shard_map(
        layer,
        mesh=mesh,
        in_specs=(
            P("fsdp", "context", None),
            P("fsdp", "context", None),
            P(),
            P(),
            P(),
            P(("fsdp", "context"), "tensor"),
            P(("fsdp", "context"), "tensor"),
            P(("fsdp", "context"), "tensor"),
            P(("fsdp", "context"), "tensor"),
            P(("fsdp", "context"), "tensor"),
            P(("fsdp", "context"), "tensor"),
            P(("fsdp", "context"), "tensor"),
        ),
        out_specs=(
            P("fsdp", "context", None),
            P("fsdp", "context", None),
            P(),
            P(),
            P(),
            P(("fsdp", "context"), "tensor"),
            P(("fsdp", "context"), "tensor"),
            P(("fsdp", "context"), "tensor"),
            P(("fsdp", "context"), "tensor"),
            P(("fsdp", "context"), "tensor"),
            P(("fsdp", "context"), "tensor"),
            P(("fsdp", "context"), "tensor"),
        ),
        check_vma=False,
    )
```

```python
import functools
import math

import jax
import jax.numpy as jnp
from jax import lax
from jax.experimental import pallas as pl
from jax.experimental.pallas import tpu as pltpu
from jax.sharding import PartitionSpec as P


HEAD_DIM = 128


EPS = 1e-06
THETA = 1000000.0


def rms_scale(values):
    return lax.rsqrt(jnp.mean(values * values, axis=-1, keepdims=True) + EPS)


def rope_tables(positions, head_size):
    halves = head_size // 2
    inverse = THETA ** (-(jnp.arange(halves, dtype=jnp.float32) * 2.0) / head_size)
    angle = positions[:, None].astype(jnp.float32) * inverse[None, :]
    return (jnp.cos(angle), jnp.sin(angle))


def rotate(values, cosine_table, sine_table):
    halves = values.shape[-1] // 2
    leading = values[..., :halves]
    trailing = values[..., halves:]
    return jnp.concatenate(
        [
            leading * cosine_table - trailing * sine_table,
            trailing * cosine_table + leading * sine_table,
        ],
        axis=-1,
    )


def unrotate(values, cosine_table, sine_table):
    halves = values.shape[-1] // 2
    leading = values[..., :halves]
    trailing = values[..., halves:]
    return jnp.concatenate(
        [
            leading * cosine_table + trailing * sine_table,
            trailing * cosine_table - leading * sine_table,
        ],
        axis=-1,
    )


def norm_back(grad_normed, normed_hat, scale_factor, gain):
    scaled = grad_normed * gain
    return scale_factor * (
        scaled - normed_hat * jnp.mean(normed_hat * scaled, axis=-1, keepdims=True)
    )


def row_product(left, right):
    return lax.dot_general(
        left, right, (((0,), (0,)), ((), ())), preferred_element_type=jnp.float32
    )


def column_product(left, right):
    return lax.dot_general(
        left, right, (((1,), (1,)), ((), ())), preferred_element_type=jnp.float32
    )


def blank(row_total, col_total):
    return jnp.zeros((row_total, col_total), jnp.float32)


def placing(left):

    def place_rows(total, piece, start):
        return column_product(left, piece)

    return place_rows


def adding(left):

    def add_rows(total, piece, start):
        return jnp.dot(left, piece, preferred_element_type=jnp.float32)

    return add_rows


def tensor_total(partial_sum):
    return lax.psum(partial_sum, "tensor")


def owner_rows(term_fn, row_total):
    return lax.psum_scatter(
        term_fn(jnp.int32(0), lax.axis_size(("fsdp", "context")) * row_total),
        ("fsdp", "context"),
        scatter_dimension=0,
        tiled=True,
    )


def shards(
    tokens,
    cotangent,
    norm_gain_attn,
    norm_gain_mlp,
    head_gains,
    query_weight,
    key_matrix,
    value_matrix,
    output_weight,
    gate_weight,
    up_weight,
    down_weight,
):
    seq_count, local_len, model_width = tokens.shape
    row_count = seq_count * local_len
    owned_rows = query_weight.shape[0]
    query_cols = query_weight.shape[1]
    kv_cols = key_matrix.shape[1]
    hidden_cols = gate_weight.shape[1]
    query_heads = query_cols // HEAD_DIM
    kv_heads = kv_cols // HEAD_DIM
    head_group = query_heads // kv_heads
    score_scale = 1.0 / math.sqrt(HEAD_DIM)
    full_len = local_len * lax.axis_size("context")
    query_pos = lax.axis_index("context") * local_len + jnp.arange(local_len, dtype=jnp.int32)
    key_pos = jnp.arange(full_len, dtype=jnp.int32)
    cosine_table, sine_table = rope_tables(query_pos, HEAD_DIM)
    cosine_table = cosine_table[:, None, :]
    sine_table = sine_table[:, None, :]
    visible = key_pos[None, :] <= query_pos[:, None]
    inputs = tokens.reshape(row_count, model_width).astype(jnp.float32)
    grad_out = cotangent.reshape(row_count, model_width)
    gain_attn = norm_gain_attn.astype(jnp.float32)
    gain_mlp = norm_gain_mlp.astype(jnp.float32)
    gain_heads = head_gains.astype(jnp.float32)

    def attn_rows(fold_fn, initial):
        return fold_fn(
            initial,
            (
                lax.all_gather(query_weight, ("fsdp", "context"), axis=0, tiled=True),
                lax.all_gather(key_matrix, ("fsdp", "context"), axis=0, tiled=True),
                lax.all_gather(value_matrix, ("fsdp", "context"), axis=0, tiled=True),
            ),
            jnp.int32(0),
        )

    def attn_out_rows(fold_fn, initial):
        return fold_fn(
            initial,
            lax.all_gather(output_weight, ("fsdp", "context"), axis=0, tiled=True),
            jnp.int32(0),
        )

    def mlp_rows(fold_fn, initial):
        return fold_fn(
            initial,
            (
                lax.all_gather(gate_weight, ("fsdp", "context"), axis=0, tiled=True),
                lax.all_gather(up_weight, ("fsdp", "context"), axis=0, tiled=True),
            ),
            jnp.int32(0),
        )

    def down_rows(fold_fn, initial):
        return fold_fn(
            initial,
            lax.all_gather(down_weight, ("fsdp", "context"), axis=0, tiled=True),
            jnp.int32(0),
        )

    scale_attn = rms_scale(inputs)
    hat_attn = inputs * scale_attn
    normed_attn = (hat_attn * gain_attn).astype(jnp.bfloat16)

    def project_in(totals, pieces, start):
        return (
            jnp.dot(normed_attn, pieces[0], preferred_element_type=jnp.float32),
            jnp.dot(normed_attn, pieces[1], preferred_element_type=jnp.float32),
            jnp.dot(normed_attn, pieces[2], preferred_element_type=jnp.float32),
        )

    query_raw, key_unrotated, value_raw = attn_rows(
        project_in,
        (blank(row_count, query_cols), blank(row_count, kv_cols), blank(row_count, kv_cols)),
    )
    query_split = query_raw.reshape(seq_count, local_len, query_heads, HEAD_DIM)
    query_scale = rms_scale(query_split)
    query_hat = query_split * query_scale
    query_rows = rotate(query_hat * gain_heads[0], cosine_table, sine_table).astype(jnp.bfloat16)
    key_split = key_unrotated.reshape(seq_count, local_len, kv_heads, HEAD_DIM)
    key_scale = rms_scale(key_split)
    key_hat = key_split * key_scale
    keys_local = rotate(key_hat * gain_heads[1], cosine_table, sine_table).astype(jnp.bfloat16)
    values_local = value_raw.astype(jnp.bfloat16)
    keys_all, value_rows_gathered = (
        lax.all_gather(
            keys_local.reshape(seq_count, local_len, kv_cols), "context", axis=1, tiled=True
        ),
        lax.all_gather(
            values_local.reshape(seq_count, local_len, kv_cols), "context", axis=1, tiled=True
        ),
    )
    query_blocks = query_rows.reshape(
        seq_count, local_len, kv_heads, head_group, HEAD_DIM
    ).transpose(2, 0, 1, 3, 4)
    key_blocks = keys_all.reshape(seq_count, full_len, kv_heads, HEAD_DIM).transpose(2, 0, 1, 3)
    value_blocks = value_rows_gathered.reshape(seq_count, full_len, kv_heads, HEAD_DIM).transpose(
        2, 0, 1, 3
    )

    def attend(operands):
        query_block, key_block, value_block = operands
        scores = (
            jnp.einsum("bigd,bjd->bgij", query_block, key_block, preferred_element_type=jnp.float32)
            * score_scale
        )
        weights = jnp.where(visible, jnp.exp(scores), 0.0)
        totals = jnp.sum(weights, axis=-1)
        probs_low = (weights / totals[..., None]).astype(jnp.bfloat16)
        mixed_heads = jnp.einsum(
            "bgij,bjd->bigd", probs_low, value_block, preferred_element_type=jnp.float32
        )
        return (mixed_heads.astype(jnp.bfloat16), jnp.log(totals))

    mixed_all, log_totals = lax.map(attend, (query_blocks, key_blocks, value_blocks))
    attended = mixed_all.transpose(1, 2, 0, 3, 4).reshape(row_count, query_cols)
    attn_part = attn_out_rows(placing(attended), blank(row_count, model_width))
    residual = inputs + tensor_total(attn_part)
    scale_mlp = rms_scale(residual)
    hat_mlp = residual * scale_mlp
    normed_mlp = (hat_mlp * gain_mlp).astype(jnp.bfloat16)

    def project_mlp(totals, pieces, start):
        return (
            jnp.dot(normed_mlp, pieces[0], preferred_element_type=jnp.float32),
            jnp.dot(normed_mlp, pieces[1], preferred_element_type=jnp.float32),
        )

    gate_act, upward = mlp_rows(
        project_mlp, (blank(row_count, hidden_cols), blank(row_count, hidden_cols))
    )
    sig_gate = jax.nn.sigmoid(gate_act)
    activated = gate_act * sig_gate
    hidden = (activated * upward).astype(jnp.bfloat16)
    mlp_part = down_rows(placing(hidden), blank(row_count, model_width))
    result = residual + tensor_total(mlp_part)
    out = result.astype(jnp.bfloat16).reshape(seq_count, local_len, model_width)
    grad_hidden = down_rows(adding(grad_out), blank(row_count, hidden_cols))
    derivative = sig_gate * (1.0 + gate_act * (1.0 - sig_gate))
    grad_gate = (grad_hidden * upward * derivative).astype(jnp.bfloat16)
    grad_up = (grad_hidden * activated).astype(jnp.bfloat16)

    def gate_back(total, pieces, start):
        part_sum = column_product(grad_gate, pieces[0]) + column_product(grad_up, pieces[1])
        return part_sum

    grad_normed_mlp = tensor_total(mlp_rows(gate_back, blank(row_count, model_width)))

    def mlp_terms(start, span_rows):
        return jnp.concatenate(
            [
                row_product(normed_mlp, grad_gate),
                row_product(normed_mlp, grad_up),
                row_product(grad_out, hidden),
            ],
            axis=1,
        )

    mlp_grads = owner_rows(mlp_terms, owned_rows)
    grad_gain_mlp = jnp.sum(grad_normed_mlp * hat_mlp, axis=0)
    grad_residual = grad_out.astype(jnp.float32) + norm_back(
        grad_normed_mlp, hat_mlp, scale_mlp, gain_mlp
    )
    grad_branch = grad_residual.astype(jnp.bfloat16)
    grad_attended = attn_out_rows(adding(grad_branch), blank(row_count, query_cols))
    grad_attended_low = grad_attended.astype(jnp.bfloat16)
    grad_blocks = grad_attended_low.reshape(
        seq_count, local_len, kv_heads, head_group, HEAD_DIM
    ).transpose(2, 0, 1, 3, 4)

    def attend_back(operands):
        query_block, key_block, value_block, grad_block, log_total = operands
        scores = (
            jnp.einsum("bigd,bjd->bgij", query_block, key_block, preferred_element_type=jnp.float32)
            * score_scale
        )
        probs = jnp.where(visible, jnp.exp(scores - log_total[..., None]), 0.0)
        probs_low = probs.astype(jnp.bfloat16)
        grad_probs = jnp.einsum(
            "bigd,bjd->bgij", grad_block, value_block, preferred_element_type=jnp.float32
        )
        delta = jnp.sum(probs * grad_probs, axis=-1, keepdims=True)
        grad_scores = (probs * (grad_probs - delta)).astype(jnp.bfloat16)
        grad_query = (
            jnp.einsum("bgij,bjd->bigd", grad_scores, key_block, preferred_element_type=jnp.float32)
            * score_scale
        )
        grad_key = (
            jnp.einsum(
                "bgij,bigd->bjd", grad_scores, query_block, preferred_element_type=jnp.float32
            )
            * score_scale
        )
        grad_value = jnp.einsum(
            "bgij,bigd->bjd", probs_low, grad_block, preferred_element_type=jnp.float32
        )
        return (grad_query, grad_key, grad_value, delta[..., 0])

    grad_query_all, grad_key_all, grad_value_all, _ = lax.map(
        attend_back, (query_blocks, key_blocks, value_blocks, grad_blocks, log_totals)
    )
    grad_key_full = grad_key_all.transpose(1, 2, 0, 3).reshape(seq_count, full_len, kv_cols)
    grad_value_full = grad_value_all.transpose(1, 2, 0, 3).reshape(seq_count, full_len, kv_cols)
    grad_key_own, grad_value_own = (
        lax.psum_scatter(
            grad_key_full.astype(jnp.bfloat16), "context", scatter_dimension=1, tiled=True
        ).astype(jnp.float32),
        lax.psum_scatter(
            grad_value_full.astype(jnp.bfloat16), "context", scatter_dimension=1, tiled=True
        ).astype(jnp.float32),
    )
    grad_query_rot = grad_query_all.transpose(1, 2, 0, 3, 4).reshape(
        seq_count, local_len, query_heads, HEAD_DIM
    )
    grad_query_hat = unrotate(grad_query_rot, cosine_table, sine_table)
    grad_key_hat = unrotate(
        grad_key_own.reshape(seq_count, local_len, kv_heads, HEAD_DIM), cosine_table, sine_table
    )
    grad_gain_query = jnp.sum(grad_query_hat * query_hat, axis=(0, 1, 2))
    grad_gain_key = jnp.sum(grad_key_hat * key_hat, axis=(0, 1, 2))
    grad_query_raw = (
        norm_back(grad_query_hat, query_hat, query_scale, gain_heads[0])
        .reshape(row_count, query_cols)
        .astype(jnp.bfloat16)
    )
    grad_key_raw = (
        norm_back(grad_key_hat, key_hat, key_scale, gain_heads[1])
        .reshape(row_count, kv_cols)
        .astype(jnp.bfloat16)
    )
    grad_value_low = grad_value_own.reshape(row_count, kv_cols).astype(jnp.bfloat16)

    def attn_back(total, pieces, start):
        part_sum = (
            column_product(grad_query_raw, pieces[0])
            + column_product(grad_key_raw, pieces[1])
            + column_product(grad_value_low, pieces[2])
        )
        return part_sum

    grad_normed_part = attn_rows(attn_back, blank(row_count, model_width))
    grad_normed_attn, grad_heads_gain = (
        lax.psum(grad_normed_part.astype(jnp.bfloat16), "tensor").astype(jnp.float32),
        lax.psum(jnp.stack([grad_gain_query, grad_gain_key]).astype(jnp.bfloat16), "tensor").astype(
            jnp.float32
        ),
    )

    def attn_terms(start, span_rows):
        return jnp.concatenate(
            [
                row_product(normed_attn, grad_query_raw),
                row_product(normed_attn, grad_key_raw),
                row_product(normed_attn, grad_value_low),
                row_product(grad_branch, attended),
            ],
            axis=1,
        )

    attn_grads = owner_rows(attn_terms, owned_rows)
    grad_gain_attn = jnp.sum(grad_normed_attn * hat_attn, axis=0)
    grad_tokens = grad_residual + norm_back(grad_normed_attn, hat_attn, scale_attn, gain_attn)
    total_attn, total_mlp, total_heads = lax.psum(
        (grad_gain_attn, grad_gain_mlp, grad_heads_gain), ("fsdp", "context")
    )
    query_grad = attn_grads[:, :query_cols]
    key_grad = attn_grads[:, query_cols : query_cols + kv_cols]
    value_grad = attn_grads[:, query_cols + kv_cols : query_cols + 2 * kv_cols]
    output_grad = attn_grads[:, query_cols + 2 * kv_cols :]
    gate_grad = mlp_grads[:, :hidden_cols]
    up_grad = mlp_grads[:, hidden_cols : 2 * hidden_cols]
    down_grad = mlp_grads[:, 2 * hidden_cols :]
    return (
        out,
        grad_tokens.reshape(seq_count, local_len, model_width),
        total_attn,
        total_mlp,
        total_heads,
        query_grad,
        key_grad,
        value_grad,
        output_grad,
        gate_grad,
        up_grad,
        down_grad,
    )


LINE_CHUNKS = 8
LINE_LAG = 2
LINE_START_TURNS = 1
LINE_FROM_TURN = 1
LINE_PLAIN_FROM = 0
LINE_PLAIN_LAG = 1
LINE_PLAIN_STEP = 1
LINE_GIVE_TURN = 6
MESH = pl.DeviceIdType.MESH


def line_copy(src, dst, send, recv, device):
    return pltpu.make_async_remote_copy(
        src_ref=src,
        dst_ref=dst,
        send_sem=send,
        recv_sem=recv,
        device_id=device,
        device_id_type=MESH,
    )


def line_barrier(n, place, core, fetching):
    barrier = pltpu.get_barrier_semaphore()

    def greet(device):
        pl.semaphore_signal(barrier, inc=1, device_id=device, device_id_type=MESH)

    greet({"tensor": 1 - core})
    if fetching:
        group = lax.axis_index("fsdp")
        greet({"fsdp": jnp.bitwise_xor(group, 1)})
        greet({"fsdp": jnp.bitwise_xor(group, 2)})
        for shift in range(1, n):
            greet({"context": lax.rem(place + shift, n)})
        pl.semaphore_wait(barrier, n + 2)
        return

    @pl.when(place > 0)
    def _():
        greet({"context": place - 1})

    @pl.when(place < n - 1)
    def _():
        greet({"context": place + 1})

    ends = jnp.where(place > 0, 1, 0) + jnp.where(place < n - 1, 1, 0)
    pl.semaphore_wait(barrier, ends + 1)


def nearest(n):
    return [sorted(range(n), key=lambda q: (abs(q - p), q)) for p in range(n)]


def ranked(n, place):
    table = nearest(n)
    return [sum(jnp.where(place == p, table[p][k], 0) for p in range(n)) for k in range(n)]


def fetch_steps(n, place, groups, weights, outs, sems, turns, start_turns, from_turn):
    own_send, line_send, line_recv, near_send, near_recv, far_send, far_recv = sems
    group = lax.axis_index("fsdp")
    rows = weights[0].shape[0]
    neighbours = ({"fsdp": jnp.bitwise_xor(group, 1)}, {"fsdp": jnp.bitwise_xor(group, 2)})
    spans = []
    for g, members in enumerate(groups):
        start = 0
        for a in members:
            width = weights[a].shape[1] // n
            spans.append((a, g, start, width))
            start += width

    def block(out, of_group, at):
        return out.at[pl.ds(pl.multiple_of((of_group * n + at) * rows, rows), rows)]

    order = ranked(n, place)

    def columns(a, at, width):
        return weights[a].at[:, pl.ds(pl.multiple_of(at * width, 128), width)]

    def own_copy(a, g, start, width):
        return pltpu.make_async_copy(
            columns(a, place, width),
            block(outs[g], group, place).at[:, pl.ds(start, width)],
            own_send.at[a],
        )

    def line_move(a, g, start, width, s):
        return line_copy(
            columns(a, order[s], width),
            block(outs[g], group, place).at[:, pl.ds(start, width)],
            line_send.at[a, s],
            line_recv.at[a, place],
            {"context": order[s]},
        )

    def line_arrival(a, g, start, width, s):
        return line_copy(
            columns(a, place, width),
            block(outs[g], group, order[s]).at[:, pl.ds(start, width)],
            line_send.at[a, s],
            line_recv.at[a, order[s]],
            {"context": order[s]},
        )

    def near_copy(way, g, s, of_group):
        piece = block(outs[g], of_group, order[s])
        return line_copy(
            piece, piece, near_send.at[way, g, s], near_recv.at[way, g, s], neighbours[way]
        )

    def far_copy(half, g, s, of_group):
        start = (of_group * n + order[s]) * rows + half * (rows // 2)
        piece = outs[g].at[pl.ds(pl.multiple_of(start, rows // 2), rows // 2)]
        return line_copy(
            piece, piece, far_send.at[half, g, s], far_recv.at[half, g, s], neighbours[1 - half]
        )

    def own_start():
        for span in spans:
            own_copy(*span).start()

    def line_start(span, s):
        return lambda: line_move(*span, s).start()

    def spread(g, s):
        def step():
            for span in spans:
                if span[1] == g:
                    if s == 0:
                        own_copy(*span).wait()
                    else:
                        line_arrival(*span, s).wait_recv()
            near_copy(0, g, s, group).start()
            near_copy(1, g, s, group).start()

        return step

    def pass_on(g, s):
        def step():
            for half in (0, 1):
                source = jnp.bitwise_xor(group, half + 1)
                near_copy(half, g, s, source).wait_recv()
                far_copy(half, g, s, source).start()

        return step

    def settle():
        for g in range(len(groups)):
            for s in range(n):
                for half in (0, 1):
                    far_copy(half, g, s, jnp.bitwise_xor(group, 3)).wait_recv()
                    far_copy(half, g, s, group).wait_send()
                    near_copy(half, g, s, group).wait_send()
        for span in spans:
            for s in range(1, n):
                line_move(*span, s).wait_send()

    issue = [(span, s) for s in range(1, n) for span in spans]
    at_turn = {(span[0], s): i * start_turns // len(issue) for i, (span, s) in enumerate(issue)}
    plan = [[] for _ in range(turns)]
    for span, s in issue:
        plan[at_turn[span[0], s]].append(line_start(span, s))
    table = nearest(n)
    moves = []
    for s in range(n):
        latest = max(table[table[p][s]].index(p) for p in range(n))
        for g in range(len(groups)):
            ready = max(at_turn[a, latest] for a in groups[g]) + 1 if s else 0
            moves.append((ready, spread(g, s)))
        moves += [(0, pass_on(g, s)) for g in range(len(groups))]
    turn = 0
    for i, (ready, step) in enumerate(moves):
        late = max(0, i - len(groups))
        even = from_turn + late * (turns - from_turn) // (len(moves) - len(groups)) if late else 0
        turn = min(max(turn, ready, even), turns - 1)
        plan[turn].append(step)
    return own_start, plan, settle


def piece_rows(count, body):
    @pl.loop(0, count // 16)
    def _(r):
        body(pl.ds(pl.multiple_of(r * 16, 16), 16))


def give_steps(n, place, groups, grads, outs, bufs, sems, turns, from_turn, deliver):
    first_send, first_recv, second_send, second_recv, line_send, line_recv, mine_sem = sems
    group = lax.axis_index("fsdp")
    rows = outs[0].shape[-2]

    half_rows = rows // 2

    far = ranked(n, place)[::-1]

    def part(g, of_group, s, half):
        block = of_group * n + far[s]
        start = pl.multiple_of(block * rows + half * half_rows, half_rows)
        return grads[g].at[pl.ds(start, half_rows)]

    def mine_copy(g, s, half, k):
        target = group if k == 0 else jnp.bitwise_xor(group, 2 - half)
        return pltpu.make_async_copy(
            part(g, target, s, half), bufs[g]["mine"].at[s, half, k], mine_sem.at[g, s, half, k]
        )

    def first_copy(g, s, half, k):
        target = jnp.bitwise_xor(group, half + 1 if k == 0 else 3)
        return line_copy(
            part(g, target, s, half),
            bufs[g]["first"].at[s, half, k],
            first_send.at[g, s, half, k],
            first_recv.at[g, s, half, k],
            {"fsdp": jnp.bitwise_xor(group, half + 1)},
        )

    def second_copy(g, s, half):
        return line_copy(
            bufs[g]["second_out"].at[s, half],
            bufs[g]["second"].at[s, half],
            second_send.at[g, s, half],
            second_recv.at[g, s, half],
            {"fsdp": jnp.bitwise_xor(group, 2 - half)},
        )

    def line_moves(g, s, arrival=False):
        start = 0
        for a in groups[g]:
            width = outs[a].shape[1] // n
            quarter = far[s] if arrival else place
            ref = outs[a].at[:, pl.ds(pl.multiple_of(quarter * width, 128), width)]
            out = bufs[g]["line_out"].at[min(s, n - 2), :, pl.ds(start, width)]
            yield line_copy(
                ref if arrival else out,
                ref,
                line_send.at[a, s],
                line_recv.at[a, quarter],
                {"context": far[s]},
            )
            start += width

    def store(g, at, values):
        start = 0
        for a in groups[g]:
            width = outs[a].shape[1] // n
            cols = pl.ds(pl.multiple_of(place * width, 128), width)
            outs[a][at, cols] = values[:, start : start + width].astype(jnp.bfloat16)
            start += width

    def send_first(g, s):
        for k in (1, 0):
            for half in (0, 1):
                first_copy(g, s, half, k).start()
                mine_copy(g, s, half, k).start()

    def begin():
        for i in range(2 * len(groups)):
            g, s = order[i]
            send_first(g, s)

    def across(i):
        g, s = order[i]

        def step():
            for half in (0, 1):
                first_copy(g, s, half, 1).wait_recv()
                mine_copy(g, s, half, 1).wait()
                own = bufs[g]["mine"].at[s, half, 1]
                came = bufs[g]["first"].at[s, half, 1]
                out = bufs[g]["second_out"].at[s, half]

                def add(at, own=own, came=came, out=out):
                    out[at, :] = (
                        own[at, :].astype(jnp.float32) + came[at, :].astype(jnp.float32)
                    ).astype(jnp.bfloat16)

                piece_rows(half_rows, add)
                second_copy(g, s, half).start()
            if i + 2 * len(groups) < len(order):
                send_first(*order[i + 2 * len(groups)])

        return step

    def total(g, s):
        def step():
            for half in (0, 1):
                first_copy(g, s, half, 0).wait_recv()
                second_copy(g, s, half).wait_recv()
                mine_copy(g, s, half, 0).wait()
                own = bufs[g]["mine"].at[s, half, 0]
                one = bufs[g]["first"].at[s, half, 0]
                two = bufs[g]["second"].at[s, half]

                def add(at, own=own, one=one, two=two, half=half):
                    value = own[at, :].astype(jnp.float32) + one[at, :].astype(jnp.float32)
                    value = value + two[at, :].astype(jnp.float32)
                    to = pl.ds(pl.multiple_of(at.start + half * half_rows, 16), 16)
                    if not deliver:
                        width = value.shape[1]
                        start = sum(grads[h].shape[1] for h in range(g))
                        outs[0][far[s], to, start : start + width] = value.astype(jnp.bfloat16)
                    elif s == n - 1:
                        store(g, to, value)
                    else:
                        bufs[g]["line_out"][s, to, :] = value.astype(jnp.bfloat16)

                piece_rows(half_rows, add)
            if deliver and s < n - 1:
                for move in line_moves(g, s):
                    move.start()

        return step

    def settle():
        for g, s in order:
            for half in (0, 1):
                first_copy(g, s, half, 0).wait_send()
                first_copy(g, s, half, 1).wait_send()
                second_copy(g, s, half).wait_send()
            if deliver and s < n - 1:
                for move in line_moves(g, s):
                    move.wait_send()
                for move in line_moves(g, s, arrival=True):
                    move.wait_recv()

    count = len(groups)
    order = [(g, s) for s in range(n) for g in range(count)]
    steps = []
    for i in range(len(order) + count):
        if i < len(order):
            steps.append(across(i))
        if 0 <= i - count < len(order):
            steps.append(total(*order[i - count]))
    plan = [[] for _ in range(turns)]
    for i, step in enumerate(steps):
        plan[from_turn + i * (turns - from_turn) // len(steps)].append(step)
    return begin, plan, settle


def spread_steps(n, pieces, out, sems, turns, from_turn):
    own_send, near_send, near_recv, far_send, far_recv = sems
    group = lax.axis_index("fsdp")
    rows = pieces.shape[1]
    neighbours = ({"fsdp": jnp.bitwise_xor(group, 1)}, {"fsdp": jnp.bitwise_xor(group, 2)})

    def block(of_group, k, half=None):
        start = (of_group * n + k) * rows
        if half is None:
            return out.at[pl.ds(pl.multiple_of(start, rows), rows)]
        return out.at[pl.ds(pl.multiple_of(start + half * (rows // 2), rows // 2), rows // 2)]

    def own_copy(k):
        return pltpu.make_async_copy(pieces.at[k], block(group, k), own_send.at[k])

    def near_copy(way, k, of_group):
        return line_copy(
            pieces.at[k],
            block(of_group, k),
            near_send.at[way, k],
            near_recv.at[way, k],
            neighbours[way],
        )

    def far_copy(half, k, of_group):
        ref = block(of_group, k, half)
        return line_copy(
            ref, ref, far_send.at[half, k], far_recv.at[half, k], neighbours[1 - half]
        )

    def begin():
        for k in range(n):
            for way in (0, 1):
                near_copy(way, k, group).start()
            own_copy(k).start()

    def pass_on(k):
        def step():
            for half in (0, 1):
                source = jnp.bitwise_xor(group, half + 1)
                near_copy(half, k, source).wait_recv()
                far_copy(half, k, source).start()

        return step

    def settle():
        for k in range(n):
            own_copy(k).wait()
            for half in (0, 1):
                far_copy(half, k, jnp.bitwise_xor(group, 3)).wait_recv()
                far_copy(half, k, group).wait_send()
                near_copy(half, k, group).wait_send()

    plan = [[] for _ in range(turns)]
    for k in range(n):
        plan[from_turn + k * (turns - from_turn) // n].append(pass_on(k))
    return begin, plan, settle


def line_body(n, chunks, n_part, gather, spreading, n_in, n_join, n_rest, groups, giving, deliver, extra, finish, *refs):
    refs = list(refs)
    take = lambda count: [refs.pop(0) for _ in range(count)]
    reduce = n_part > 0
    fetching = bool(groups) and not giving
    arrays = sum(len(members) for members in groups)
    parts = take(n_part)
    ins = take(n_in)
    weights = take(arrays) if fetching else []
    grads = take(len(groups)) if giving else []
    others = take(1)[0] if extra else None
    pieces = take(1)[0] if spreading else None
    gathered_all = take(gather)
    joined = take(n_join)
    rest = take(n_rest)
    fetched = take(len(groups)) if fetching else []
    spread_out = take(1)[0] if spreading else None
    given = take(arrays if deliver else 1) if giving else []
    gains_out = take(1)[0] if extra else None
    if reduce:
        own, own_sem, across, sums_in, sums_out, summed = take(6)
        cross_send, cross_recv, sum_send, sum_recv = take(4)
    if gather:
        row_send, row_recv, pair_send, pair_recv = take(4)
    if n_join:
        join_send, join_recv = take(2)
    fetch_sems = take(7) if fetching else None
    spread_sems = take(5) if spreading else None
    if giving:
        names = ("mine", "first", "second_out", "second", "line_out")[: 5 if deliver else 4]
        give_bufs = [dict(zip(names, take(len(names)))) for _ in groups]
        give_sems = take(7)
    if extra:
        gain_own, gain_came, gain_line, gain_send, gain_recv, gain_line_send, gain_line_recv = take(7)

    place = lax.axis_index("context")
    core = lax.axis_index("tensor")
    other = {"tensor": 1 - core}
    step_rows = (ins[0].shape[0]) // chunks

    def rows(j):
        return pl.ds(j * step_rows, step_rows)

    line_barrier(n, place, core, bool(groups) or spreading)
    lag = LINE_LAG if reduce else 0
    turns = chunks * max(n_part, 1) + lag + n
    plan = [[] for _ in range(turns)]
    if fetching:
        start_turns = min(LINE_START_TURNS, chunks) if reduce else 1
        from_turn = LINE_FROM_TURN if reduce else 1
        own_start, plan, settle = fetch_steps(
            n, place, groups, weights, fetched, fetch_sems, turns, start_turns, from_turn
        )
    if fetching:
        own_start()
    if spreading:
        begin, plan, settle = spread_steps(
            n, pieces, spread_out, spread_sems, turns, LINE_FROM_TURN
        )
        begin()
    if giving:
        begin, plan, settle = give_steps(
            n, place, groups, grads, given, give_bufs, give_sems, turns, LINE_GIVE_TURN, deliver
        )
        begin()

    def cross(j):
        return line_copy(
            parts[j // chunks].at[:, 1 - core, rows(j % chunks)],
            across.at[:, rows(j)],
            cross_send.at[j],
            cross_recv.at[j],
            other,
        )

    def own_copy(j):
        return pltpu.make_async_copy(
            parts[j // chunks].at[:, core, rows(j % chunks)], own.at[:, rows(j)], own_sem.at[j]
        )

    def sum_copy(way, k, j):
        return line_copy(
            sums_out.at[way, k, rows(j)],
            sums_in.at[way, k, rows(j)],
            sum_send.at[way, k, j],
            sum_recv.at[way, k, j],
            {"context": place + 1 - 2 * way},
        )

    def own_term(target, j):
        return own[target, rows(j), :].astype(jnp.float32) + across[
            target, rows(j), :
        ].astype(jnp.float32)

    def send_sums(way, j):
        first = place == (n - 1) * way

        @pl.loop(0, n - 1)
        def _(k):
            target = jnp.where(way == 0, n - 1 - k, k)
            passes = jnp.where(way == 0, target - place, place - target) > 0

            @pl.when(passes & jnp.logical_not(first))
            def _():
                sum_copy(way, k, j).wait_recv()

            @pl.when(passes)
            def _():
                came = sums_in[way, k, rows(j), :].astype(jnp.float32)
                value = own_term(target, j) + jnp.where(first, 0.0, came)
                sums_out[way, k, rows(j), :] = value.astype(jnp.bfloat16)
                sum_copy(way, k, j).start()

    def row_copy(way, k, j, w=0):
        block = place - k if way == 0 else place + k
        device = {"context": place + 1 if way == 0 else place - 1}
        ref = gathered_all[w].at[block, core, rows(j)]
        return line_copy(ref, ref, row_send.at[w, way, k, j], row_recv.at[w, way, k, j], device)

    def row_arrival(way, k, j, w=0):
        block = place - 1 - k if way == 0 else place + 1 + k
        ref = gathered_all[w].at[block, core, rows(j)]
        return line_copy(ref, ref, row_send.at[w, way, k, j], row_recv.at[w, way, k, j], other)

    def pair_copy(block, half, j, w=0):
        ref = gathered_all[w].at[block, half, rows(j)]
        return line_copy(ref, ref, pair_send.at[w, block, j], pair_recv.at[w, block, j], other)

    def send_rows(j, values, w=0):
        gathered_all[w][place, core, rows(j), :] = values

        @pl.when(place < n - 1)
        def _():
            row_copy(0, 0, j, w).start()

        @pl.when(place > 0)
        def _():
            row_copy(1, 0, j, w).start()

        pair_copy(place, core, j, w).start()

    def finish_rows(j):
        total = None
        if reduce:

            summed[...] = own_term(place, j)

            @pl.when(place > 0)
            def _():
                sum_copy(0, n - 1 - place, j).wait_recv()
                summed[...] += sums_in[0, n - 1 - place, rows(j), :].astype(jnp.float32)

            @pl.when(place < n - 1)
            def _():
                sum_copy(1, place, j).wait_recv()
                summed[...] += sums_in[1, place, rows(j), :].astype(jnp.float32)

            total = summed[...]
        made = finish(j, rows(j % chunks), total, ins, rest)
        made = made if isinstance(made, tuple) else (made,)
        made = list(made)
        if gather and j < chunks:
            send_rows(j, made.pop(0))
        if made:
            i = j // chunks - (gather > 0)
            joined[i][core, rows(j % chunks), :] = made.pop(0)
            join_copy(i, core, j % chunks).start()

    def join_copy(i, half, j):
        ref = joined[i].at[half, rows(j)]
        return line_copy(ref, ref, join_send.at[i, j], join_recv.at[i, j], other)

    def pass_rows(k, j, w=0):
        for way in (0, 1):
            block = place - 1 - k if way == 0 else place + 1 + k
            here = block >= 0 if way == 0 else block <= n - 1
            onward = place < n - 1 if way == 0 else place > 0

            @pl.when(here)
            def _(way=way, block=block):
                row_arrival(way, k, j, w).wait_recv()

            if k + 1 <= n - 2:

                @pl.when(here & onward)
                def _(way=way):
                    row_copy(way, k + 1, j, w).start()

            @pl.when(here)
            def _(way=way, block=block):
                pair_copy(block, core, j, w).start()

    all_chunks = chunks * max(n_part, 1)
    if reduce:
        for j in range(all_chunks):
            cross(j).start()
            own_copy(j).start()

    def gains_plan():
        group = lax.axis_index("fsdp")
        hops = (
            other,
            {"fsdp": jnp.bitwise_xor(group, 1)},
            {"fsdp": jnp.bitwise_xor(group, 2)},
        )

        def hop(h):
            return line_copy(
                gain_own.at[h], gain_came.at[h], gain_send.at[h], gain_recv.at[h], hops[h]
            )

        def line_hop(s):
            return line_copy(
                gain_line.at[place],
                gain_line.at[place],
                gain_line_send.at[s - 1],
                gain_line_recv.at[s - 1],
                {"context": lax.rem(place + s, n)},
            )

        def line_hop_in(s):
            ref = gain_line.at[lax.rem(place + n - s, n)]
            return line_copy(
                ref, ref, gain_line_send.at[s - 1], gain_line_recv.at[s - 1], other
            )

        def first():
            gain_own[0] = others[...]
            hop(0).start()

        def next_hop(h):
            def step():
                hop(h).wait_recv()
                value = gain_own[h] + gain_came[h]
                if h < 2:
                    gain_own[h + 1] = value
                    hop(h + 1).start()
                else:
                    gain_line[place] = value
                    for s in range(1, n):
                        line_hop(s).start()

            return step

        def last():
            for s in range(1, n):
                line_hop_in(s).wait_recv()
            value = gain_line[0]
            for p in range(1, n):
                value = value + gain_line[p]
            gains_out[...] = value
            for h in range(3):
                hop(h).wait_send()
            for s in range(1, n):
                line_hop(s).wait_send()

        return [first, next_hop(0), next_hop(1), next_hop(2), last]

    near = jnp.where(place < n // 2, 0, 1)
    gain_steps = gains_plan() if extra else []
    if not reduce:
        for j in range(chunks):
            finish_rows(j)
    for i in range(turns):
        for step in plan[i]:
            step()
        if gather > 1 and 0 <= i - LINE_PLAIN_FROM < chunks:
            j = i - LINE_PLAIN_FROM
            send_rows(j, ins[-1][rows(j), :], 1)
        if reduce and i < all_chunks:
            own_copy(i).wait()
            cross(i).wait_recv()
            send_sums(near, i)
        if reduce and 0 <= i - 1 < all_chunks:
            send_sums(1 - near, i - 1)
        if reduce and 0 <= i - lag < all_chunks:
            finish_rows(i - lag)
        if i > 0 and gain_steps:
            gain_steps.pop(0)()
        if gather:
            for k in range(n - 1):
                if 0 <= i - lag - 1 - k < chunks:
                    pass_rows(k, i - lag - 1 - k)
                if gather > 1 and 0 <= i - LINE_PLAIN_LAG - k * LINE_PLAIN_STEP < chunks:
                    pass_rows(k, i - LINE_PLAIN_LAG - k * LINE_PLAIN_STEP, 1)

    for step in gain_steps:
        step()
    if gather > 1:
        for i in range(turns, turns + LINE_PLAIN_LAG + (n - 2) * LINE_PLAIN_STEP):
            for k in range(n - 1):
                if 0 <= i - LINE_PLAIN_LAG - k * LINE_PLAIN_STEP < chunks:
                    pass_rows(k, i - LINE_PLAIN_LAG - k * LINE_PLAIN_STEP, 1)
    if groups or spreading:
        settle()
    for j in range(all_chunks):
        if reduce:
            cross(j).wait_send()
            for k in range(n - 1):

                @pl.when(place < n - 1 - k)
                def _(k=k, j=j):
                    sum_copy(0, k, j).wait_send()

                @pl.when(place > k)
                def _(k=k, j=j):
                    sum_copy(1, k, j).wait_send()

        for w in range(gather if j < chunks else 0):
            for block in range(n):
                pair_copy(block, 1 - core, j, w).wait_recv()
                pair_copy(block, core, j, w).wait_send()
            for k in range(n - 1):

                @pl.when((place < n - 1) & (place >= k))
                def _(k=k, j=j, w=w):
                    row_copy(0, k, j, w).wait_send()

                @pl.when((place > 0) & (place + k <= n - 1))
                def _(k=k, j=j, w=w):
                    row_copy(1, k, j, w).wait_send()

        i = j // chunks - (gather > 0)
        if n_join and i >= 0:
            join_copy(i, 1 - core, j % chunks).wait_recv()
            join_copy(i, core, j % chunks).wait_send()


def line_call(
    n,
    collective,
    finish,
    part,
    ins,
    gather=0,
    joins=(),
    rests=(),
    chunks=LINE_CHUNKS,
    groups=(),
    weights=(),
    grads=(),
    deliver=True,
    extra=None,
    pieces=None,
):
    parts = () if part is None else part if isinstance(part, tuple) else (part,)
    reduce = len(parts) > 0
    giving = len(grads) > 0
    row_count, model_width = ins[0].shape
    vmem = pl.BlockSpec(memory_space=pltpu.VMEM)
    outs = []
    for _ in range(gather):
        outs.append(jax.ShapeDtypeStruct((n, 2, row_count, model_width), jnp.bfloat16))
    outs += [jax.ShapeDtypeStruct((2, row_count, model_width), kind) for kind in joins]
    outs += list(rests)
    out_specs = [vmem] * len(outs)
    for members in groups if not giving else ():
        rows = weights[0].shape[0] * n * lax.axis_size("fsdp")
        width = sum(weights[a].shape[1] for a in members) // n
        outs.append(jax.ShapeDtypeStruct((rows, width), jnp.bfloat16))
        out_specs.append(pl.BlockSpec(memory_space=pl.ANY))
    dma = pltpu.SemaphoreType.DMA
    if pieces is not None:
        rows = pieces.shape[0] * pieces.shape[1] * lax.axis_size("fsdp")
        outs.append(jax.ShapeDtypeStruct((rows, pieces.shape[2]), jnp.bfloat16))
        out_specs.append(pl.BlockSpec(memory_space=pl.ANY))
    if giving:
        owned = grads[0].shape[0] // (n * lax.axis_size("fsdp"))
        shapes = [(owned, width * n) for width in weights]
        if not deliver:
            shapes = [(n, owned, sum(grad.shape[1] for grad in grads))]
        for shape in shapes:
            outs.append(jax.ShapeDtypeStruct(shape, jnp.bfloat16))
            out_specs.append(vmem)
    if extra is not None:
        outs.append(jax.ShapeDtypeStruct(extra.shape, jnp.float32))
        out_specs.append(vmem)
    total_chunks = chunks * max(len(parts), 1)
    sum_rows = row_count * max(len(parts), 1)
    scratch = []
    if reduce:
        slot = pltpu.VMEM((2, n - 1, sum_rows, model_width), jnp.bfloat16)
        scratch += [pltpu.VMEM((n, sum_rows, model_width), jnp.bfloat16), dma((total_chunks,))]
        scratch += [pltpu.VMEM((n, sum_rows, model_width), jnp.bfloat16), slot, slot]
        scratch += [pltpu.VMEM((row_count // chunks, model_width), jnp.float32)]
        tally = (2, n - 1, total_chunks)
        scratch += [dma((total_chunks,)), dma((total_chunks,)), dma(tally), dma(tally)]
    if gather:
        tally = (gather, 2, n - 1, chunks)
        scratch += [dma(tally), dma(tally), dma((gather, n, chunks)), dma((gather, n, chunks))]
    if joins:
        scratch += [dma((len(joins), chunks)), dma((len(joins), chunks))]
    if groups and not giving:
        arrays = len(weights)
        tally = (2, len(groups), n)
        scratch += [dma((arrays,)), dma((arrays, n)), dma((arrays, n))]
        scratch += [dma(tally), dma(tally), dma(tally), dma(tally)]
    if pieces is not None:
        scratch += [dma((n,))] + [dma((2, n))] * 4
    if giving:
        for grad in grads:
            halves = (owned // 2, grad.shape[1])
            for lead in ((n, 2, 2), (n, 2, 2), (n, 2), (n, 2)):
                scratch.append(pltpu.VMEM(lead + halves, jnp.bfloat16))
            if deliver:
                scratch.append(pltpu.VMEM((n - 1, owned, grad.shape[1]), jnp.bfloat16))
        count = len(groups)
        scratch += [dma((count, n, 2, 2)), dma((count, n, 2, 2))]
        scratch += [dma((count, n, 2)), dma((count, n, 2))]
        scratch += [dma((len(weights), n)), dma((len(weights), n)), dma((count, n, 2, 2))]
    if extra is not None:
        stack = pltpu.VMEM((3,) + extra.shape, jnp.float32)
        scratch += [stack, stack, pltpu.VMEM((n,) + extra.shape, jnp.float32)]
        scratch += [dma((3,)), dma((3,)), dma((n - 1,)), dma((n - 1,))]
    operands = list(parts) + list(ins) + (list(grads) if giving else list(weights))
    operands += [] if extra is None else [extra]
    operands += [] if pieces is None else [pieces]
    anywhere = [*parts, *grads]
    in_specs = [
        pl.BlockSpec(memory_space=pl.ANY) if any(a is b for b in anywhere) else vmem
        for a in operands
    ]
    moved = row_count * model_width * 2 * n * (2 * reduce + 2 * gather)
    return pl.pallas_call(
        functools.partial(
            line_body,
            n,
            chunks,
            len(parts),
            gather,
            pieces is not None,
            len(ins),
            len(joins),
            len(rests),
            groups,
            giving,
            deliver,
            extra is not None,
            finish,
        ),
        out_shape=tuple(outs),
        in_specs=in_specs,
        out_specs=tuple(out_specs),
        scratch_shapes=scratch,
        compiler_params=pltpu.CompilerParams(
            collective_id=collective, has_side_effects=True, vmem_limit_bytes=56 << 20
        ),
        cost_estimate=pl.CostEstimate(
            flops=moved, bytes_accessed=20 * moved, transcendentals=0
        ),
    )(*operands)


def finish_gather(j, rows, total, ins, rest):
    values = ins[0][rows, :].astype(jnp.float32)
    return (values * rms_scale(values) * ins[1][...]).astype(jnp.bfloat16)


def finish_attention(j, rows, total, ins, rest):
    residual = ins[0][rows, :].astype(jnp.float32) + total
    rest[0][rows, :] = residual
    return (residual * rms_scale(residual) * ins[1][...]).astype(jnp.bfloat16)


def gain_rows(j, rest, terms):
    sums = jnp.sum(terms, axis=0, keepdims=True)
    rest[...] = sums if j == 0 else rest[...] + sums


def finish_mlp_back(j, rows, total, ins, rest):
    residual = ins[0][rows, :]
    if j >= LINE_CHUNKS:
        return (residual + total).astype(jnp.bfloat16)
    scale = rms_scale(residual)
    hat = residual * scale
    grad = ins[1][rows, :].astype(jnp.float32) + norm_back(total, hat, scale, ins[2][...])
    rest[0][rows, :] = grad
    gain_rows(j, rest[1], total * hat)
    return grad.astype(jnp.bfloat16)


def finish_tokens(j, rows, total, ins, rest):
    values = ins[1][rows, :].astype(jnp.float32)
    scale = rms_scale(values)
    hat = values * scale
    return ins[0][rows, :] + norm_back(total, hat, scale, ins[2][...])


def permuted_tokens(rows):
    n = lax.axis_size("context")
    place = lax.axis_index("context")
    core = lax.axis_index("tensor")
    shape = rows.shape
    near = jnp.zeros((n,) + shape, rows.dtype)
    for s in range(n):
        ring = [(i, (i + s) % n) for i in range(n)]
        came = lax.ppermute(rows, "context", ring) if s else rows
        near = lax.dynamic_update_slice(near, came[None], (lax.rem(place + n - s, n), 0, 0))
    far = lax.ppermute(near, "tensor", [(0, 1), (1, 0)])
    both = jnp.zeros((n, 2) + shape, rows.dtype)
    both = lax.dynamic_update_slice(both, near[:, None], (0, core, 0, 0))
    both = lax.dynamic_update_slice(both, far[:, None], (0, 1 - core, 0, 0))
    return both.reshape(n * 2 * shape[0], shape[1])


BACK_BLOCK = 256


def attend_back_body(kv_heads, group, queries, keys, values, grads, d_queries, d_keys, d_values):
    length = queries.shape[0]
    scale = 1.0 / math.sqrt(HEAD_DIM)
    d_keys[...] = jnp.zeros_like(d_keys)
    d_values[...] = jnp.zeros_like(d_values)
    for h in range(kv_heads):
        own = slice(h * HEAD_DIM, (h + 1) * HEAD_DIM)
        for start in range(0, length, BACK_BLOCK):
            end = start + BACK_BLOCK
            shape = (BACK_BLOCK, end)
            at = lax.broadcasted_iota(jnp.int32, shape, 0) + start
            visible = lax.broadcasted_iota(jnp.int32, shape, 1) <= at
            key, value = keys[0:end, own], values[0:end, own]
            for m in range(h * group, (h + 1) * group):
                cols = slice(m * HEAD_DIM, (m + 1) * HEAD_DIM)
                query, grad = queries[start:end, cols], grads[start:end, cols]
                weights = jnp.where(visible, jnp.exp(column_product(query, key) * scale), 0.0)
                probs = weights / jnp.sum(weights, axis=1, keepdims=True)
                grad_probs = column_product(grad, value)
                delta = jnp.sum(probs * grad_probs, axis=1, keepdims=True)
                grad_scores = (probs * (grad_probs - delta)).astype(jnp.bfloat16)
                d_queries[start:end, cols] = (
                    jnp.dot(grad_scores, key, preferred_element_type=jnp.float32) * scale
                )
                d_keys[0:end, own] += row_product(grad_scores, query) * scale
                d_values[0:end, own] += row_product(probs.astype(jnp.bfloat16), grad)


def attend_back(kv_heads, group, queries, keys, values, grads):
    vmem = pl.BlockSpec(memory_space=pltpu.VMEM)
    shapes = [jax.ShapeDtypeStruct(a.shape, jnp.float32) for a in (queries, keys, values)]
    work = 5 * queries.shape[0] ** 2 * queries.shape[1]
    return pl.pallas_call(
        functools.partial(attend_back_body, kv_heads, group),
        out_shape=tuple(shapes),
        in_specs=[vmem] * 4,
        out_specs=(vmem,) * 3,
        compiler_params=pltpu.CompilerParams(vmem_limit_bytes=48 << 20),
        cost_estimate=pl.CostEstimate(flops=work, bytes_accessed=4 << 20, transcendentals=0),
        name="attend_back",
    )(queries, keys, values, grads)


def widen_body(h_cols, out, tokens, mlp, *refs):
    attn, results = refs[:4], refs[4:]
    results[0][...] = out[...]
    results[1][...] = tokens[...]
    for a in range(4):
        results[2 + a][...] = attn[a][...].astype(jnp.float32)
    for q in range(mlp.shape[0]):
        for a in range(3):
            piece = mlp[q, :, a * h_cols : (a + 1) * h_cols].astype(jnp.float32)
            results[6 + a][:, q * h_cols : (q + 1) * h_cols] = piece


def widen(parts, h_cols, out, tokens, mlp, *attn):
    rows = mlp.shape[1]
    width = out.shape[-1]
    out, tokens = out.reshape(-1, width), tokens.reshape(-1, width)
    steps = parts // 2
    token_rows = pl.BlockSpec((out.shape[0] // steps, width), lambda i: (i, 0))
    quarters = [pl.BlockSpec((rows, a.shape[1] // steps), lambda i: (0, i)) for a in attn]
    hidden = pl.BlockSpec((rows, 2 * h_cols), lambda i: (0, i))
    pieces = pl.BlockSpec((2,) + mlp.shape[1:], lambda i: (i, 0, 0))
    results = [jax.ShapeDtypeStruct(a.shape, a.dtype) for a in (out, tokens)]
    results += [jax.ShapeDtypeStruct(a.shape, jnp.float32) for a in attn]
    results += [jax.ShapeDtypeStruct((rows, h_cols * parts), jnp.float32)] * 3
    return pl.pallas_call(
        functools.partial(widen_body, h_cols),
        grid=(steps,),
        in_specs=[token_rows, token_rows, pieces] + quarters,
        out_specs=tuple([token_rows, token_rows] + quarters + [hidden] * 3),
        out_shape=tuple(results),
        name="widen",
    )(out, tokens, mlp, *attn)


def token_half(block, index, parts):
    rows = block.shape[0] // parts
    return lax.dynamic_slice_in_dim(block, index * rows, rows, axis=0)


def line_shards(
    tokens,
    cotangent,
    norm_gain_attn,
    norm_gain_mlp,
    head_gains,
    query_weight,
    key_matrix,
    value_matrix,
    output_weight,
    gate_weight,
    up_weight,
    down_weight,
):
    _, local_len, model_width = tokens.shape
    parts = lax.axis_size("context")
    cores = lax.axis_size("tensor")
    core = lax.axis_index("tensor")
    full_len = local_len * parts
    q_cols = query_weight.shape[1] // parts
    kv_cols = key_matrix.shape[1] // parts
    h_cols = gate_weight.shape[1] // parts
    q_heads = q_cols // HEAD_DIM
    kv_heads = kv_cols // HEAD_DIM
    head_group = q_heads // kv_heads
    score_scale = 1.0 / math.sqrt(HEAD_DIM)
    positions = jnp.arange(full_len, dtype=jnp.int32)
    cosine_table, sine_table = rope_tables(positions, HEAD_DIM)
    cosine_table = cosine_table[:, None, :]
    sine_table = sine_table[:, None, :]
    visible = positions[None, :] <= positions[:, None]
    gain_attn = norm_gain_attn.astype(jnp.float32)[None]
    gain_mlp = norm_gain_mlp.astype(jnp.float32)[None]
    gain_heads = head_gains.astype(jnp.float32)

    def line_parts(left, right):
        product = column_product(left, right).astype(jnp.bfloat16)
        return product.reshape(parts, cores, half_len, model_width)

    own_cot = token_half(cotangent.reshape(local_len, model_width), core, cores)
    inputs = token_half(tokens.reshape(local_len, model_width), core, cores)
    half_len = local_len // cores
    rows_f32 = jax.ShapeDtypeStruct((half_len, model_width), jnp.float32)
    sums_f32 = jax.ShapeDtypeStruct((1, model_width), jnp.float32)
    normed_attn, in_weights, out_weights = line_call(
        parts,
        1,
        finish_gather,
        None,
        (inputs, gain_attn),
        gather=1,
        groups=((0, 1, 2), (3,)),
        weights=(query_weight, key_matrix, value_matrix, output_weight),
    )
    normed_attn = normed_attn.reshape(full_len, model_width)
    own_cot, normed_attn = lax.optimization_barrier((own_cot, normed_attn))
    grad_out = permuted_tokens(own_cot)

    raw = jnp.dot(normed_attn, in_weights, preferred_element_type=jnp.float32)
    query_split = raw[:, :q_cols].reshape(full_len, q_heads, HEAD_DIM)
    query_scale = rms_scale(query_split)
    query_hat = query_split * query_scale
    queries = rotate(query_hat * gain_heads[0], cosine_table, sine_table).astype(jnp.bfloat16)
    key_split = raw[:, q_cols : q_cols + kv_cols].reshape(full_len, kv_heads, HEAD_DIM)
    key_scale = rms_scale(key_split)
    key_hat = key_split * key_scale
    keys = rotate(key_hat * gain_heads[1], cosine_table, sine_table).astype(jnp.bfloat16)
    values = raw[:, q_cols + kv_cols :].astype(jnp.bfloat16).reshape(full_len, kv_heads, HEAD_DIM)
    queries = queries.reshape(full_len, kv_heads, head_group, HEAD_DIM)

    scores = (
        jnp.einsum("ikgd,jkd->kgij", queries, keys, preferred_element_type=jnp.float32)
        * score_scale
    )
    weights = jnp.where(visible, jnp.exp(scores), 0.0)
    probs = weights / jnp.sum(weights, axis=-1, keepdims=True)
    probs_low = probs.astype(jnp.bfloat16)
    attended = (
        jnp.einsum("kgij,jkd->ikgd", probs_low, values, preferred_element_type=jnp.float32)
        .astype(jnp.bfloat16)
        .reshape(full_len, q_cols)
    )
    normed_mlp, residual, mlp_in, mlp_down = line_call(
        parts,
        2,
        finish_attention,
        line_parts(attended, out_weights),
        (inputs, gain_mlp),
        gather=1,
        rests=(rows_f32,),
        groups=((0, 1), (2,)),
        weights=(gate_weight, up_weight, down_weight),
    )
    normed_mlp = normed_mlp.reshape(full_len, model_width)

    both = jnp.dot(normed_mlp, mlp_in, preferred_element_type=jnp.float32)
    gate_act = both[:, :h_cols]
    upward = both[:, h_cols:]
    sig_gate = jax.nn.sigmoid(gate_act)
    activated = gate_act * sig_gate
    hidden = (activated * upward).astype(jnp.bfloat16)
    grad_hidden = jnp.dot(grad_out, mlp_down, preferred_element_type=jnp.float32)
    derivative = sig_gate * (1.0 + gate_act * (1.0 - sig_gate))
    grad_gate = (grad_hidden * upward * derivative).astype(jnp.bfloat16)
    grad_up = (grad_hidden * activated).astype(jnp.bfloat16)
    grad_both = jnp.concatenate([grad_gate, grad_up], axis=1)
    grad_in = row_product(normed_mlp, grad_both).astype(jnp.bfloat16)
    grad_down = row_product(grad_out, hidden).astype(jnp.bfloat16)
    grad_branch, out, grad_residual, gain_mlp_part, mlp_grads = line_call(
        parts,
        3,
        finish_mlp_back,
        (line_parts(grad_both, mlp_in), line_parts(hidden, mlp_down)),
        (residual, own_cot, gain_mlp),
        gather=1,
        joins=(jnp.bfloat16,),
        rests=(rows_f32, sums_f32),
        groups=((0, 1), (2,)),
        weights=(h_cols, h_cols, h_cols),
        grads=(grad_in, grad_down),
        deliver=False,
    )
    mlp_grads = lax.all_to_all(mlp_grads, "context", split_axis=0, concat_axis=0, tiled=True)
    grad_branch = grad_branch.reshape(full_len, model_width)
    grad_attended = jnp.dot(grad_branch, out_weights, preferred_element_type=jnp.float32)
    grad_attended = grad_attended.astype(jnp.bfloat16)
    grad_queries, grad_keys, grad_values = attend_back(
        kv_heads,
        head_group,
        queries.reshape(full_len, q_cols),
        keys.reshape(full_len, kv_cols),
        values.reshape(full_len, kv_cols),
        grad_attended,
    )
    grad_queries = grad_queries.reshape(full_len, q_heads, HEAD_DIM)
    grad_keys = grad_keys.reshape(full_len, kv_heads, HEAD_DIM)
    grad_query_hat = unrotate(grad_queries, cosine_table, sine_table)
    grad_key_hat = unrotate(grad_keys, cosine_table, sine_table)
    heads_part = jnp.stack(
        [
            jnp.sum(grad_query_hat * query_hat, axis=(0, 1)),
            jnp.sum(grad_key_hat * key_hat, axis=(0, 1)),
        ]
    )
    grad_raw = jnp.concatenate(
        [
            norm_back(grad_query_hat, query_hat, query_scale, gain_heads[0]).reshape(
                full_len, q_cols
            ),
            norm_back(grad_key_hat, key_hat, key_scale, gain_heads[1]).reshape(full_len, kv_cols),
            grad_values.reshape(full_len, kv_cols),
        ],
        axis=1,
    ).astype(jnp.bfloat16)
    attn_in_grad = row_product(normed_attn, grad_raw).astype(jnp.bfloat16)
    attn_out_grad = row_product(grad_branch, attended).astype(jnp.bfloat16)
    gain_attn_part = (
        jnp.sum(attn_in_grad.astype(jnp.float32) * in_weights.astype(jnp.float32), axis=1)[None]
        / gain_attn
    )
    gains = jnp.concatenate(
        [
            gain_attn_part,
            gain_mlp_part,
            jnp.pad(heads_part.reshape(1, -1), ((0, 0), (0, model_width - heads_part.size))),
            jnp.zeros((5, model_width), jnp.float32),
        ],
        axis=0,
    )
    grad_tokens, query_grad, key_grad, value_grad, output_grad, totals = line_call(
        parts,
        4,
        finish_tokens,
        line_parts(grad_raw, in_weights),
        (grad_residual, inputs, gain_attn),
        joins=(jnp.float32,),
        groups=((0, 1, 2), (3,)),
        weights=(q_cols, kv_cols, kv_cols, q_cols),
        grads=(attn_in_grad, attn_out_grad),
        extra=gains,
    )
    ready = (out, grad_tokens, mlp_grads, query_grad, key_grad, value_grad, output_grad)
    out, grad_tokens, *weight_grads = widen(parts, h_cols, *ready)
    return (
        out.reshape(tokens.shape),
        grad_tokens.reshape(tokens.shape),
        totals[0],
        totals[1],
        totals[2, : heads_part.size].reshape(heads_part.shape),
        *weight_grads,
    )


def layer(*operands):
    tokens, key_matrix, gate_weight = operands[0], operands[6], operands[9]
    parts = lax.axis_size("context")
    cores = lax.axis_size("tensor")
    fits = (
        tokens.shape[0] == 1
        and key_matrix.shape[1] % (parts * HEAD_DIM) == 0
        and gate_weight.shape[1] % (parts * HEAD_DIM) == 0
        and tokens.shape[1] % (cores * LINE_CHUNKS * 16) == 0
        and cores == 2
        and parts % 2 == 0
        and tokens.shape[1] * parts % BACK_BLOCK == 0
        and lax.axis_size("fsdp") == 4
    )
    return line_shards(*operands) if fits else shards(*operands)


def solution(mesh):
    return jax.shard_map(
        layer,
        mesh=mesh,
        in_specs=(
            P("fsdp", "context", None),
            P("fsdp", "context", None),
            P(),
            P(),
            P(),
            P(("fsdp", "context"), "tensor"),
            P(("fsdp", "context"), "tensor"),
            P(("fsdp", "context"), "tensor"),
            P(("fsdp", "context"), "tensor"),
            P(("fsdp", "context"), "tensor"),
            P(("fsdp", "context"), "tensor"),
            P(("fsdp", "context"), "tensor"),
        ),
        out_specs=(
            P("fsdp", "context", None),
            P("fsdp", "context", None),
            P(),
            P(),
            P(),
            P(("fsdp", "context"), "tensor"),
            P(("fsdp", "context"), "tensor"),
            P(("fsdp", "context"), "tensor"),
            P(("fsdp", "context"), "tensor"),
            P(("fsdp", "context"), "tensor"),
            P(("fsdp", "context"), "tensor"),
            P(("fsdp", "context"), "tensor"),
        ),
        check_vma=False,
    )
```
